8 devices in a mesh: tp: 4 (over z, y, x), ep: 2 (over core).
Axes of the slice: x: 2, y: 2, z: 1, core: 2. Of those that a mesh axis runs over, the one named last changes fastest.
Arguments:
- x: bfloat16 [8192, 2048], P(('ep', 'tp'))
- y_grad: bfloat16 [8192, 2048], P(('ep', 'tp'))
- expert_ids: int32 [8192, 2], P(('ep', 'tp'))
- norm_gain: bfloat16 [2048], replicated
- w_router: bfloat16 [2048, 8], replicated
- w_gate: bfloat16 [8, 2048, 5632], P('ep', None, 'tp')
- w_up: bfloat16 [8, 2048, 5632], P('ep', None, 'tp')
- w_down: bfloat16 [8, 5632, 2048], P('ep', 'tp')
Outputs:
- output 1: bfloat16 [8192, 2048], P(('ep', 'tp'))
- output 2: bfloat16 [8192, 2048], P(('ep', 'tp'))
- output 3: bfloat16 [2048], replicated
- output 4: bfloat16 [2048, 8], replicated
- output 5: bfloat16 [8, 2048, 5632], P('ep', None, 'tp')
- output 6: bfloat16 [8, 2048, 5632], P('ep', None, 'tp')
- output 7: bfloat16 [8, 5632, 2048], P('ep', 'tp')
- output 8: float32 [], replicated
- output 9: float32 [], replicated
All inputs are finite; a program needn't handle non-finite values.
Results may differ from the reference program's by a relative error of at most 0.0154491.
Values are sent between devices in bfloat16 or wider.
A program may use at most 1 GiB of HBM per device.

```python
import jax
import jax.numpy as jnp
from jax import lax

BLOCKS = 8
BLOCK_TOKENS = 1024
MODEL_DIM = 2048
FFN_DIM = 5632
NUM_EXPERTS = 8
TOP_K = 2
CAPACITY = 512
SEQ_LEN = BLOCKS * BLOCK_TOKENS
EXPERT_ROWS = BLOCKS * CAPACITY
NORM_EPS = 1e-6
ACT_COEF = 1e-5
BALANCE_COEF = 1e-3


def draw_routing(key):
    key_delta, key_label, key_order = jax.random.split(key, 3)
    half_cap = CAPACITY // 2
    pair_total = (NUM_EXPERTS - 4) // 2
    deltas = jax.random.randint(key_delta, (BLOCKS, pair_total), 0, half_cap, dtype=jnp.int32)
    pair_counts = jnp.stack([half_cap + deltas, half_cap - deltas], axis=-1).reshape(BLOCKS, 2 * pair_total)
    head_counts = jnp.broadcast_to(jnp.array([2 * half_cap, 1, half_cap - 1, half_cap], dtype=jnp.int32), (BLOCKS, 4))
    run_ends = jnp.cumsum(jnp.concatenate([head_counts, pair_counts.astype(jnp.int32)], axis=1), axis=1)
    positions = jnp.arange(TOP_K * BLOCK_TOKENS, dtype=jnp.int32)
    ordinal = jax.vmap(lambda row_ends: jnp.searchsorted(row_ends, positions, side="right"))(run_ends)
    labels = jax.random.permutation(key_label, NUM_EXPERTS).astype(jnp.int32)
    choice = labels[ordinal].reshape(BLOCKS, TOP_K, BLOCK_TOKENS)
    orders = jax.vmap(lambda one_key: jax.random.permutation(one_key, BLOCK_TOKENS))(jax.random.split(key_order, BLOCKS))
    shuffled = jnp.take_along_axis(choice, jnp.broadcast_to(orders[:, None, :], choice.shape), axis=2)
    return jnp.transpose(shuffled, (0, 2, 1)).reshape(SEQ_LEN, TOP_K).astype(jnp.int32)


def setup_inputs(seed: int = 0) -> dict:
    key_list = jax.random.split(jax.random.key(seed), 10)
    noise = jax.random.normal(key_list[0], (BLOCKS, BLOCK_TOKENS, MODEL_DIM), jnp.float32)
    block_shift = 0.7 * jax.random.normal(key_list[1], (BLOCKS, 1, MODEL_DIM), jnp.float32)
    x = (noise + block_shift).reshape(SEQ_LEN, MODEL_DIM).astype(jnp.bfloat16)
    y_grad = jax.random.normal(key_list[2], (SEQ_LEN, MODEL_DIM), jnp.float32).astype(jnp.bfloat16)
    norm_gain = (1.0 + 0.3 * jax.random.normal(key_list[3], (MODEL_DIM,), jnp.float32)).astype(jnp.bfloat16)
    col_scale = jax.random.uniform(key_list[4], (NUM_EXPERTS,), jnp.float32, 0.5, 2.0)
    w_router = (jax.random.normal(key_list[5], (MODEL_DIM, NUM_EXPERTS), jnp.float32) * col_scale * MODEL_DIM ** -0.5).astype(jnp.bfloat16)
    wide_shape = (NUM_EXPERTS, MODEL_DIM, FFN_DIM)
    w_gate = (jax.random.normal(key_list[6], wide_shape, jnp.float32) * MODEL_DIM ** -0.5).astype(jnp.bfloat16)
    w_up = (jax.random.normal(key_list[7], wide_shape, jnp.float32) * MODEL_DIM ** -0.5).astype(jnp.bfloat16)
    down_scale = 0.8 * NUM_EXPERTS * (TOP_K * FFN_DIM) ** -0.5
    w_down = (jax.random.normal(key_list[8], (NUM_EXPERTS, FFN_DIM, MODEL_DIM), jnp.float32) * down_scale).astype(jnp.bfloat16)
    expert_ids = draw_routing(key_list[9])
    return {"x": x, "y_grad": y_grad, "expert_ids": expert_ids, "norm_gain": norm_gain, "w_router": w_router, "w_gate": w_gate, "w_up": w_up, "w_down": w_down}


def expert_block(operands):
    rows, gate_mat, up_mat, down_mat = operands
    pre_gate = jnp.dot(rows, gate_mat, preferred_element_type=jnp.float32)
    pre_up = jnp.dot(rows, up_mat, preferred_element_type=jnp.float32)
    hidden = (jax.nn.silu(pre_gate) * pre_up).astype(jnp.bfloat16)
    return jnp.dot(hidden, down_mat, preferred_element_type=jnp.float32).astype(jnp.bfloat16)


def reference(x, y_grad, expert_ids, norm_gain, w_router, w_gate, w_up, w_down):
    flat_ids = expert_ids.reshape(-1)
    expert_range = jnp.arange(NUM_EXPERTS, dtype=jnp.int32)
    id_hot = (flat_ids[:, None] == expert_range[None, :]).astype(jnp.int32)
    position = jnp.sum((jnp.cumsum(id_hot, axis=0) - 1) * id_hot, axis=1)
    slot = flat_ids * EXPERT_ROWS + position
    assign_count = SEQ_LEN * TOP_K
    owner = jnp.arange(assign_count, dtype=jnp.int32) // TOP_K - SEQ_LEN
    source = jax.ops.segment_sum(owner, slot, num_segments=NUM_EXPERTS * EXPERT_ROWS) + SEQ_LEN
    choice = (expert_ids[:, :, None] == expert_range[None, None, :]).astype(jnp.float32)
    counts = jnp.sum(choice, axis=(0, 1))

    def forward(x_in, gain_in, router_in, gate_in, up_in, down_in):
        x_float = x_in.astype(jnp.float32)
        inv_rms = lax.rsqrt(jnp.mean(x_float * x_float, axis=-1, keepdims=True) + NORM_EPS)
        x_norm = (x_float * inv_rms * gain_in.astype(jnp.float32)).astype(jnp.bfloat16)
        route_prob = jax.nn.softmax(jnp.dot(x_norm, router_in, preferred_element_type=jnp.float32), axis=-1)
        gates = jnp.sum(choice * route_prob[:, None, :], axis=-1)
        rows = jnp.take(x_norm, source, axis=0, mode="fill", fill_value=0).reshape(NUM_EXPERTS, EXPERT_ROWS, MODEL_DIM)
        expert_out = lax.map(jax.checkpoint(expert_block), (rows, gate_in, up_in, down_in))
        picked = jnp.take(expert_out.reshape(NUM_EXPERTS * EXPERT_ROWS, MODEL_DIM), slot, axis=0)
        moe_out = jnp.sum(gates[:, :, None] * picked.reshape(SEQ_LEN, TOP_K, MODEL_DIM).astype(jnp.float32), axis=1)
        y = (x_float + moe_out).astype(jnp.bfloat16)
        balance_loss = BALANCE_COEF * NUM_EXPERTS * jnp.sum(counts / (SEQ_LEN * TOP_K) * jnp.mean(route_prob, axis=0))
        act_loss = ACT_COEF * jnp.mean(moe_out * moe_out)
        return y, balance_loss, act_loss

    (y, balance_loss, act_loss), pullback = jax.vjp(forward, x, norm_gain, w_router, w_gate, w_up, w_down)
    loss_weight = jnp.ones((), jnp.float32)
    x_grad, gain_grad, router_grad, gate_grad, up_grad, down_grad = pullback((y_grad, loss_weight, loss_weight))
    return (y, x_grad, gain_grad, router_grad, gate_grad, up_grad, down_grad, balance_loss, act_loss)
```

```python
import functools

import jax
import jax.numpy as jnp
from jax import lax
from jax.experimental import pallas as pl
from jax.experimental.pallas import tpu as pltpu
from jax.sharding import PartitionSpec as P

NORM_EPS = 1e-6
ACT_COEF = 1e-5
BALANCE_COEF = 1e-3
TILE = 256
HALF = 128
LANES = 128
CHUNKS = 2
VMEM_LIMIT = 62 * 1024 * 1024


def params(**kwargs):
    return pltpu.CompilerParams(vmem_limit_bytes=VMEM_LIMIT, **kwargs)


def row_block(height, width):
    return pl.BlockSpec((height, width), lambda t: (t, 0))


def dispatch_kernel(with_gate, count_ref, group_ref, lo_ref, steps_ref, pos_ref, prob_ref, tok_hbm, *rest):
    outs = rest[:2 if with_gate else 1]
    scratch = rest[len(outs):]
    specs = [row_block(HALF, out.shape[1]) for out in outs]

    def tile_body(*blocks):
        dispatch_tile(with_gate, group_ref, lo_ref, steps_ref, pos_ref, prob_ref, tok_hbm, *blocks, *scratch)

    pltpu.emit_pipeline(tile_body, grid=(count_ref[0] * (TILE // HALF),), out_specs=specs)(*outs)


def dispatch_tile(with_gate, group_ref, lo_ref, steps_ref, pos_ref, prob_ref, tok_hbm, *rest):
    if with_gate:
        x_ref, gate_ref, tok, acc, waited, sems = rest
    else:
        x_ref, tok, acc, waited, sems = rest
    tile = pl.program_id(0)
    tokens = tok.shape[0]
    blocks = tokens // TILE
    expert = group_ref[tile // (TILE // HALF)]
    lo = lo_ref[tile]
    steps = steps_ref[tile]
    row_id = lax.broadcasted_iota(jnp.int32, (HALF, LANES), 0) + tile * HALF

    def block_copy(index):
        rows = pl.ds(pl.multiple_of(index * TILE, TILE), TILE)
        return pltpu.make_async_copy(tok_hbm.at[rows, :], tok.at[rows, :], sems.at[index])

    @pl.when(tile == 0)
    def _():
        waited[0] = 0

        @pl.loop(0, blocks)
        def _(index):
            block_copy(index).start()

    def await_tokens(stop_chunk):
        need = (stop_chunk * LANES + TILE - 1) // TILE

        @pl.loop(waited[0], need)
        def _(index):
            block_copy(index).wait()

        waited[0] = jnp.maximum(waited[0], need)

    def window(start, count, first=None):
        hot, gate = [], jnp.zeros((HALF, LANES), jnp.float32)
        for q in range(count):
            match = pos_ref[expert, pl.ds(start + q, 1), :] == row_id
            if first is not None:
                match = jnp.logical_and(match, jnp.broadcast_to(start + q >= first, match.shape))
            hot.append(jnp.where(match, 1.0, 0.0).astype(jnp.bfloat16))
            if with_gate:
                gate = gate + jnp.where(match, prob_ref[expert, pl.ds(start + q, 1), :], 0.0)
        rows = tok[pl.ds(pl.multiple_of(start * LANES, LANES), count * LANES), :]
        return jnp.dot(jnp.concatenate(hot, axis=1), rows, preferred_element_type=jnp.float32), gate

    def put_gate(gate):
        if with_gate:
            gate_ref[...] = jnp.broadcast_to(jnp.sum(gate, axis=1, keepdims=True), (HALF, LANES))

    @pl.when(steps == 0)
    def _():
        x_ref[...] = jnp.zeros_like(x_ref)
        put_gate(jnp.zeros((HALF, LANES), jnp.float32))

    for k in range(1, 5):
        @pl.when(steps == k)
        def _(k=k):
            start = jnp.minimum(lo, tokens // LANES - 2 * k)
            await_tokens(start + 2 * k)
            out, gate = window(start, 2 * k)
            x_ref[...] = out.astype(x_ref.dtype)
            put_gate(gate)

    @pl.when(steps > 4)
    def _():
        acc[...] = jnp.zeros_like(acc)
        if with_gate:
            gate_ref[...] = jnp.zeros_like(gate_ref)

        @pl.loop(0, (steps + 3) // 4)
        def _(index):
            first = lo + 8 * index
            start = jnp.minimum(first, tokens // LANES - 8)
            await_tokens(start + 8)
            out, gate = window(start, 8, first)
            acc[...] += out
            if with_gate:
                gate_ref[...] += gate

        x_ref[...] = acc[...].astype(x_ref.dtype)
        if with_gate:
            put_gate(gate_ref[...])

    @pl.when(tile == pl.num_programs(0) - 1)
    def _():
        await_tokens(tokens // LANES)


def dispatch(meta, pos, prob, tok, rows_max, with_gate):
    tokens, dim = tok.shape
    any_spec = pl.BlockSpec(memory_space=pl.ANY)
    whole = pl.BlockSpec(memory_space=pltpu.VMEM)
    out_shape = [jax.ShapeDtypeStruct((rows_max, dim), jnp.bfloat16)]
    if with_gate:
        out_shape.append(jax.ShapeDtypeStruct((rows_max, LANES), jnp.float32))
    return pl.pallas_call(
        functools.partial(dispatch_kernel, with_gate),
        grid_spec=pltpu.PrefetchScalarGridSpec(
            num_scalar_prefetch=4,
            in_specs=[whole, whole, any_spec],
            out_specs=[any_spec] * len(out_shape),
            scratch_shapes=[
                pltpu.VMEM((tokens, dim), jnp.bfloat16),
                pltpu.VMEM((HALF, dim), jnp.float32),
                pltpu.SMEM((1,), jnp.int32),
                pltpu.SemaphoreType.DMA((tokens // TILE,)),
            ],
        ),
        out_shape=out_shape,
        compiler_params=params(),
        cost_estimate=pl.CostEstimate(flops=22 * 10**9, bytes_accessed=45 * 10**6, transcendentals=0),
        name="dispatch",
    )(meta["count"], meta["group"], meta["lo"], meta["steps"], pos, prob, tok)


def combine_kernel(with_gate, local_experts, start_ref, first_ref, over_ref, count_ref, pos_ref, rows_hbm, *rest):
    if with_gate:
        gate_hbm, out_ref, gout_ref, rows, gates, waited, sems = rest
    else:
        out_ref, rows, waited, sems = rest
    tile = pl.program_id(0)
    tiles = pl.num_programs(0)
    row_iota = lax.broadcasted_iota(jnp.int32, (HALF, LANES), 0)
    total_rows = count_ref[0] * TILE

    def block_copies(index):
        at = pl.ds(pl.multiple_of(index * TILE, TILE), TILE)
        copies = [pltpu.make_async_copy(rows_hbm.at[at, :], rows.at[at, :], sems.at[0, index])]
        if with_gate:
            copies.append(pltpu.make_async_copy(gate_hbm.at[at, :], gates.at[at, :], sems.at[1, index]))
        return copies

    @pl.when(tile == 0)
    def _():
        for e in range(local_experts):
            waited[e] = first_ref[e]

        @pl.loop(0, count_ref[0])
        def _(index):
            for copy in block_copies(index):
                copy.start()

    starts = []
    for e in range(local_experts):
        starts.append(pl.multiple_of(start_ref[e * tiles + tile], 16))

    over = over_ref[tile]
    for e in range(local_experts):
        stop = first_ref[e + 1]
        need = jnp.minimum((starts[e] + HALF + over * HALF + TILE - 1) // TILE, stop)

        @pl.loop(waited[e], need)
        def _(index):
            for copy in block_copies(index):
                copy.wait()

        waited[e] = jnp.maximum(waited[e], need)

    def window(second):
        hot, data, gdata = [], [], []
        for e in range(local_experts):
            if second:
                begin = starts[e] + HALF
                at = pl.multiple_of(jnp.minimum(begin, total_rows - HALF), 16)
            else:
                begin = at = starts[e]
            row = row_iota + at
            match = pos_ref[e, pl.ds(tile, 1), :] == row
            if second:
                match = jnp.logical_and(match, row >= begin)
            hot.append(jnp.where(match, 1.0, 0.0).astype(jnp.bfloat16))
            data.append(rows[pl.ds(at, HALF), :])
            if with_gate:
                gdata.append(gates[pl.ds(at, HALF), :])
        hot = jnp.concatenate(hot, axis=0)
        dims = (((0,), (0,)), ((), ()))
        out = lax.dot_general(hot, jnp.concatenate(data, axis=0), dims, preferred_element_type=jnp.float32)
        if not with_gate:
            return out, None
        exact = jnp.concatenate(gdata, axis=0)
        high = exact.astype(jnp.bfloat16)
        low = (exact - high.astype(jnp.float32)).astype(jnp.bfloat16)
        pair = lax.dot_general(hot, jnp.concatenate([high, low], axis=1), dims, preferred_element_type=jnp.float32)
        return out, pair[:, :LANES] + pair[:, LANES:]

    @pl.when(over == 0)
    def _():
        out, gate = window(False)
        out_ref[...] = out.astype(out_ref.dtype)
        if with_gate:
            gout_ref[...] = gate

    @pl.when(over != 0)
    def _():
        out, gate = window(False)
        out2, gate2 = window(True)
        out_ref[...] = (out + out2).astype(out_ref.dtype)
        if with_gate:
            gout_ref[...] = gate + gate2

    @pl.when(tile == tiles - 1)
    def _():
        for e in range(local_experts):
            @pl.loop(waited[e], first_ref[e + 1])
            def _(index):
                for copy in block_copies(index):
                    copy.wait()


def combine(meta, pos, rows, tokens, gate_rows=None):
    rows_max, dim = rows.shape
    local_experts = pos.shape[0]
    with_gate = gate_rows is not None
    any_spec = pl.BlockSpec(memory_space=pl.ANY)
    out_shape = [jax.ShapeDtypeStruct((tokens, dim), jnp.bfloat16)]
    out_specs = [pl.BlockSpec((HALF, dim), lambda t, *_: (t, 0))]
    scratch = [pltpu.VMEM((rows_max, dim), jnp.bfloat16)]
    if with_gate:
        out_shape.append(jax.ShapeDtypeStruct((tokens, LANES), jnp.float32))
        out_specs.append(pl.BlockSpec((HALF, LANES), lambda t, *_: (t, 0)))
        scratch.append(pltpu.VMEM((rows_max, LANES), jnp.float32))
    operands = (rows, gate_rows) if with_gate else (rows,)
    return pl.pallas_call(
        functools.partial(combine_kernel, with_gate, local_experts),
        grid_spec=pltpu.PrefetchScalarGridSpec(
            num_scalar_prefetch=4,
            grid=(tokens // HALF,),
            in_specs=[pl.BlockSpec(pos.shape, lambda t, *_: (0, 0, 0))] + [any_spec] * len(operands),
            out_specs=out_specs,
            scratch_shapes=scratch + [
                pltpu.SMEM((local_experts,), jnp.int32),
                pltpu.SemaphoreType.DMA((2, rows_max // TILE)),
            ],
        ),
        out_shape=out_shape,
        compiler_params=params(),
        cost_estimate=pl.CostEstimate(flops=11 * 10**9, bytes_accessed=40 * 10**6, transcendentals=0),
        name="combine",
    )(meta["start"], meta["first"], meta["over"], meta["count"], pos, *operands)


def weight_stream(group_ref, wg_hbm, wu_hbm, wd_hbm, wide, down, sems):
    tile = pl.program_id(0)
    experts = wg_hbm.shape[0]
    ffn = wg_hbm.shape[2]
    expert = group_ref[tile]
    slot = lax.rem(expert, 2)

    def copies(e, s):
        return (
            pltpu.make_async_copy(wg_hbm.at[e], wide.at[s, :, pl.ds(0, ffn)], sems.at[s, 0]),
            pltpu.make_async_copy(wu_hbm.at[e], wide.at[s, :, pl.ds(ffn, ffn)], sems.at[s, 1]),
            pltpu.make_async_copy(wd_hbm.at[e], down.at[s], sems.at[s, 2]),
        )

    @pl.when(tile == 0)
    def _():
        for copy in copies(0, 0):
            copy.start()

    fresh = jnp.logical_or(tile == 0, expert != group_ref[jnp.maximum(tile - 1, 0)])

    @pl.when(fresh)
    def _():
        @pl.when(expert + 1 < experts)
        def _():
            for copy in copies(expert + 1, 1 - slot):
                copy.start()

        for copy in copies(expert, slot):
            copy.wait()

    return slot


def forward_kernel(count_ref, group_ref, x_hbm, gate_hbm, wg_hbm, wu_hbm, wd_hbm, ab_hbm, h_hbm, out_hbm, wide, down, sems):
    def tile_body(x_ref, gate_ref, *outs):
        forward_tile(group_ref, x_ref, gate_ref, wg_hbm, wu_hbm, wd_hbm, *outs, wide, down, sems)

    piped_in, piped_out = (x_hbm, gate_hbm), (ab_hbm, h_hbm, out_hbm)
    pipeline = pltpu.emit_pipeline(
        tile_body, grid=(count_ref[0],),
        in_specs=[row_block(TILE, ref.shape[1]) for ref in piped_in],
        out_specs=[row_block(TILE, ref.shape[1]) for ref in piped_out],
    )
    pipeline(*piped_in, *piped_out)


def forward_tile(group_ref, x_ref, gate_ref, wg_hbm, wu_hbm, wd_hbm, ab_ref, h_ref, out_ref, wide, down, sems):
    slot = weight_stream(group_ref, wg_hbm, wu_hbm, wd_hbm, wide, down, sems)
    ffn = wg_hbm.shape[2]
    x = x_ref[...]
    for j in range(ffn // LANES):
        cols = slice(j * LANES, (j + 1) * LANES)
        ucols = slice(ffn + j * LANES, ffn + (j + 1) * LANES)
        weights = jnp.concatenate([wide[slot, :, cols], wide[slot, :, ucols]], axis=1)
        both = jnp.dot(x, weights, preferred_element_type=jnp.float32)
        a, b = both[:, :LANES], both[:, LANES:]
        ab_ref[:, cols] = a
        ab_ref[:, ucols] = b
        h_ref[:, cols] = (a * jax.nn.sigmoid(a) * b).astype(h_ref.dtype)
    out = jnp.dot(h_ref[...], down[slot], preferred_element_type=jnp.float32)
    gate = gate_ref[...]
    for j in range(out.shape[1] // LANES):
        cols = slice(j * LANES, (j + 1) * LANES)
        out_ref[:, cols] = (out[:, cols] * gate).astype(out_ref.dtype)


def backward_kernel(count_ref, group_ref, base_ref, m_hbm, ab_hbm, h_hbm, gate_hbm, wg_hbm, wu_hbm, wd_hbm, *rest):
    piped_in, piped_out, weights = (m_hbm, ab_hbm, h_hbm, gate_hbm), rest[:4], (wg_hbm, wu_hbm, wd_hbm)

    def tile_body(*blocks):
        backward_tile(group_ref, base_ref, *blocks[:4], *weights, *blocks[4:], *rest[4:])

    pipeline = pltpu.emit_pipeline(
        tile_body, grid=(count_ref[0],),
        in_specs=[row_block(TILE, ref.shape[1]) for ref in piped_in],
        out_specs=[row_block(TILE, ref.shape[1]) for ref in piped_out],
    )
    pipeline(*piped_in, *piped_out)


def backward_tile(group_ref, base_ref, m_ref, ab_ref, h_ref, gate_ref, wg_hbm, wu_hbm, wd_hbm, d_ref, in_ref, mg_ref, dgate_ref, wide, down, sems):
    slot = weight_stream(group_ref, wg_hbm, wu_hbm, wd_hbm, wide, down, sems)
    ffn = wg_hbm.shape[2]
    trans = (((1,), (1,)), ((), ()))
    m = m_ref[...]
    gate = gate_ref[...]
    dgate = jnp.zeros(gate.shape, jnp.float32)
    for c in range(0, ffn, 2 * LANES):
        width = min(2 * LANES, ffn - c)
        raw = lax.dot_general(m, down[slot, c:c + width, :], trans, preferred_element_type=jnp.float32)
        for k in range(width // LANES):
            lo = c + k * LANES
            cols = slice(lo, lo + LANES)
            ucols = slice(ffn + lo, ffn + lo + LANES)
            g = raw[:, k * LANES:(k + 1) * LANES]
            a, b = ab_ref[:, cols], ab_ref[:, ucols]
            sig = jax.nn.sigmoid(a)
            hidden_grad = g * gate
            d_ref[:, cols] = (hidden_grad * b * sig * (1.0 + a * (1.0 - sig))).astype(d_ref.dtype)
            d_ref[:, ucols] = (hidden_grad * (a * sig)).astype(d_ref.dtype)
            dgate = dgate + g * h_ref[:, cols].astype(jnp.float32)
    in_ref[...] = lax.dot_general(d_ref[...], wide[slot], trans, preferred_element_type=jnp.float32).astype(in_ref.dtype)
    for j in range(m.shape[1] // LANES):
        cols = slice(j * LANES, (j + 1) * LANES)
        mg_ref[:, cols] = (m[:, cols].astype(jnp.float32) * gate).astype(mg_ref.dtype)
    lane = lax.broadcasted_iota(jnp.int32, gate.shape, 1)
    mine = base_ref[0] + group_ref[pl.program_id(0)]
    dgate_ref[...] = jnp.where(lane == mine, jnp.sum(dgate, axis=1, keepdims=True), 0.0)


def weight_scratch(wg):
    _, dim, ffn = wg.shape
    return [
        pltpu.VMEM((2, dim, 2 * ffn), wg.dtype),
        pltpu.VMEM((2, ffn, dim), wg.dtype),
        pltpu.SemaphoreType.DMA((2, 3)),
    ]


def forward(meta, x_rows, gate_rows, wg, wu, wd):
    rows_max, dim = x_rows.shape
    ffn = wg.shape[2]
    any_spec = pl.BlockSpec(memory_space=pl.ANY)
    return pl.pallas_call(
        forward_kernel,
        grid_spec=pltpu.PrefetchScalarGridSpec(
            num_scalar_prefetch=2,
            in_specs=[any_spec] * 5,
            out_specs=[any_spec] * 3,
            scratch_shapes=weight_scratch(wg),
        ),
        out_shape=[
            jax.ShapeDtypeStruct((rows_max, 2 * ffn), jnp.float32),
            jax.ShapeDtypeStruct((rows_max, ffn), jnp.bfloat16),
            jax.ShapeDtypeStruct((rows_max, dim), jnp.bfloat16),
        ],
        compiler_params=params(),
        cost_estimate=pl.CostEstimate(flops=95 * 10**9, bytes_accessed=190 * 10**6, transcendentals=0),
        name="forward",
    )(meta["count"], meta["group"], x_rows, gate_rows, wg, wu, wd)


def backward(meta, base, m_rows, ab, hidden, gate_rows, wg, wu, wd):
    rows_max, dim = m_rows.shape
    ffn = wg.shape[2]
    any_spec = pl.BlockSpec(memory_space=pl.ANY)
    return pl.pallas_call(
        backward_kernel,
        grid_spec=pltpu.PrefetchScalarGridSpec(
            num_scalar_prefetch=3,
            in_specs=[any_spec] * 7,
            out_specs=[any_spec] * 4,
            scratch_shapes=weight_scratch(wg),
        ),
        out_shape=[
            jax.ShapeDtypeStruct((rows_max, 2 * ffn), jnp.bfloat16),
            jax.ShapeDtypeStruct((rows_max, dim), jnp.bfloat16),
            jax.ShapeDtypeStruct((rows_max, dim), jnp.bfloat16),
            jax.ShapeDtypeStruct((rows_max, LANES), jnp.float32),
        ],
        compiler_params=params(),
        cost_estimate=pl.CostEstimate(flops=95 * 10**9, bytes_accessed=220 * 10**6, transcendentals=0),
        name="backward",
    )(meta["count"], meta["group"], base, m_rows, ab, hidden, gate_rows, wg, wu, wd)


def weight_grad_kernel(tiles_max, outs, begin_ref, src0_ref, src1_ref, pair_ref, la_hbm, lb_hbm, ra_hbm, rb_hbm, *rest):
    out_refs, (lhs, rhs, lhs_t, acc, sems) = rest[:outs], rest[outs:]
    expert = pl.program_id(0)
    experts = pl.num_programs(0)
    begin, stop, steps = begin_ref[expert], begin_ref[expert + 1], begin_ref[experts]

    def copies(chunk, row, s, half):
        src_l, src_r = ((la_hbm, ra_hbm), (lb_hbm, rb_hbm))[chunk]
        at = pl.ds(pl.multiple_of(row, TILE), TILE)
        into = pl.ds(half * TILE, TILE)
        return (
            pltpu.make_async_copy(src_l.at[at, :], lhs.at[s, into, :], sems.at[s, half, 0]),
            pltpu.make_async_copy(src_r.at[at, :], rhs.at[s, into, :], sems.at[s, half, 1]),
        )

    def start_half(src, s, half):
        @pl.when(src < tiles_max)
        def _():
            for copy in copies(0, src * TILE, s, half):
                copy.start()

        @pl.when(src >= tiles_max)
        def _():
            for copy in copies(1, (src - tiles_max) * TILE, s, half):
                copy.start()

    def start(index, s):
        start_half(src0_ref[index], s, 0)

        @pl.when(pair_ref[index] != 0)
        def _():
            start_half(src1_ref[index], s, 1)

    @pl.when(expert == 0)
    def _():
        start(0, 0)

    def accumulate(slot, fresh, depth):
        lhs_t[:, :depth] = jnp.transpose(lhs[slot, :depth, :], (1, 0))
        block = 2 * LANES
        for c in range(0, acc.shape[1], block):
            part = jnp.dot(lhs_t[:, :depth], rhs[slot, :depth, c:c + block], preferred_element_type=jnp.float32)
            acc[:, c:c + block] = jnp.where(fresh, 0.0, acc[:, c:c + block]) + part

    @pl.loop(begin, stop)
    def _(step):
        slot = lax.rem(step, 2)

        @pl.when(step + 1 < steps)
        def _():
            start(step + 1, 1 - slot)

        fresh = step == begin
        pair = pair_ref[step] != 0
        for copy in copies(0, 0, slot, 0):
            copy.wait()

        @pl.when(pair)
        def _():
            for copy in copies(0, 0, slot, 1):
                copy.wait()
            accumulate(slot, fresh, 2 * TILE)

        @pl.when(jnp.logical_not(pair))
        def _():
            accumulate(slot, fresh, TILE)

    width = acc.shape[1] // outs
    for i in range(outs):
        out_refs[i][...] = acc[:, i * width:(i + 1) * width].astype(out_refs[i].dtype)


def weight_grad(meta, lhs, rhs, experts, outs, tiles_max):
    rows_max, left = lhs[0].shape
    right = rhs[0].shape[1]
    width = right // outs
    any_spec = pl.BlockSpec(memory_space=pl.ANY)
    return pl.pallas_call(
        functools.partial(weight_grad_kernel, tiles_max, outs),
        grid_spec=pltpu.PrefetchScalarGridSpec(
            num_scalar_prefetch=4,
            grid=(experts,),
            in_specs=[any_spec] * 4,
            out_specs=[pl.BlockSpec((pl.squeezed, left, width), lambda e, *_: (e, 0, 0))] * outs,
            scratch_shapes=[
                pltpu.VMEM((2, 2 * TILE, left), jnp.bfloat16),
                pltpu.VMEM((2, 2 * TILE, right), jnp.bfloat16),
                pltpu.VMEM((left, 2 * TILE), jnp.bfloat16),
                pltpu.VMEM((left, right), jnp.float32),
                pltpu.SemaphoreType.DMA((2, 2, 2)),
            ],
        ),
        out_shape=[jax.ShapeDtypeStruct((experts, left, width), jnp.bfloat16)] * outs,
        compiler_params=params(),
        cost_estimate=pl.CostEstimate(flops=2 * 10000 * left * right, bytes_accessed=100 * 10**6, transcendentals=0),
        name="weight_grad",
    )(meta["begin"], meta["src0"], meta["src1"], meta["pair"], *lhs, *rhs)


def below(size, strict):
    i = lax.broadcasted_iota(jnp.int32, (size, size), 0)
    j = lax.broadcasted_iota(jnp.int32, (size, size), 1)
    return (i < j if strict else i <= j).astype(jnp.float32)


def running(values):
    size = values.shape[0]
    i = lax.broadcasted_iota(jnp.int32, (size, size), 0)
    j = lax.broadcasted_iota(jnp.int32, (size, size), 1)
    return jnp.sum(jnp.where(i <= j, values[:, None], 0), axis=0)


def routing(hot, tiles_max):
    experts, tokens = hot.shape
    spans = tokens // LANES
    hot = hot.reshape(experts, spans, LANES)
    within = jnp.einsum("esi,ij->esj", hot, below(LANES, False), preferred_element_type=jnp.float32)
    span_count = jnp.sum(hot, axis=-1)
    before = jnp.einsum("ei,ij->ej", span_count, below(spans, True), preferred_element_type=jnp.float32)
    total = jnp.sum(span_count, axis=-1).astype(jnp.int32)
    tiles = jnp.maximum((total + TILE - 1) // TILE, 1)
    tile_stop = running(tiles)
    tile_start = tile_stop - tiles
    base = tile_start * TILE
    span_first = base[:, None] + before.astype(jnp.int32)
    span_stop = span_first + span_count.astype(jnp.int32)
    pos = jnp.where(hot > 0, span_first[:, :, None] + within.astype(jnp.int32) - 1, -1)
    count = tile_stop[experts - 1]

    tile_iota = jnp.arange(tiles_max, dtype=jnp.int32)
    group = jnp.sum((tile_iota[:, None] >= tile_stop[None, :experts - 1]).astype(jnp.int32), axis=1)
    halves = tiles_max * (TILE // HALF)
    half_iota = jnp.arange(halves, dtype=jnp.int32)
    half_group = jnp.sum((half_iota[:, None] // (TILE // HALF) >= tile_stop[None, :experts - 1]).astype(jnp.int32), axis=1)
    pick = half_group[:, None] == jnp.arange(experts, dtype=jnp.int32)[None, :]
    stops = jnp.sum(jnp.where(pick[:, :, None], span_stop[None], 0), axis=1)
    row0 = half_iota[:, None] * HALF
    lo = jnp.sum((stops <= row0).astype(jnp.int32), axis=1)
    hi = jnp.minimum(jnp.sum((stops < row0 + HALF).astype(jnp.int32), axis=1), spans - 1)
    steps = (hi - lo + 2) // 2
    start = jnp.minimum(span_first // 16 * 16, count * TILE - HALF)
    over = jnp.any(span_stop - start > HALF, axis=0).astype(jnp.int32)
    first = jnp.concatenate([jnp.zeros((1,), jnp.int32), tile_stop])
    return pos, tile_start, tiles, {
        "group": group, "lo": lo, "steps": steps,
        "start": start.reshape(-1), "first": first, "over": over, "count": count.reshape(1),
    }


def pair_tables(starts, tiles, tiles_max):
    experts = tiles[0].shape[0]
    both = tiles[0] + tiles[1]
    stop = running((both + 1) // 2)
    begin = stop - (both + 1) // 2
    step = jnp.arange(tiles_max + experts, dtype=jnp.int32)
    expert = jnp.sum((step[:, None] >= stop[None, :experts - 1]).astype(jnp.int32), axis=1)
    pick = expert[:, None] == jnp.arange(experts, dtype=jnp.int32)[None, :]

    def of(table):
        return jnp.sum(jnp.where(pick, table[None, :], 0), axis=1)

    first = 2 * (step - of(begin))
    in_a = of(tiles[0])

    def source(index):
        return jnp.where(index < in_a, of(starts[0]) + index, tiles_max + of(starts[1]) + index - in_a)

    pair = (first + 1 < of(both)).astype(jnp.int32)
    return {
        "begin": jnp.concatenate([jnp.zeros((1,), jnp.int32), stop]), "src0": source(first),
        "src1": jnp.where(pair != 0, source(first + 1), 0), "pair": pair,
    }


def solution(mesh):
    tp_size = mesh.shape["tp"]
    ep_size = mesh.shape["ep"]
    dev_count = tp_size * ep_size
    rows_axes = ("ep", "tp")
    row_spec = P(rows_axes, None)
    wide_spec = P("ep", None, "tp")
    down_spec = P("ep", "tp", None)

    def body(x, y_grad, expert_ids, norm_gain, w_router, w_gate, w_up, w_down):
        tokens, model_dim = x.shape
        top_k = expert_ids.shape[1]
        num_experts = w_router.shape[1]
        local_experts = w_gate.shape[0]
        total_tokens = tokens * dev_count
        part = tokens // CHUNKS
        chunk_tokens = part * dev_count
        tiles_max = chunk_tokens * top_k // TILE + local_experts
        rows_max = tiles_max * TILE
        my_base = lax.axis_index("ep") * local_experts

        x_float = x.astype(jnp.float32)
        inv_rms = lax.rsqrt(jnp.mean(x_float * x_float, axis=-1, keepdims=True) + NORM_EPS)
        unit = x_float * inv_rms
        gain = norm_gain.astype(jnp.float32)
        x_norm = (unit * gain).astype(jnp.bfloat16)

        def gather(rows):
            return lax.all_gather(rows, rows_axes, axis=0, tiled=True)

        def scatter(rows):
            return lax.psum_scatter(rows, rows_axes, scatter_dimension=0, tiled=True)

        def of_chunk(rows, c):
            return rows[c * part:(c + 1) * part]

        tok = [gather(of_chunk(x_norm, c)) for c in range(CHUNKS)]

        route_prob = jax.nn.softmax(jnp.dot(x_norm, w_router, preferred_element_type=jnp.float32), axis=-1)
        expert_range = jnp.arange(num_experts, dtype=jnp.int32)
        choice = jnp.sum((expert_ids[:, :, None] == expert_range[None, None, :]).astype(jnp.float32), axis=1)
        small = lax.all_gather(jnp.concatenate([choice, route_prob], axis=1).T, rows_axes, axis=0, tiled=False)
        all_choice, all_prob = small[:, :num_experts], small[:, num_experts:]
        counts = jnp.sum(all_choice, axis=(0, 2))
        balance_scale = BALANCE_COEF * num_experts / (total_tokens * total_tokens * top_k)
        balance_loss = balance_scale * jnp.sum(counts * jnp.sum(all_prob, axis=(0, 2)))

        def mine(values, c):
            own = lax.dynamic_slice_in_dim(values, my_base, local_experts, axis=1)
            own = own[:, :, c * part:(c + 1) * part]
            return own.transpose(1, 0, 2).reshape(local_experts, chunk_tokens)

        pos, prob, meta, starts, tiles = [], [], [], [], []
        for c in range(CHUNKS):
            p, s, t, m = routing(mine(all_choice, c), tiles_max)
            pos.append(p)
            starts.append(s)
            tiles.append(t)
            meta.append(m)
            prob.append(mine(all_prob, c).reshape(p.shape))

        x_rows, gate_rows, pre, hidden, moe_out, m_tok = [], [], [], [], [], []
        grad_scale = 2.0 * ACT_COEF / (total_tokens * model_dim)

        def out_cotangent(c):
            moe_grad = of_chunk(y_grad, c).astype(jnp.float32) + grad_scale * moe_out[c]
            return moe_grad.astype(jnp.bfloat16)

        raw_out = []
        for c in range(CHUNKS):
            rows, gates = dispatch(meta[c], pos[c], prob[c], tok[c], rows_max, True)
            ab, h, out_rows = forward(meta[c], rows, gates, w_gate, w_up, w_down)
            if c > 0:
                out_rows, raw_out[c - 1] = lax.optimization_barrier((out_rows, raw_out[c - 1]))
                moe_out.append(raw_out[c - 1].astype(jnp.float32))
                m_tok.append(gather(out_cotangent(c - 1)))
            (partial,) = combine(meta[c], pos[c], out_rows, chunk_tokens)
            if c > 0:
                partial, m_tok[c - 1] = lax.optimization_barrier((partial, m_tok[c - 1]))
            raw_out.append(scatter(partial))
            x_rows.append(rows)
            gate_rows.append(gates)
            pre.append(ab)
            hidden.append(h)

        base = jnp.reshape(my_base, (1,)).astype(jnp.int32)
        d_rows, mg_rows, returned, gate_part = [], [], [], []
        for c in range(CHUNKS):
            (m_rows,) = dispatch(meta[c], pos[c], prob[c], m_tok[c], rows_max, False)
            d, in_rows, mg, dgate = backward(meta[c], base, m_rows, pre[c], hidden[c], gate_rows[c], w_gate, w_up, w_down)
            if c == 0:
                in_rows, raw_out[-1] = lax.optimization_barrier((in_rows, raw_out[-1]))
                moe_out.append(raw_out[-1].astype(jnp.float32))
                m_tok.append(gather(out_cotangent(CHUNKS - 1)))
            partial, gate_tok = combine(meta[c], pos[c], in_rows, chunk_tokens, dgate)
            if c == 0:
                partial, m_tok[-1] = lax.optimization_barrier((partial, m_tok[-1]))
            returned.append(scatter(partial))
            gate_part.append(gate_tok[:, :num_experts])
            d_rows.append(d)
            mg_rows.append(mg)

        steps = pair_tables(starts, tiles, tiles_max)
        gate_grad, up_grad = weight_grad(steps, x_rows, d_rows, local_experts, 2, tiles_max)
        (down_grad,) = weight_grad(steps, hidden, mg_rows, local_experts, 1, tiles_max)

        moe_all = jnp.concatenate(moe_out, axis=0)
        y = (x_float + moe_all).astype(jnp.bfloat16)
        gate_sum = scatter(jnp.concatenate(gate_part, axis=1))
        gate_weight_grad = jnp.concatenate([gate_sum[:, :num_experts], gate_sum[:, num_experts:]], axis=0)
        prob_grad = gate_weight_grad + balance_scale * counts[None, :]
        logit_grad = (route_prob * (prob_grad - jnp.sum(route_prob * prob_grad, axis=-1, keepdims=True))).astype(jnp.bfloat16)
        x_norm_grad = jnp.concatenate(returned, axis=0).astype(jnp.float32)
        x_norm_grad = x_norm_grad + jnp.einsum("se,de->sd", logit_grad, w_router, preferred_element_type=jnp.float32)
        unit_grad = x_norm_grad * gain
        x_grad = y_grad.astype(jnp.float32) + inv_rms * (unit_grad - unit * jnp.mean(unit_grad * unit, axis=-1, keepdims=True))
        gain_sum, router_sum, act_sum = lax.psum(
            (
                jnp.sum(x_norm_grad * unit, axis=0),
                jnp.einsum("sd,se->de", x_norm, logit_grad, preferred_element_type=jnp.float32),
                jnp.sum(moe_all * moe_all),
            ),
            ("tp", "ep"),
        )
        act_loss = ACT_COEF * act_sum / (total_tokens * model_dim)
        return (y, x_grad.astype(jnp.bfloat16), gain_sum.astype(jnp.bfloat16), router_sum.astype(jnp.bfloat16), gate_grad, up_grad, down_grad, balance_loss, act_loss)

    return jax.shard_map(body, mesh=mesh, in_specs=(row_spec, row_spec, row_spec, P(), P(), wide_spec, wide_spec, down_spec), out_specs=(row_spec, row_spec, P(), P(), wide_spec, wide_spec, down_spec, P(), P()), check_vma=False)
```

```python
import functools

import jax
import jax.numpy as jnp
from jax import lax
from jax.experimental import pallas as pl
from jax.experimental.pallas import tpu as pltpu
from jax.sharding import PartitionSpec as P

NORM_EPS = 1e-6
ACT_COEF = 1e-5
BALANCE_COEF = 1e-3
TILE = 256
LANES = 128
GROUP = 4
CHUNKS = 4
WINDOWS = (1, 2, 3, 4)
VMEM_LIMIT = 62 * 1024 * 1024


def call(kernel, name, table, operands, in_specs, out_shape, out_specs, scratch, cost, grid=()):
    return pl.pallas_call(
        kernel,
        grid_spec=pltpu.PrefetchScalarGridSpec(
            num_scalar_prefetch=1, grid=grid, in_specs=in_specs, out_specs=out_specs, scratch_shapes=scratch
        ),
        out_shape=out_shape,
        compiler_params=pltpu.CompilerParams(vmem_limit_bytes=VMEM_LIMIT),
        cost_estimate=pl.CostEstimate(flops=cost[0], bytes_accessed=cost[1], transcendentals=0),
        name=name,
    )(table, *operands)


ANY = pl.BlockSpec(memory_space=pl.ANY)
WHOLE = pl.BlockSpec(memory_space=pltpu.VMEM)


def row_block(width):
    return pl.BlockSpec((TILE, width), lambda t: (t, 0))


def dispatch_phase(at, chunk, table_ref, pos_ref, prob_ref, token_refs, outs):
    half_tokens, dim = token_refs[0].shape
    if len(token_refs) == 1:
        half_tokens //= 2
    own_hbm = token_refs[0]
    blocks = half_tokens // TILE
    spans = 2 * half_tokens // LANES

    def run(tok, waited, sems):
        def block_copy(index):
            part, offset = index // blocks, (index % blocks) * TILE
            if len(token_refs) == 1:
                source, offset = own_hbm, pl.multiple_of(offset + lax.rem(part + table_ref[at["ep"]], 2) * half_tokens, TILE)
            else:
                source = token_refs[part]
            return pltpu.make_async_copy(source.at[pl.ds(offset, TILE), :], tok.at[pl.ds(index * TILE, TILE), :], sems.at[index])

        waited[0] = 0
        for index in range(2 * blocks):
            block_copy(index).start()

        def await_tokens(stop_span):
            need = (stop_span * LANES + TILE - 1) // TILE

            @pl.loop(waited[0], need)
            def _(index):
                pltpu.make_async_copy(
                    own_hbm.at[pl.ds(0, TILE), :], tok.at[pl.ds(pl.multiple_of(index * TILE, TILE), TILE), :], sems.at[index]
                ).wait()

            waited[0] = jnp.maximum(waited[0], need)

        def tile_body(x_ref, gate_ref=None):
            tile = pl.program_id(0)
            expert = table_ref[at["group"] + tile]
            width = table_ref[at["width"] + tile]

            def window(half, count, start):
                row_id = lax.broadcasted_iota(jnp.int32, (LANES, LANES), 0) + (tile * TILE + half * LANES)
                into = pl.ds(half * LANES if isinstance(half, int) else pl.multiple_of(half * LANES, LANES), LANES)
                hot, gate = [], jnp.zeros((LANES, LANES), jnp.float32)
                for q in range(count):
                    match = pos_ref[chunk, expert, pl.ds(start + q, 1), :] == row_id
                    hot.append(jnp.where(match, 1.0, 0.0).astype(jnp.bfloat16))
                    if gate_ref is not None:
                        gate = gate + jnp.where(match, prob_ref[chunk, expert, pl.ds(start + q, 1), :], 0.0)
                rows = tok[pl.ds(pl.multiple_of(start * LANES, LANES), count * LANES), :]
                out = jnp.dot(jnp.concatenate(hot, axis=1), rows, preferred_element_type=jnp.float32)
                x_ref[into, :] = out.astype(x_ref.dtype)
                if gate_ref is not None:
                    gate_ref[into, :] = jnp.broadcast_to(jnp.sum(gate, axis=1, keepdims=True), (LANES, LANES))

            @pl.when(width > WINDOWS[-1])
            def _():
                await_tokens(spans)

                @pl.loop(0, 2)
                def _(half):
                    window(half, spans, 0)

            for k in WINDOWS:
                @pl.when(width == k)
                def _(k=k):
                    starts = [jnp.minimum(table_ref[at["lo"] + 2 * tile + half], spans - 2 * k) for half in range(2)]
                    await_tokens(jnp.maximum(starts[0], starts[1]) + 2 * k)
                    for half in range(2):
                        window(half, 2 * k, starts[half])

        pltpu.emit_pipeline(
            tile_body, grid=(table_ref[at["count"]],), out_specs=[row_block(out.shape[1]) for out in outs]
        )(*outs)
        await_tokens(spans)

    pl.run_scoped(
        run,
        pltpu.VMEM((2 * half_tokens, dim), jnp.bfloat16),
        pltpu.SMEM((1,), jnp.int32),
        pltpu.SemaphoreType.DMA((2 * blocks,)),
    )


def combine_kernel(at, chunk, part, spans, experts, with_gate, add, table_ref, pos_ref, rows_hbm, *rest):
    rest = list(rest)
    gate_hbm = rest.pop(0) if with_gate else None
    recv_ref = rest.pop(0) if add else None
    out_ref = rest.pop(0)
    gout_ref = rest.pop(0) if with_gate else None
    rows = rest.pop(0)
    gates = rest.pop(0) if with_gate else None
    waited, sems = rest
    step = pl.program_id(0)
    steps = pl.num_programs(0)
    half = spans // 2
    row_iota = lax.broadcasted_iota(jnp.int32, (LANES, LANES), 0)
    over = table_ref[at["over"] + part * (half // GROUP) + step]

    def region_stop(e):
        return table_ref[at["first"] + e + 1]

    def start_of(e, span):
        return pl.multiple_of(table_ref[at["start"] + e * spans + span], 16)

    def block_stop(e, span, wide):
        return jnp.minimum((start_of(e, span) + LANES + wide * LANES + TILE - 1) // TILE, region_stop(e))

    def block_copies(index):
        into = pl.ds(pl.multiple_of(index * TILE, TILE), TILE)
        copies = [pltpu.make_async_copy(rows_hbm.at[into, :], rows.at[into, :], sems.at[0, index])]
        if with_gate:
            copies.append(pltpu.make_async_copy(gate_hbm.at[into, :], gates.at[into, :], sems.at[1, index]))
        return copies

    @pl.when(step == 0)
    def _():
        for e in range(experts):
            begin = start_of(e, part * half) // TILE
            waited[e] = begin

            @pl.loop(begin, block_stop(e, part * half + half - 1, 1))
            def _(index):
                for copy in block_copies(index):
                    copy.start()

    for e in range(experts):
        need = block_stop(e, part * half + (step + 1) * GROUP - 1, jnp.where(step == steps - 1, 1, over))

        @pl.loop(waited[e], need)
        def _(index):
            for copy in block_copies(index):
                copy.wait()

        waited[e] = jnp.maximum(waited[e], need)

    def window(q, second):
        span = part * half + step * GROUP + q
        hot, data, gdata = [], [], []
        for e in range(experts):
            begin = place = start_of(e, span)
            if second:
                begin = begin + LANES
                place = pl.multiple_of(jnp.minimum(begin, region_stop(e) * TILE - LANES), 16)
            row = row_iota + place
            match = pos_ref[chunk, e, pl.ds(span, 1), :] == row
            if second:
                match = jnp.logical_and(match, row >= begin)
            hot.append(jnp.where(match, 1.0, 0.0).astype(jnp.bfloat16))
            data.append(rows[pl.ds(place, LANES), :])
            if with_gate:
                gdata.append(gates[pl.ds(place, LANES), :])
        hot = jnp.concatenate(hot, axis=0)
        dims = (((0,), (0,)), ((), ()))
        out = lax.dot_general(hot, jnp.concatenate(data, axis=0), dims, preferred_element_type=jnp.float32)
        if not with_gate:
            return out, None
        exact = jnp.concatenate(gdata, axis=0)
        high = exact.astype(jnp.bfloat16)
        low = (exact - high.astype(jnp.float32)).astype(jnp.bfloat16)
        pair = lax.dot_general(hot, jnp.concatenate([high, low], axis=1), dims, preferred_element_type=jnp.float32)
        return out, pair[:, :LANES] + pair[:, LANES:]

    def put(q, wide):
        out, gate = window(q, False)
        if wide:
            out2, gate2 = window(q, True)
            out = out + out2
            gate = gate + gate2 if with_gate else None
        into = pl.ds(q * LANES if isinstance(q, int) else pl.multiple_of(q * LANES, LANES), LANES)
        if add:
            out = out + recv_ref[into, :].astype(jnp.float32)
        out_ref[into, :] = out.astype(out_ref.dtype)
        if with_gate:
            gout_ref[into, :] = gate

    @pl.when(over == 0)
    def _():
        for q in range(GROUP):
            put(q, False)

    @pl.when(over != 0)
    def _():
        @pl.loop(0, GROUP)
        def _(q):
            put(q, True)


def combine(layout, chunk, part, table, pos, rows, gate_rows=None, received=None):
    rows_max, dim = rows.shape
    _, experts, spans, _ = pos.shape
    tokens = spans * LANES // 2
    with_gate, add = gate_rows is not None, received is not None
    block = GROUP * LANES
    operands, in_specs = [pos, rows], [WHOLE, ANY]
    if with_gate:
        operands.append(gate_rows)
        in_specs.append(ANY)
    if add:
        operands.append(received)
        in_specs.append(pl.BlockSpec((block, dim), lambda t, *_: (t, 0)))
    out_shape = [jax.ShapeDtypeStruct((tokens, dim), jnp.bfloat16)]
    out_specs = [pl.BlockSpec((block, dim), lambda t, *_: (t, 0))]
    scratch = [pltpu.VMEM((rows_max, dim), jnp.bfloat16)]
    if with_gate:
        out_shape.append(jax.ShapeDtypeStruct((tokens, LANES), jnp.float32))
        out_specs.append(pl.BlockSpec((block, LANES), lambda t, *_: (t, 0)))
        scratch.append(pltpu.VMEM((rows_max, LANES), jnp.float32))
    scratch += [pltpu.SMEM((experts,), jnp.int32), pltpu.SemaphoreType.DMA((2, rows_max // TILE))]
    kernel = functools.partial(combine_kernel, layout[chunk], chunk, part, spans, experts, with_gate, add)
    return call(kernel, "combine", table, operands, in_specs, out_shape, out_specs, scratch, (3 * 10**9, 15 * 10**6), (tokens // block,))


def weight_copies(weights, wide, down, sems, e, s):
    wg_hbm, wu_hbm, wd_hbm = weights
    ffn = wg_hbm.shape[2]
    return (
        pltpu.make_async_copy(wg_hbm.at[e], wide.at[s, :, pl.ds(0, ffn)], sems.at[s, 0]),
        pltpu.make_async_copy(wu_hbm.at[e], wide.at[s, :, pl.ds(ffn, ffn)], sems.at[s, 1]),
        pltpu.make_async_copy(wd_hbm.at[e], down.at[s], sems.at[s, 2]),
    )


def weight_slot(at, table_ref, weights, scratch):
    tile = pl.program_id(0)
    experts = weights[0].shape[0]
    expert = table_ref[at["group"] + tile]
    slot = lax.rem(expert, 2)
    fresh = jnp.logical_or(tile == 0, expert != table_ref[at["group"] + jnp.maximum(tile - 1, 0)])

    @pl.when(fresh)
    def _():
        @pl.when(expert + 1 < experts)
        def _():
            for copy in weight_copies(weights, *scratch, expert + 1, 1 - slot):
                copy.start()

        for copy in weight_copies(weights, *scratch, expert, slot):
            copy.wait()

    return expert, slot


def forward_kernel(at, chunk, sources, table_ref, pos_ref, prob_ref, *rest):
    token_refs, weights = rest[:sources], rest[sources:sources + 3]
    x_hbm, gate_hbm, ab_hbm, h_hbm, out_hbm, *scratch = rest[sources + 3:]
    wide, down, _ = scratch
    ffn = weights[0].shape[2]
    for copy in weight_copies(weights, *scratch, 0, 0):
        copy.start()
    dispatch_phase(at, chunk, table_ref, pos_ref, prob_ref, token_refs, (x_hbm, gate_hbm))

    def tile_body(x_ref, gate_ref, ab_ref, h_ref, out_ref):
        _, slot = weight_slot(at, table_ref, weights, scratch)
        x = x_ref[...]
        for j in range(ffn // LANES):
            cols = slice(j * LANES, (j + 1) * LANES)
            ucols = slice(ffn + j * LANES, ffn + (j + 1) * LANES)
            both = jnp.dot(x, jnp.concatenate([wide[slot, :, cols], wide[slot, :, ucols]], axis=1), preferred_element_type=jnp.float32)
            a, b = both[:, :LANES], both[:, LANES:]
            ab_ref[:, cols] = a
            ab_ref[:, ucols] = b
            h_ref[:, cols] = (a * jax.nn.sigmoid(a) * b).astype(h_ref.dtype)
        out = jnp.dot(h_ref[...], down[slot], preferred_element_type=jnp.float32)
        gate = gate_ref[...]
        for j in range(out.shape[1] // LANES):
            cols = slice(j * LANES, (j + 1) * LANES)
            out_ref[:, cols] = (out[:, cols] * gate).astype(out_ref.dtype)

    piped_in, piped_out = (x_hbm, gate_hbm), (ab_hbm, h_hbm, out_hbm)
    pltpu.emit_pipeline(
        tile_body, grid=(table_ref[at["count"]],),
        in_specs=[row_block(ref.shape[1]) for ref in piped_in],
        out_specs=[row_block(ref.shape[1]) for ref in piped_out],
    )(*piped_in, *piped_out)


def backward_kernel(at, chunk, table_ref, pos_ref, own_hbm, other_hbm, ab_hbm, h_hbm, gate_hbm, wg_hbm, wu_hbm, wd_hbm, m_hbm, d_hbm, in_hbm, mg_hbm, dgate_hbm, *scratch):
    weights = (wg_hbm, wu_hbm, wd_hbm)
    wide, down, _ = scratch
    ffn = wg_hbm.shape[2]
    trans = (((1,), (1,)), ((), ()))
    for copy in weight_copies(weights, *scratch, 0, 0):
        copy.start()
    dispatch_phase(at, chunk, table_ref, pos_ref, None, (own_hbm, other_hbm), (m_hbm,))

    def tile_body(m_ref, ab_ref, h_ref, gate_ref, d_ref, in_ref, mg_ref, dgate_ref):
        expert, slot = weight_slot(at, table_ref, weights, scratch)
        m = m_ref[...]
        gate = gate_ref[...]
        dgate = jnp.zeros(gate.shape, jnp.float32)
        for c in range(0, ffn, 2 * LANES):
            width = min(2 * LANES, ffn - c)
            raw = lax.dot_general(m, down[slot, c:c + width, :], trans, preferred_element_type=jnp.float32)
            for k in range(width // LANES):
                lo = c + k * LANES
                cols = slice(lo, lo + LANES)
                ucols = slice(ffn + lo, ffn + lo + LANES)
                g = raw[:, k * LANES:(k + 1) * LANES]
                a, b = ab_ref[:, cols], ab_ref[:, ucols]
                sig = jax.nn.sigmoid(a)
                hidden_grad = g * gate
                d_ref[:, cols] = (hidden_grad * b * sig * (1.0 + a * (1.0 - sig))).astype(d_ref.dtype)
                d_ref[:, ucols] = (hidden_grad * (a * sig)).astype(d_ref.dtype)
                dgate = dgate + g * h_ref[:, cols].astype(jnp.float32)
        in_ref[...] = lax.dot_general(d_ref[...], wide[slot], trans, preferred_element_type=jnp.float32).astype(in_ref.dtype)
        for j in range(m.shape[1] // LANES):
            cols = slice(j * LANES, (j + 1) * LANES)
            mg_ref[:, cols] = (m[:, cols].astype(jnp.float32) * gate).astype(mg_ref.dtype)
        lane = lax.broadcasted_iota(jnp.int32, gate.shape, 1)
        dgate_ref[...] = jnp.where(lane == table_ref[at["ep"]] * weights[0].shape[0] + expert, jnp.sum(dgate, axis=1, keepdims=True), 0.0)

    piped_in, piped_out = (m_hbm, ab_hbm, h_hbm, gate_hbm), (d_hbm, in_hbm, mg_hbm, dgate_hbm)
    pltpu.emit_pipeline(
        tile_body, grid=(table_ref[at["count"]],),
        in_specs=[row_block(ref.shape[1]) for ref in piped_in],
        out_specs=[row_block(ref.shape[1]) for ref in piped_out],
    )(*piped_in, *piped_out)


def weight_scratch(wg):
    _, dim, ffn = wg.shape
    return [
        pltpu.VMEM((2, dim, 2 * ffn), wg.dtype),
        pltpu.VMEM((2, ffn, dim), wg.dtype),
        pltpu.SemaphoreType.DMA((2, 3)),
    ]


def shapes(rows_max, *kinds):
    return [jax.ShapeDtypeStruct((rows_max, width), dtype) for width, dtype in kinds]


def forward(layout, chunk, table, pos, prob, tokens, weights):
    _, dim, ffn = weights[0].shape
    kinds = ((dim, jnp.bfloat16), (LANES, jnp.float32), (2 * ffn, jnp.float32), (ffn, jnp.bfloat16), (dim, jnp.bfloat16))
    kernel = functools.partial(forward_kernel, layout[chunk], chunk, len(tokens))
    rows_max = layout["tiles_max"] * TILE
    return call(
        kernel, "forward", table, (pos, prob, *tokens, *weights), [WHOLE, WHOLE] + [ANY] * (len(tokens) + 3),
        shapes(rows_max, *kinds), [ANY] * 5, weight_scratch(weights[0]), (52 * 10**9, 110 * 10**6),
    )


def backward(layout, chunk, table, pos, own, other, ab, hidden, gates, weights):
    _, dim, ffn = weights[0].shape
    kinds = ((dim, jnp.bfloat16), (2 * ffn, jnp.bfloat16), (dim, jnp.bfloat16), (dim, jnp.bfloat16), (LANES, jnp.float32))
    kernel = functools.partial(backward_kernel, layout[chunk], chunk)
    rows_max = layout["tiles_max"] * TILE
    return call(
        kernel, "backward", table, (pos, own, other, ab, hidden, gates, *weights), [WHOLE] + [ANY] * 8,
        shapes(rows_max, *kinds), [ANY] * 5, weight_scratch(weights[0]), (52 * 10**9, 110 * 10**6),
    )


def weight_grad_kernel(at, tiles_max, outs, table_ref, *rest):
    lhs_hbm, rhs_hbm = rest[:CHUNKS], rest[CHUNKS:2 * CHUNKS]
    out_refs, (lhs, rhs, lhs_t, acc, sems) = rest[2 * CHUNKS:2 * CHUNKS + outs], rest[2 * CHUNKS + outs:]
    expert = pl.program_id(0)
    experts = pl.num_programs(0)
    begin, stop = table_ref[at["begin"] + expert], table_ref[at["begin"] + expert + 1]
    steps = table_ref[at["begin"] + experts]

    def copies(chunk, row, s, half):
        source = pl.ds(pl.multiple_of(row, TILE), TILE)
        into = pl.ds(half * TILE, TILE)
        return (
            pltpu.make_async_copy(lhs_hbm[chunk].at[source, :], lhs.at[s, into, :], sems.at[s, half, 0]),
            pltpu.make_async_copy(rhs_hbm[chunk].at[source, :], rhs.at[s, into, :], sems.at[s, half, 1]),
        )

    def start_half(src, s, half):
        for chunk in range(CHUNKS):
            @pl.when(jnp.logical_and(src >= chunk * tiles_max, src < (chunk + 1) * tiles_max))
            def _(chunk=chunk):
                for copy in copies(chunk, (src - chunk * tiles_max) * TILE, s, half):
                    copy.start()

    def start(index, s):
        for half in range(2):
            start_half(table_ref[at["src"] + 2 * index + half], s, half)

    @pl.when(expert == 0)
    def _():
        start(0, 0)

    def accumulate(slot, fresh, depth):
        lhs_t[:, :depth] = jnp.transpose(lhs[slot, :depth, :], (1, 0))
        block = 2 * LANES
        for c in range(0, acc.shape[1], block):
            part = jnp.dot(lhs_t[:, :depth], rhs[slot, :depth, c:c + block], preferred_element_type=jnp.float32)
            acc[:, c:c + block] = jnp.where(fresh, 0.0, acc[:, c:c + block]) + part

    @pl.loop(begin, stop)
    def _(step):
        slot = lax.rem(step, 2)

        @pl.when(step + 1 < steps)
        def _():
            start(step + 1, 1 - slot)

        fresh = step == begin
        pair = table_ref[at["src"] + 2 * step + 1] >= 0
        for copy in copies(0, 0, slot, 0):
            copy.wait()

        @pl.when(pair)
        def _():
            for copy in copies(0, 0, slot, 1):
                copy.wait()
            accumulate(slot, fresh, 2 * TILE)

        @pl.when(jnp.logical_not(pair))
        def _():
            accumulate(slot, fresh, TILE)

    width = acc.shape[1] // outs
    for i in range(outs):
        out_refs[i][...] = acc[:, i * width:(i + 1) * width].astype(out_refs[i].dtype)


def weight_grad(layout, table, lhs, rhs, experts, outs):
    left, right = lhs[0].shape[1], rhs[0].shape[1]
    width = right // outs
    kernel = functools.partial(weight_grad_kernel, layout["grad"], layout["tiles_max"], outs)
    scratch = [
        pltpu.VMEM((2, 2 * TILE, left), jnp.bfloat16),
        pltpu.VMEM((2, 2 * TILE, right), jnp.bfloat16),
        pltpu.VMEM((left, 2 * TILE), jnp.bfloat16),
        pltpu.VMEM((left, right), jnp.float32),
        pltpu.SemaphoreType.DMA((2, 2, 2)),
    ]
    return call(
        kernel, "weight_grad", table, (*lhs, *rhs), [ANY] * (2 * CHUNKS),
        [jax.ShapeDtypeStruct((experts, left, width), jnp.bfloat16)] * outs,
        [pl.BlockSpec((pl.squeezed, left, width), lambda e, *_: (e, 0, 0))] * outs,
        scratch, (2 * 10000 * left * right, 100 * 10**6), (experts,),
    )


def below(size, strict):
    i = lax.broadcasted_iota(jnp.int32, (size, size), 0)
    j = lax.broadcasted_iota(jnp.int32, (size, size), 1)
    return (i < j if strict else i <= j).astype(jnp.float32)


def running(values):
    size = values.shape[-1]
    i = lax.broadcasted_iota(jnp.int32, (size, size), 0)
    j = lax.broadcasted_iota(jnp.int32, (size, size), 1)
    return jnp.sum(jnp.where(i <= j, values[..., :, None], 0), axis=-2)


def pick(table, index):
    hot = index[..., None] == jnp.arange(table.shape[1], dtype=jnp.int32)
    hot = hot.reshape(hot.shape + (1,) * (table.ndim - 2))
    return jnp.sum(jnp.where(hot, table[:, None], 0), axis=2)


def routing(hot, my_ep):
    chunks, experts, spans, _ = hot.shape
    tiles_max = spans * LANES * 2 // TILE + experts
    within = jnp.einsum("cesi,ij->cesj", hot, below(LANES, False), preferred_element_type=jnp.float32)
    span_count = jnp.sum(hot, axis=-1)
    before = jnp.einsum("cei,ij->cej", span_count, below(spans, True), preferred_element_type=jnp.float32)
    total = jnp.sum(span_count, axis=-1).astype(jnp.int32)
    tiles = jnp.maximum((total + TILE - 1) // TILE, 1)
    tile_stop = running(tiles)
    tile_start = tile_stop - tiles
    span_first = (tile_start * TILE)[..., None] + before.astype(jnp.int32)
    span_stop = span_first + span_count.astype(jnp.int32)
    pos = jnp.where(hot > 0, span_first[..., None] + within.astype(jnp.int32) - 1, -1)

    tile_iota = jnp.arange(tiles_max, dtype=jnp.int32)
    group = jnp.sum((tile_iota[None, :, None] >= tile_stop[:, None, :experts - 1]).astype(jnp.int32), axis=2)
    stops = pick(span_stop, jnp.repeat(group, 2, axis=1))
    row0 = jnp.arange(2 * tiles_max, dtype=jnp.int32)[None, :, None] * LANES
    lo = jnp.sum((stops <= row0).astype(jnp.int32), axis=2)
    hi = jnp.minimum(jnp.sum((stops < row0 + LANES).astype(jnp.int32), axis=2), spans - 1)
    width = jnp.maximum(jnp.max(((hi - lo + 2) // 2).reshape(chunks, tiles_max, 2), axis=2), 1)
    width = jnp.where(width > WINDOWS[-1], spans // 2, width)
    start = jnp.minimum(span_first // 16 * 16, (tile_stop * TILE)[..., None] - LANES)
    over = jnp.any(span_stop - start > LANES, axis=1).reshape(chunks, spans // GROUP, GROUP)
    over = jnp.any(over, axis=2).astype(jnp.int32)
    first = jnp.concatenate([jnp.zeros((chunks, 1), jnp.int32), tile_stop], axis=1)

    in_chunks = running(tiles.T)
    both = in_chunks[:, -1]
    stop = running((both + 1) // 2)
    begin = stop - (both + 1) // 2
    step = jnp.arange(chunks * tiles_max // 2 + experts, dtype=jnp.int32)
    expert = jnp.sum((step[:, None] >= stop[None, :experts - 1]).astype(jnp.int32), axis=1)
    mine = expert[:, None] == jnp.arange(experts, dtype=jnp.int32)
    local = 2 * (step - jnp.sum(jnp.where(mine, begin, 0), axis=1))[:, None] + jnp.arange(2, dtype=jnp.int32)
    ends = jnp.sum(jnp.where(mine[:, :, None], in_chunks, 0), axis=1)[:, None, :]
    starts = jnp.sum(jnp.where(mine[:, :, None], tile_start.T, 0), axis=1)[:, None, :]
    sizes = jnp.sum(jnp.where(mine[:, :, None], tiles.T, 0), axis=1)[:, None, :]
    offset = local[:, :, None] - (ends - sizes)
    inside = jnp.logical_and(offset >= 0, local[:, :, None] < ends)
    place = starts + offset + jnp.arange(chunks, dtype=jnp.int32) * tiles_max
    src = jnp.sum(jnp.where(inside, place + 1, 0), axis=2) - 1

    sections = [("ep", my_ep.reshape(1)), ("begin", jnp.concatenate([jnp.zeros((1,), jnp.int32), stop])), ("src", src)]
    for name, values in (("count", tile_stop[:, -1:]), ("group", group), ("lo", lo), ("width", width), ("start", start), ("first", first), ("over", over)):
        sections.append((name, values))
    layout = [{} for _ in range(chunks)]
    places, at = {}, 0
    for name, values in sections:
        places[name] = at
        for c in range(chunks):
            layout[c][name] = at + (0 if name in ("ep", "begin", "src") else c * (values.size // chunks))
        at += values.size
    table = jnp.concatenate([values.reshape(-1).astype(jnp.int32) for _, values in sections])
    layout = dict(enumerate(layout))
    layout |= {"grad": {"begin": places["begin"], "src": places["src"]}, "tiles_max": tiles_max}
    return pos, table, layout


def solution(mesh):
    tp_size = mesh.shape["tp"]
    ep_size = mesh.shape["ep"]
    dev_count = tp_size * ep_size
    rows_axes = ("ep", "tp")
    row_spec = P(rows_axes, None)
    wide_spec = P("ep", None, "tp")
    down_spec = P("ep", "tp", None)
    swap = [(0, 1), (1, 0)]

    def body(x, y_grad, expert_ids, norm_gain, w_router, w_gate, w_up, w_down):
        tokens, model_dim = x.shape
        top_k = expert_ids.shape[1]
        num_experts = w_router.shape[1]
        local_experts = w_gate.shape[0]
        total_tokens = tokens * dev_count
        part = tokens // CHUNKS
        weights = (w_gate, w_up, w_down)
        my_ep = lax.axis_index("ep")

        def of_chunk(rows, c):
            return rows[c * part:(c + 1) * part]

        def gather(rows):
            return lax.all_gather(rows, "tp", axis=0, tiled=True)

        def with_other(own):
            return own, lax.ppermute(own, "ep", swap)

        def after(values, first):
            return lax.optimization_barrier((values, first))

        x_float = x.astype(jnp.float32)
        inv_rms = lax.rsqrt(jnp.mean(x_float * x_float, axis=-1, keepdims=True) + NORM_EPS)
        unit = x_float * inv_rms
        gain = norm_gain.astype(jnp.float32)
        x_norm = (unit * gain).astype(jnp.bfloat16)
        tok = [(lax.all_gather(of_chunk(x_norm, c), rows_axes, axis=0, tiled=True),) for c in range(2)]
        tok += [gather(of_chunk(x_norm, c)) for c in range(2, CHUNKS)]

        route_prob = jax.nn.softmax(jnp.dot(x_norm, w_router, preferred_element_type=jnp.float32), axis=-1)
        expert_range = jnp.arange(num_experts, dtype=jnp.int32)
        choice = jnp.sum((expert_ids[:, :, None] == expert_range[None, None, :]).astype(jnp.float32), axis=1)
        small = lax.all_gather(jnp.concatenate([choice, route_prob], axis=1).T, rows_axes, axis=0, tiled=False)
        counts = jnp.sum(small[:, :num_experts], axis=(0, 2))
        balance_scale = BALANCE_COEF * num_experts / (total_tokens * total_tokens * top_k)
        balance_loss = balance_scale * jnp.sum(counts * jnp.sum(small[:, num_experts:], axis=(0, 2)))

        small = small.reshape(ep_size, tp_size, 2, ep_size, local_experts, CHUNKS, part)
        small = lax.dynamic_index_in_dim(small, my_ep, axis=3, keepdims=False)
        small = jnp.where(my_ep == 0, small, small[::-1])
        small = small.transpose(2, 4, 3, 0, 1, 5).reshape(2, CHUNKS, local_experts, dev_count * part // LANES, LANES)
        prob = small[1]
        pos, table, layout = routing(small[0], my_ep.astype(jnp.int32))

        grad_scale = 2.0 * ACT_COEF / (total_tokens * model_dim)
        x_rows, gate_rows, pre, hidden = [], [], [], []
        d_rows, mg_rows, gate_own, gate_other = [], [], [], []
        out_sum, out_raw, moe_out, m_tok, in_sum, in_raw = [], [], [], [], [], []

        def run_forward(c):
            rows, gates, ab, h, out_rows = forward(layout, c, table, pos, prob, tok[c], weights)
            x_rows.append(rows)
            gate_rows.append(gates)
            pre.append(ab)
            hidden.append(h)
            return out_rows

        def run_backward(c):
            _, d, in_rows, mg, dgate = backward(layout, c, table, pos, *m_tok[c], pre[c], hidden[c], gate_rows[c], weights)
            d_rows.append(d)
            mg_rows.append(mg)
            return in_rows, dgate

        def send_out(c, rows):
            (other,) = combine(layout, c, 1, table, pos, rows)
            out_sum.append((rows, lax.ppermute(other, "ep", swap)))

        def sum_out(c, gate):
            rows, received = out_sum[c]
            received, gate = after(received, gate)
            (own,) = combine(layout, c, 0, table, pos, rows, None, received)
            out_raw.append(lax.psum_scatter(own, "tp", scatter_dimension=0, tiled=True))
            return gate

        def send_in(c, rows, dgate):
            other, gates = combine(layout, c, 1, table, pos, rows, dgate)
            gate_other.append(gates[:, :num_experts])
            in_sum.append((rows, dgate, lax.ppermute(other, "ep", swap)))

        def sum_in(c, gate):
            rows, dgate, received = in_sum[c]
            received, gate = after(received, gate)
            own, gates = combine(layout, c, 0, table, pos, rows, dgate, received)
            gate_own.append(gates[:, :num_experts])
            in_raw.append(lax.psum_scatter(own, "tp", scatter_dimension=0, tiled=True))
            return gate

        def send_cotangent(c, gate):
            raw, gate = after(out_raw[c], (gate, m_own[-1:]))
            gate = gate[0]
            moe_out.append(raw.astype(jnp.float32))
            moe_grad = of_chunk(y_grad, c).astype(jnp.float32) + grad_scale * moe_out[c]
            m_own.append(moe_grad.astype(jnp.bfloat16))
            m_tok.append(with_other(gather(m_own[c])))
            return gate

        m_own = []
        for c in range(CHUNKS):
            rows = run_forward(c)
            if c + 2 < CHUNKS:
                tok[c + 2], rows = after(tok[c + 2], rows)
                tok[c + 2] = with_other(tok[c + 2])
            if c >= 2:
                rows = send_cotangent(c - 2, rows)
            if c >= 1:
                rows = sum_out(c - 1, rows)
            send_out(c, rows)
        for c in range(CHUNKS):
            rows, dgate = run_backward(c)
            if c == 0:
                rows = send_cotangent(CHUNKS - 2, rows)
                rows = sum_out(CHUNKS - 1, rows)
            if c == 1:
                rows = send_cotangent(CHUNKS - 1, rows)
            if c >= 1:
                rows = sum_in(c - 1, rows)
            send_in(c, rows, dgate)
        (down_grad,) = weight_grad(layout, table, hidden, mg_rows, local_experts, 1)
        down_grad = sum_in(CHUNKS - 1, down_grad)
        d_rows[0], down_grad = after(d_rows[0], down_grad)
        gate_grad, up_grad = weight_grad(layout, table, x_rows, d_rows, local_experts, 2)

        moe_all = jnp.concatenate(moe_out, axis=0)
        y = (x_float + moe_all).astype(jnp.bfloat16)
        gate_own[0], _ = after(gate_own[0], in_raw[:CHUNKS - 1])
        sums = jnp.stack([jnp.concatenate(gate_own, axis=0), jnp.concatenate(gate_other, axis=0)])
        sums = jnp.where(my_ep == 0, sums, sums[::-1])
        sums = sums.reshape(ep_size, CHUNKS, tp_size, part * num_experts).transpose(0, 2, 1, 3)
        gate_weight_grad = lax.psum_scatter(sums.reshape(dev_count, tokens * num_experts), rows_axes, scatter_dimension=0, tiled=False)
        prob_grad = gate_weight_grad.reshape(tokens, num_experts) + balance_scale * counts[None, :]
        logit_grad = (route_prob * (prob_grad - jnp.sum(route_prob * prob_grad, axis=-1, keepdims=True))).astype(jnp.bfloat16)
        x_norm_grad = jnp.concatenate(in_raw, axis=0).astype(jnp.float32)
        x_norm_grad = x_norm_grad + jnp.einsum("se,de->sd", logit_grad, w_router, preferred_element_type=jnp.float32)
        unit_grad = x_norm_grad * gain
        x_grad = y_grad.astype(jnp.float32) + inv_rms * (unit_grad - unit * jnp.mean(unit_grad * unit, axis=-1, keepdims=True))
        gain_sum, router_sum, act_sum = lax.psum(
            (
                jnp.sum(x_norm_grad * unit, axis=0),
                jnp.einsum("sd,se->de", x_norm, logit_grad, preferred_element_type=jnp.float32),
                jnp.sum(moe_all * moe_all),
            ),
            ("tp", "ep"),
        )
        act_loss = ACT_COEF * act_sum / (total_tokens * model_dim)
        return (y, x_grad.astype(jnp.bfloat16), gain_sum.astype(jnp.bfloat16), router_sum.astype(jnp.bfloat16), gate_grad, up_grad, down_grad, balance_loss, act_loss)

    return jax.shard_map(body, mesh=mesh, in_specs=(row_spec, row_spec, row_spec, P(), P(), wide_spec, wide_spec, down_spec), out_specs=(row_spec, row_spec, P(), P(), wide_spec, wide_spec, down_spec, P(), P()), check_vma=False)
```

```python
import functools

import jax
import jax.numpy as jnp
from jax import lax
from jax.experimental import pallas as pl
from jax.experimental.pallas import tpu as pltpu
from jax.sharding import PartitionSpec as P

NORM_EPS = 1e-6
ACT_COEF = 1e-5
BALANCE_COEF = 1e-3
TILE = 256
LANES = 128
GROUP = 4
PARTS = (384, 256, 384)
CHUNKS = len(PARTS)
WINDOWS = (1, 2, 3, 4)
VMEM_LIMIT = 62 * 1024 * 1024


def call(kernel, name, table, operands, in_specs, out_shape, out_specs, scratch, cost, grid=()):
    return pl.pallas_call(
        kernel,
        grid_spec=pltpu.PrefetchScalarGridSpec(
            num_scalar_prefetch=1, grid=grid, in_specs=in_specs, out_specs=out_specs, scratch_shapes=scratch
        ),
        out_shape=out_shape,
        compiler_params=pltpu.CompilerParams(vmem_limit_bytes=VMEM_LIMIT),
        cost_estimate=pl.CostEstimate(flops=cost[0], bytes_accessed=cost[1], transcendentals=0),
        name=name,
    )(table, *operands)


ANY = pl.BlockSpec(memory_space=pl.ANY)
WHOLE = pl.BlockSpec(memory_space=pltpu.VMEM)


def row_block(width):
    return pl.BlockSpec((TILE, width), lambda t: (t, 0))


def dispatch_phase(at, spans, table_ref, pos_ref, prob_ref, tok_hbm, outs):
    tokens, dim = tok_hbm.shape
    blocks = tokens // TILE

    def run(tok, waited, sems):
        def block_copy(index):
            rows = pl.ds(index * TILE if isinstance(index, int) else pl.multiple_of(index * TILE, TILE), TILE)
            return pltpu.make_async_copy(tok_hbm.at[rows, :], tok.at[rows, :], sems.at[index])

        waited[0] = 0
        for index in range(blocks):
            block_copy(index).start()

        def await_tokens(stop_span):
            need = (stop_span * LANES + TILE - 1) // TILE

            @pl.loop(waited[0], need)
            def _(index):
                block_copy(index).wait()

            waited[0] = jnp.maximum(waited[0], need)

        def tile_body(x_ref, gate_ref=None):
            tile = pl.program_id(0)
            group = table_ref[at["group"] + tile]
            width = table_ref[at["width"] + tile]

            def window(half, count, start):
                row_id = lax.broadcasted_iota(jnp.int32, (LANES, LANES), 0) + (tile * TILE + half * LANES)
                into = pl.ds(half * LANES if isinstance(half, int) else pl.multiple_of(half * LANES, LANES), LANES)
                hot, gate = [], jnp.zeros((LANES, LANES), jnp.float32)
                for q in range(count):
                    span = pl.ds(spans[0] + start + q, 1)
                    match = pos_ref[group, span, :] == row_id
                    hot.append(jnp.where(match, 1.0, 0.0).astype(jnp.bfloat16))
                    if gate_ref is not None:
                        gate = gate + jnp.where(match, prob_ref[group, span, :], 0.0)
                rows = tok[pl.ds(pl.multiple_of(start * LANES, LANES), count * LANES), :]
                out = jnp.dot(jnp.concatenate(hot, axis=1), rows, preferred_element_type=jnp.float32)
                x_ref[into, :] = out.astype(x_ref.dtype)
                if gate_ref is not None:
                    gate_ref[into, :] = jnp.broadcast_to(jnp.sum(gate, axis=1, keepdims=True), (LANES, LANES))

            @pl.when(width > WINDOWS[-1])
            def _():
                await_tokens(spans[1])

                @pl.loop(0, 2)
                def _(half):
                    window(half, spans[1], 0)

            for k in WINDOWS:
                @pl.when(width == k)
                def _(k=k):
                    starts = [jnp.minimum(table_ref[at["lo"] + 2 * tile + half], spans[1] - 2 * k) for half in range(2)]
                    await_tokens(jnp.maximum(starts[0], starts[1]) + 2 * k)
                    for half in range(2):
                        window(half, 2 * k, starts[half])

        pltpu.emit_pipeline(
            tile_body, grid=(table_ref[at["count"]],), out_specs=[row_block(out.shape[1]) for out in outs]
        )(*outs)
        await_tokens(spans[1])

    pl.run_scoped(
        run,
        pltpu.VMEM((tokens, dim), jnp.bfloat16),
        pltpu.SMEM((1,), jnp.int32),
        pltpu.SemaphoreType.DMA((blocks,)),
    )


def combine_kernel(at, spans, groups, with_gate, table_ref, pos_ref, rows_hbm, *rest):
    if with_gate:
        gate_hbm, out_ref, gout_ref, rows, gates, waited, sems = rest
    else:
        out_ref, rows, waited, sems = rest
    step = pl.program_id(0)
    steps = pl.num_programs(0)
    row_iota = lax.broadcasted_iota(jnp.int32, (LANES, LANES), 0)
    over = table_ref[at["over"] + step]

    def region(g):
        return table_ref[at["first"] + g], table_ref[at["first"] + g + 1]

    def start_of(g, span):
        return pl.multiple_of(table_ref[at["start"][g] + span], 16)

    def block_copies(index):
        into = pl.ds(pl.multiple_of(index * TILE, TILE), TILE)
        copies = [pltpu.make_async_copy(rows_hbm.at[into, :], rows.at[into, :], sems.at[0, index])]
        if with_gate:
            copies.append(pltpu.make_async_copy(gate_hbm.at[into, :], gates.at[into, :], sems.at[1, index]))
        return copies

    @pl.when(step == 0)
    def _():
        for g in range(groups):
            waited[g] = region(g)[0]
        longest = region(0)[1] - region(0)[0]
        for g in range(1, groups):
            longest = jnp.maximum(longest, region(g)[1] - region(g)[0])

        @pl.loop(0, longest)
        def _(index):
            for g in range(groups):
                begin, stop = region(g)

                @pl.when(begin + index < stop)
                def _(begin=begin):
                    for copy in block_copies(begin + index):
                        copy.start()

    for g in range(groups):
        stop = region(g)[1]
        need = jnp.minimum((start_of(g, (step + 1) * GROUP - 1) + LANES + over * LANES + TILE - 1) // TILE, stop)
        need = jnp.where(step == steps - 1, stop, need)

        @pl.loop(waited[g], need)
        def _(index):
            for copy in block_copies(index):
                copy.wait()

        waited[g] = jnp.maximum(waited[g], need)

    def window(q, second):
        span = step * GROUP + q
        hot, data, gdata = [], [], []
        for g in range(groups):
            begin = place = start_of(g, span)
            if second:
                first, stop = region(g)
                place = pl.multiple_of(jnp.where(first == stop, begin, jnp.minimum(begin + LANES, stop * TILE - LANES)), 16)
                begin = begin + LANES
            row = row_iota + place
            match = pos_ref[g, pl.ds(spans[0] + span, 1), :] == row
            if second:
                match = jnp.logical_and(match, row >= begin)
            hot.append(jnp.where(match, 1.0, 0.0).astype(jnp.bfloat16))
            data.append(rows[pl.ds(place, LANES), :])
            if with_gate:
                gdata.append(gates[pl.ds(place, LANES), :])
        hot = jnp.concatenate(hot, axis=0)
        dims = (((0,), (0,)), ((), ()))
        out = lax.dot_general(hot, jnp.concatenate(data, axis=0), dims, preferred_element_type=jnp.float32)
        if not with_gate:
            return out, None
        exact = jnp.concatenate(gdata, axis=0)
        high = exact.astype(jnp.bfloat16)
        low = (exact - high.astype(jnp.float32)).astype(jnp.bfloat16)
        pair = lax.dot_general(hot, jnp.concatenate([high, low], axis=1), dims, preferred_element_type=jnp.float32)
        return out, pair[:, :LANES] + pair[:, LANES:]

    def put(q, wide):
        out, gate = window(q, False)
        if wide:
            out2, gate2 = window(q, True)
            out = out + out2
            gate = gate + gate2 if with_gate else None
        into = pl.ds(q * LANES if isinstance(q, int) else pl.multiple_of(q * LANES, LANES), LANES)
        out_ref[into, :] = out.astype(out_ref.dtype)
        if with_gate:
            gout_ref[into, :] = gate

    @pl.when(over == 0)
    def _():
        for q in range(GROUP):
            put(q, False)

    @pl.when(over != 0)
    def _():
        @pl.loop(0, GROUP)
        def _(q):
            put(q, True)


def combine(layout, chunk, table, pos, rows, gate_rows=None):
    rows_max, dim = rows.shape
    groups = pos.shape[0]
    spans = layout[chunk]["spans"]
    tokens = spans[1] * LANES
    with_gate = gate_rows is not None
    block = GROUP * LANES
    operands, in_specs = [pos, rows], [WHOLE, ANY]
    out_shape = [jax.ShapeDtypeStruct((tokens, dim), jnp.bfloat16)]
    out_specs = [pl.BlockSpec((block, dim), lambda t, *_: (t, 0))]
    scratch = [pltpu.VMEM((rows_max, dim), jnp.bfloat16)]
    if with_gate:
        operands.append(gate_rows)
        in_specs.append(ANY)
        out_shape.append(jax.ShapeDtypeStruct((tokens, LANES), jnp.float32))
        out_specs.append(pl.BlockSpec((block, LANES), lambda t, *_: (t, 0)))
        scratch.append(pltpu.VMEM((rows_max, LANES), jnp.float32))
    scratch += [pltpu.SMEM((groups,), jnp.int32), pltpu.SemaphoreType.DMA((2, rows_max // TILE))]
    kernel = functools.partial(combine_kernel, layout[chunk], spans, groups, with_gate)
    return call(kernel, "combine", table, operands, in_specs, out_shape, out_specs, scratch, (9 * 10**9, 35 * 10**6), (tokens // block,))


class WeightStream:
    def __init__(self, at, table_ref, weights, scratch):
        self.at, self.table_ref, self.own, self.helped = at, table_ref, weights[:3], weights[3:]
        self.wide, self.down, self.sems = scratch
        self.experts, _, self.ffn = weights[0].shape

    def copies(self, sources, s):
        wg, wu, wd = sources
        return (
            pltpu.make_async_copy(wg, self.wide.at[s, :, pl.ds(0, self.ffn)], self.sems.at[s, 0]),
            pltpu.make_async_copy(wu, self.wide.at[s, :, pl.ds(self.ffn, self.ffn)], self.sems.at[s, 1]),
            pltpu.make_async_copy(wd, self.down.at[s], self.sems.at[s, 2]),
        )

    def start(self, group, s):
        @pl.when(jnp.logical_and(group >= 0, group < self.experts))
        def _():
            for copy in self.copies([w.at[group] for w in self.own], s):
                copy.start()

        @pl.when(group == self.experts)
        def _():
            for copy in self.copies([w.at[0] for w in self.helped], s):
                copy.start()

    def begin(self):
        self.start(self.table_ref[self.at["group"]], 0)

    def slot(self):
        tile = pl.program_id(0)
        s = table_slot = self.table_ref[self.at["slot"] + tile]

        @pl.when(self.table_ref[self.at["fresh"] + tile] != 0)
        def _():
            self.start(self.table_ref[self.at["next"] + tile], 1 - table_slot)
            for copy in self.copies([w.at[0] for w in self.own], table_slot):
                copy.wait()

        return s


def forward_kernel(at, spans, table_ref, pos_ref, prob_ref, tok_hbm, *rest):
    x_hbm, gate_hbm, ab_hbm, h_hbm, out_hbm = rest[6:11]
    stream = WeightStream(at, table_ref, rest[:6], rest[11:])
    wide, down, ffn = stream.wide, stream.down, stream.ffn
    stream.begin()
    dispatch_phase(at, spans, table_ref, pos_ref, prob_ref, tok_hbm, (x_hbm, gate_hbm))

    def tile_body(x_ref, gate_ref, ab_ref, h_ref, out_ref):
        slot = stream.slot()
        x = x_ref[...]
        for j in range(ffn // LANES):
            cols = slice(j * LANES, (j + 1) * LANES)
            ucols = slice(ffn + j * LANES, ffn + (j + 1) * LANES)
            both = jnp.dot(x, jnp.concatenate([wide[slot, :, cols], wide[slot, :, ucols]], axis=1), preferred_element_type=jnp.float32)
            a, b = both[:, :LANES], both[:, LANES:]
            ab_ref[:, cols] = a
            ab_ref[:, ucols] = b
            h_ref[:, cols] = (a * jax.nn.sigmoid(a) * b).astype(h_ref.dtype)
        out = jnp.dot(h_ref[...], down[slot], preferred_element_type=jnp.float32)
        gate = gate_ref[...]
        for j in range(out.shape[1] // LANES):
            cols = slice(j * LANES, (j + 1) * LANES)
            out_ref[:, cols] = (out[:, cols] * gate).astype(out_ref.dtype)

    piped_in, piped_out = (x_hbm, gate_hbm), (ab_hbm, h_hbm, out_hbm)
    pltpu.emit_pipeline(
        tile_body, grid=(table_ref[at["count"]],),
        in_specs=[row_block(ref.shape[1]) for ref in piped_in],
        out_specs=[row_block(ref.shape[1]) for ref in piped_out],
    )(*piped_in, *piped_out)


def backward_kernel(at, spans, table_ref, pos_ref, tok_hbm, ab_hbm, h_hbm, gate_hbm, *rest):
    m_hbm, d_hbm, in_hbm, mg_hbm, dgate_hbm = rest[6:11]
    stream = WeightStream(at, table_ref, rest[:6], rest[11:])
    wide, down, ffn = stream.wide, stream.down, stream.ffn
    trans = (((1,), (1,)), ((), ()))
    stream.begin()
    dispatch_phase(at, spans, table_ref, pos_ref, None, tok_hbm, (m_hbm,))

    def tile_body(m_ref, ab_ref, h_ref, gate_ref, d_ref, in_ref, mg_ref, dgate_ref):
        slot = stream.slot()
        m = m_ref[...]
        gate = gate_ref[...]
        dgate = jnp.zeros(gate.shape, jnp.float32)
        for c in range(0, ffn, 2 * LANES):
            width = min(2 * LANES, ffn - c)
            raw = lax.dot_general(m, down[slot, c:c + width, :], trans, preferred_element_type=jnp.float32)
            for k in range(width // LANES):
                lo = c + k * LANES
                cols = slice(lo, lo + LANES)
                ucols = slice(ffn + lo, ffn + lo + LANES)
                g = raw[:, k * LANES:(k + 1) * LANES]
                a, b = ab_ref[:, cols], ab_ref[:, ucols]
                sig = jax.nn.sigmoid(a)
                hidden_grad = g * gate
                d_ref[:, cols] = (hidden_grad * b * sig * (1.0 + a * (1.0 - sig))).astype(d_ref.dtype)
                d_ref[:, ucols] = (hidden_grad * (a * sig)).astype(d_ref.dtype)
                dgate = dgate + g * h_ref[:, cols].astype(jnp.float32)
        in_ref[...] = lax.dot_general(d_ref[...], wide[slot], trans, preferred_element_type=jnp.float32).astype(in_ref.dtype)
        for j in range(m.shape[1] // LANES):
            cols = slice(j * LANES, (j + 1) * LANES)
            mg_ref[:, cols] = (m[:, cols].astype(jnp.float32) * gate).astype(mg_ref.dtype)
        lane = lax.broadcasted_iota(jnp.int32, gate.shape, 1)
        expert = table_ref[at["expert"] + table_ref[at["group"] + pl.program_id(0)]]
        dgate_ref[...] = jnp.where(lane == expert, jnp.sum(dgate, axis=1, keepdims=True), 0.0)

    piped_in, piped_out = (m_hbm, ab_hbm, h_hbm, gate_hbm), (d_hbm, in_hbm, mg_hbm, dgate_hbm)
    pltpu.emit_pipeline(
        tile_body, grid=(table_ref[at["count"]],),
        in_specs=[row_block(ref.shape[1]) for ref in piped_in],
        out_specs=[row_block(ref.shape[1]) for ref in piped_out],
    )(*piped_in, *piped_out)


def weight_scratch(wg):
    _, dim, ffn = wg.shape
    return [
        pltpu.VMEM((2, dim, 2 * ffn), wg.dtype),
        pltpu.VMEM((2, ffn, dim), wg.dtype),
        pltpu.SemaphoreType.DMA((2, 3)),
    ]


def shapes(rows_max, *kinds):
    return [jax.ShapeDtypeStruct((rows_max, width), dtype) for width, dtype in kinds]


def forward(layout, chunk, table, pos, prob, tok, weights):
    _, dim, ffn = weights[0].shape
    kinds = ((dim, jnp.bfloat16), (LANES, jnp.float32), (2 * ffn, jnp.float32), (ffn, jnp.bfloat16), (dim, jnp.bfloat16))
    at = layout[chunk]
    kernel = functools.partial(forward_kernel, at, at["spans"])
    return call(
        kernel, "forward", table, (pos, prob, tok, *weights), [WHOLE, WHOLE] + [ANY] * 7,
        shapes(at["rows_max"], *kinds), [ANY] * 5, weight_scratch(weights[0]), (75 * 10**9, 150 * 10**6),
    )


def backward(layout, chunk, table, pos, tok, ab, hidden, gates, weights):
    _, dim, ffn = weights[0].shape
    kinds = ((dim, jnp.bfloat16), (2 * ffn, jnp.bfloat16), (dim, jnp.bfloat16), (dim, jnp.bfloat16), (LANES, jnp.float32))
    at = layout[chunk]
    kernel = functools.partial(backward_kernel, at, at["spans"])
    return call(
        kernel, "backward", table, (pos, tok, ab, hidden, gates, *weights), [WHOLE] + [ANY] * 10,
        shapes(at["rows_max"], *kinds), [ANY] * 5, weight_scratch(weights[0]), (75 * 10**9, 150 * 10**6),
    )


def weight_grad_kernel(at, tiles_max, outs, table_ref, *rest):
    lhs_hbm, rhs_hbm = rest[:CHUNKS], rest[CHUNKS:2 * CHUNKS]
    own_out, helped_out = rest[2 * CHUNKS:2 * CHUNKS + outs], rest[2 * CHUNKS + outs:2 * CHUNKS + 2 * outs]
    lhs, rhs, lhs_t, acc, staged, pending, sems, out_sems = rest[2 * CHUNKS + 2 * outs:]
    experts = own_out[0].shape[0]
    steps = table_ref[at["steps"]]

    def copies(chunk, row, s, half):
        source = pl.ds(pl.multiple_of(row, TILE), TILE)
        into = pl.ds(half * TILE, TILE)
        return (
            pltpu.make_async_copy(lhs_hbm[chunk].at[source, :], lhs.at[s, into, :], sems.at[s, half, 0]),
            pltpu.make_async_copy(rhs_hbm[chunk].at[source, :], rhs.at[s, into, :], sems.at[s, half, 1]),
        )

    def start(index, s):
        for half in range(2):
            src = table_ref[at["src"] + 2 * index + half]
            for chunk in range(CHUNKS):
                @pl.when(jnp.logical_and(src >= chunk * tiles_max, src < (chunk + 1) * tiles_max))
                def _(chunk=chunk, src=src, half=half):
                    for copy in copies(chunk, (src - chunk * tiles_max) * TILE, s, half):
                        copy.start()

    def out_copies(targets):
        return [pltpu.make_async_copy(staged.at[i], target, out_sems.at[i]) for i, target in enumerate(targets)]

    def drain():
        @pl.when(pending[0] != 0)
        def _():
            for copy in out_copies([out.at[0] for out in own_out]):
                copy.wait()

        pending[0] = 0

    pending[0] = 0
    start(0, 0)

    def accumulate(slot, fresh, depth):
        lhs_t[:, :depth] = jnp.transpose(lhs[slot, :depth, :], (1, 0))
        block = 2 * LANES
        for c in range(0, acc.shape[1], block):
            part = jnp.dot(lhs_t[:, :depth], rhs[slot, :depth, c:c + block], preferred_element_type=jnp.float32)
            acc[:, c:c + block] = jnp.where(fresh, 0.0, acc[:, c:c + block]) + part

    @pl.loop(0, steps)
    def _(step):
        slot = lax.rem(step, 2)
        group = table_ref[at["owner"] + step]

        @pl.when(step + 1 < steps)
        def _():
            start(step + 1, 1 - slot)

        fresh = jnp.logical_or(step == 0, group != table_ref[at["owner"] + jnp.maximum(step - 1, 0)])
        last = jnp.logical_or(step == steps - 1, group != table_ref[at["owner"] + step + 1])
        pair = table_ref[at["src"] + 2 * step + 1] >= 0
        for copy in copies(0, 0, slot, 0):
            copy.wait()

        @pl.when(pair)
        def _():
            for copy in copies(0, 0, slot, 1):
                copy.wait()
            accumulate(slot, fresh, 2 * TILE)

        @pl.when(jnp.logical_not(pair))
        def _():
            accumulate(slot, fresh, TILE)

        @pl.when(last)
        def _():
            drain()
            width = acc.shape[1] // outs
            for i in range(outs):
                staged[i, :, :] = acc[:, i * width:(i + 1) * width].astype(staged.dtype)

            @pl.when(group < experts)
            def _():
                for copy in out_copies([out.at[group] for out in own_out]):
                    copy.start()

            @pl.when(group == experts)
            def _():
                for copy in out_copies([out.at[0] for out in helped_out]):
                    copy.start()

            pending[0] = 1

    drain()


def weight_grad(layout, table, lhs, rhs, experts, outs):
    left, right = lhs[0].shape[1], rhs[0].shape[1]
    width = right // outs
    kernel = functools.partial(weight_grad_kernel, layout["grad"], layout["tiles_max"], outs)
    scratch = [
        pltpu.VMEM((2, 2 * TILE, left), jnp.bfloat16),
        pltpu.VMEM((2, 2 * TILE, right), jnp.bfloat16),
        pltpu.VMEM((left, 2 * TILE), jnp.bfloat16),
        pltpu.VMEM((left, right), jnp.float32),
        pltpu.VMEM((outs, left, width), jnp.bfloat16),
        pltpu.SMEM((1,), jnp.int32),
        pltpu.SemaphoreType.DMA((2, 2, 2)),
        pltpu.SemaphoreType.DMA((outs,)),
    ]
    out_shape = [jax.ShapeDtypeStruct((n, left, width), jnp.bfloat16) for n in [experts] * outs + [1] * outs]
    return call(
        kernel, "weight_grad", table, (*lhs, *rhs), [ANY] * (2 * CHUNKS), out_shape, [ANY] * len(out_shape),
        scratch, (2 * 9000 * left * right, 100 * 10**6),
    )


def insert_kernel(at, table_ref, *rest):
    back, outs, staged, sems = rest[:3], rest[6:9], rest[9:12], rest[12]
    place = table_ref[at]

    @pl.when(place >= 0)
    def _():
        fetch = [pltpu.make_async_copy(b.at[0], s, sems.at[0, i]) for i, (b, s) in enumerate(zip(back, staged))]
        store = [pltpu.make_async_copy(s, out.at[place], sems.at[1, i]) for i, (s, out) in enumerate(zip(staged, outs))]
        for copy in fetch:
            copy.start()
        for i in range(3):
            fetch[i].wait()
            store[i].start()
        for copy in store:
            copy.wait()


def insert(layout, table, back, grads):
    kernel = functools.partial(insert_kernel, layout["insert"])
    return pl.pallas_call(
        kernel,
        grid_spec=pltpu.PrefetchScalarGridSpec(
            num_scalar_prefetch=1,
            in_specs=[ANY] * 6,
            out_specs=[ANY] * 3,
            scratch_shapes=[pltpu.VMEM(g.shape[1:], g.dtype) for g in grads] + [pltpu.SemaphoreType.DMA((2, 3))],
        ),
        out_shape=[jax.ShapeDtypeStruct(g.shape, g.dtype) for g in grads],
        input_output_aliases={4 + i: i for i in range(3)},
        compiler_params=pltpu.CompilerParams(vmem_limit_bytes=VMEM_LIMIT),
        cost_estimate=pl.CostEstimate(flops=10**9, bytes_accessed=35 * 10**6, transcendentals=0),
        name="insert",
    )(table, *back, *grads)


def below(size, strict):
    i = lax.broadcasted_iota(jnp.int32, (size, size), 0)
    j = lax.broadcasted_iota(jnp.int32, (size, size), 1)
    return (i < j if strict else i <= j).astype(jnp.float32)


def running(values):
    size = values.shape[-1]
    i = lax.broadcasted_iota(jnp.int32, (size, size), 0)
    j = lax.broadcasted_iota(jnp.int32, (size, size), 1)
    return jnp.sum(jnp.where(i <= j, values[..., :, None], 0), axis=-2)


def count(condition, axis):
    return jnp.sum(condition.astype(jnp.int32), axis=axis)


def choose_help(tiles, experts):
    half = [jnp.sum(tiles[:experts]), jnp.sum(tiles[experts:])]
    gap = jnp.abs(half[0] - half[1])
    index = jnp.arange(2 * experts, dtype=jnp.int32)
    on_busier = (index >= experts) == (half[1] > half[0])
    left = jnp.where(on_busier, jnp.abs(gap - 2 * tiles), gap)
    best = jnp.min(left)
    moved = jnp.min(jnp.where(left == best, index, 2 * experts))
    return jnp.where(best < gap, moved, -1)


def routing(hot, experts_of, place):
    groups, span_total, _ = hot.shape
    spans_of = [part * (span_total * LANES // sum(PARTS)) // LANES for part in PARTS]
    firsts = [sum(spans_of[:c]) for c in range(CHUNKS)]
    chunk_of = jnp.concatenate([jnp.full((n,), c, jnp.int32) for c, n in enumerate(spans_of)])
    member = chunk_of[:, None] == jnp.arange(CHUNKS, dtype=jnp.int32)[None, :]
    same = chunk_of[:, None] == chunk_of[None, :]
    tiles_of = [2 * n * LANES // TILE + groups for n in spans_of]
    tiles_max = max(tiles_of)

    within = jnp.einsum("gsi,ij->gsj", hot, below(LANES, False), preferred_element_type=jnp.float32)
    span_count = jnp.sum(hot, axis=-1)
    before = jnp.einsum("gi,ij->gj", span_count, jnp.where(same, below(span_total, True), 0.0), preferred_element_type=jnp.float32)
    total = jnp.sum(jnp.where(member[:, None, :], span_count.T[:, :, None], 0.0), axis=0).T.astype(jnp.int32)
    tiles = (total + TILE - 1) // TILE
    none = jnp.logical_and(jnp.sum(tiles, axis=1, keepdims=True) == 0, jnp.arange(groups, dtype=jnp.int32) == 0)
    tiles = jnp.where(none, 1, tiles)
    stop = running(tiles)
    begin = stop - tiles

    def to_spans(values):
        return jnp.sum(jnp.where(member[None], values.T[:, None, :], 0), axis=2)

    span_first = to_spans(begin) * TILE + before.astype(jnp.int32)
    span_stop = span_first + span_count.astype(jnp.int32)
    pos = jnp.where(hot > 0, span_first[:, :, None] + within.astype(jnp.int32) - 1, -1)

    index = jnp.arange(groups, dtype=jnp.int32)
    tile = jnp.arange(tiles_max, dtype=jnp.int32)
    group = jnp.minimum(count(tile[None, :, None] >= stop[:, None, :], 2), groups - 1)
    mine = group[:, :, None] == index
    ordinal = running((tiles > 0).astype(jnp.int32)) - 1
    later = jnp.logical_and(index[None, None, :] > group[:, :, None], tiles[:, None, :] > 0)
    follow = jnp.min(jnp.where(later, index, groups), axis=2)
    follow = jnp.where(follow == groups, -1, follow)
    fresh = jnp.sum(jnp.where(mine, begin[:, None, :], 0), axis=2) == tile
    slot = jnp.sum(jnp.where(mine, ordinal[:, None, :], 0), axis=2) % 2

    half_mine = jnp.repeat(mine, 2, axis=1)
    stops = jnp.sum(jnp.where(half_mine[..., None], span_stop[None, None], 0), axis=2)
    row0 = jnp.arange(2 * tiles_max, dtype=jnp.int32)[None, :, None] * LANES
    inside = member.T[:, None, :]
    lo = count(jnp.logical_and(inside, stops <= row0), 2)
    hi = jnp.minimum(count(jnp.logical_and(inside, stops < row0 + LANES), 2), jnp.array(spans_of, jnp.int32)[:, None] - 1)
    width = jnp.maximum(jnp.max(((hi - lo + 2) // 2).reshape(CHUNKS, tiles_max, 2), axis=2), 1)
    start = jnp.minimum(span_first // 16 * 16, to_spans(stop) * TILE - LANES)
    empty = to_spans(tiles) == 0
    leading = jnp.logical_and(jnp.logical_not(empty), to_spans(ordinal) == 0)
    start = jnp.where(empty, jnp.sum(jnp.where(leading, start, 0), axis=0), start)
    over = jnp.any(jnp.logical_and(jnp.logical_not(empty), span_stop - start > LANES), axis=0)
    over = jnp.any(over.reshape(-1, GROUP), axis=1)

    in_chunks = running(tiles.T)
    both = in_chunks[:, -1]
    step_stop = running((both + 1) // 2)
    step_first = step_stop - (both + 1) // 2
    steps = CHUNKS * tiles_max // 2 + groups
    step = jnp.arange(steps, dtype=jnp.int32)
    owner = jnp.minimum(count(step[:, None] >= step_stop[None, :], 1), groups - 1)
    step_mine = owner[:, None] == index

    def of_step(values):
        return jnp.sum(jnp.where(step_mine[:, :, None], values[None], 0), axis=1)[:, None, :]

    local = 2 * (step - of_step(step_first[:, None])[:, 0, 0])[:, None, None] + jnp.arange(2, dtype=jnp.int32)[None, :, None]
    ends, sizes = of_step(in_chunks), of_step(tiles.T)
    offset = local - (ends - sizes)
    found = jnp.logical_and(offset >= 0, local < ends)
    chunk_at = jnp.arange(CHUNKS, dtype=jnp.int32) * tiles_max
    src = jnp.sum(jnp.where(found, of_step(begin.T) + offset + chunk_at + 1, 0), axis=2) - 1

    sections = (
        ("expert", experts_of), ("insert", place.reshape(1)), ("steps", step_stop[-1:]), ("owner", owner), ("src", src),
        ("count", stop[:, -1:]), ("group", group), ("slot", slot), ("fresh", fresh), ("next", follow), ("lo", lo), ("width", width),
        ("first", jnp.concatenate([jnp.zeros((CHUNKS, 1), jnp.int32), stop], axis=1)), ("start", start), ("over", over),
    )
    table = jnp.concatenate([values.reshape(-1).astype(jnp.int32) for _, values in sections])
    places, sizes_of, at = {}, {}, 0
    for name, values in sections:
        places[name], sizes_of[name] = at, values.size
        at += values.size
    layout = {}
    for c in range(CHUNKS):
        layout[c] = {name: places[name] + c * (sizes_of[name] // CHUNKS) for name in ("count", "group", "slot", "fresh", "next", "lo", "width", "first")}
        layout[c] |= {
            "expert": places["expert"], "spans": (firsts[c], spans_of[c]), "rows_max": tiles_of[c] * TILE,
            "start": [places["start"] + g * span_total + firsts[c] for g in range(groups)],
            "over": places["over"] + firsts[c] // GROUP,
        }
    layout |= {"grad": {name: places[name] for name in ("steps", "owner", "src")}, "insert": places["insert"], "tiles_max": tiles_max}
    return pos, table, layout


def solution(mesh):
    tp_size = mesh.shape["tp"]
    ep_size = mesh.shape["ep"]
    dev_count = tp_size * ep_size
    rows_axes = ("ep", "tp")
    row_spec = P(rows_axes, None)
    wide_spec = P("ep", None, "tp")
    down_spec = P("ep", "tp", None)
    swap = [(0, 1), (1, 0)]

    def body(x, y_grad, expert_ids, norm_gain, w_router, w_gate, w_up, w_down):
        tokens, model_dim = x.shape
        top_k = expert_ids.shape[1]
        num_experts = w_router.shape[1]
        local_experts = w_gate.shape[0]
        total_tokens = tokens * dev_count
        my_ep = lax.axis_index("ep").astype(jnp.int32)
        firsts = [sum(PARTS[:c]) for c in range(CHUNKS)]

        def of_chunk(rows, c, axis=0):
            return lax.slice_in_dim(rows, firsts[c], firsts[c] + PARTS[c], axis=axis)

        def gather(rows):
            return lax.all_gather(rows, rows_axes, axis=0, tiled=True)

        def scatter(rows):
            return lax.psum_scatter(rows, rows_axes, scatter_dimension=0, tiled=True)

        def after(values, first):
            return lax.optimization_barrier((values, first))

        x_float = x.astype(jnp.float32)
        inv_rms = lax.rsqrt(jnp.mean(x_float * x_float, axis=-1, keepdims=True) + NORM_EPS)
        unit = x_float * inv_rms
        gain = norm_gain.astype(jnp.float32)
        x_norm = (unit * gain).astype(jnp.bfloat16)
        tok = [gather(of_chunk(x_norm, c)) for c in range(CHUNKS)]

        route_prob = jax.nn.softmax(jnp.dot(x_norm, w_router, preferred_element_type=jnp.float32), axis=-1)
        expert_range = jnp.arange(num_experts, dtype=jnp.int32)
        choice = jnp.sum((expert_ids[:, :, None] == expert_range[None, None, :]).astype(jnp.float32), axis=1)
        small = lax.all_gather(jnp.concatenate([choice, route_prob], axis=1).T, rows_axes, axis=0, tiled=False)
        counts = jnp.sum(small[:, :num_experts], axis=(0, 2))
        balance_scale = BALANCE_COEF * num_experts / (total_tokens * total_tokens * top_k)
        balance_loss = balance_scale * jnp.sum(counts * jnp.sum(small[:, num_experts:], axis=(0, 2)))

        rows_in = jnp.stack([jnp.sum(of_chunk(small[:, :num_experts], c, 2), axis=(0, 2)) for c in range(CHUNKS)])
        tiles_in = jnp.sum((rows_in.astype(jnp.int32) + TILE - 1) // TILE, axis=0)
        moved = choose_help(tiles_in, local_experts)
        my_base = my_ep * local_experts
        local = jnp.arange(local_experts, dtype=jnp.int32)
        giving = jnp.logical_and(moved >= my_base, moved < my_base + local_experts)
        helping = jnp.logical_and(moved >= 0, jnp.logical_not(giving))
        given = jnp.where(giving, moved - my_base, 0)
        group_experts = jnp.concatenate([my_base + local, jnp.maximum(moved, 0).reshape(1)])
        active = jnp.concatenate([my_base + local != moved, helping.reshape(1)])
        take = jnp.logical_and(group_experts[:, None] == expert_range, active[:, None])
        spread = jnp.concatenate([of_chunk(small, c, 2).transpose(1, 0, 2).reshape(2 * num_experts, -1) for c in range(CHUNKS)], axis=1)
        spread = spread.reshape(2, 1, num_experts, -1, LANES)
        own = jnp.sum(jnp.where(take[None, :, :, None, None], spread, 0.0), axis=2)
        prob = own[1]
        pos, table, layout = routing(own[0], group_experts, jnp.where(giving, given, -1))
        helped = [lax.ppermute(lax.dynamic_slice_in_dim(w, given, 1, axis=0), "ep", swap) for w in (w_gate, w_up, w_down)]
        weights = (w_gate, w_up, w_down, *helped)

        grad_scale = 2.0 * ACT_COEF / (total_tokens * model_dim)
        x_rows, gate_rows, pre, hidden, d_rows, mg_rows = [], [], [], [], [], []
        out_raw, moe_out, m_own, m_tok, in_raw, gate_part = [], [], [], [], [], []

        def send_cotangent(c, gate):
            raw, (gate, _) = after(out_raw[c], (gate, m_own[-1:]))
            moe_out.append(raw.astype(jnp.float32))
            moe_grad = of_chunk(y_grad, c).astype(jnp.float32) + grad_scale * moe_out[c]
            m_own.append(moe_grad.astype(jnp.bfloat16))
            m_tok.append(gather(m_own[c]))
            return gate

        for c in range(CHUNKS):
            rows, gates, ab, h, out_rows = forward(layout, c, table, pos, prob, tok[c], weights)
            (partial,) = combine(layout, c, table, pos, out_rows)
            if c == 0:
                partial, tok[1:] = after(partial, tok[1:])
            else:
                partial = send_cotangent(c - 1, partial)
            out_raw.append(scatter(partial))
            x_rows.append(rows)
            gate_rows.append(gates)
            pre.append(ab)
            hidden.append(h)
        for c in range(CHUNKS):
            _, d, in_rows, mg, dgate = backward(layout, c, table, pos, m_tok[c], pre[c], hidden[c], gate_rows[c], weights)
            if c == 0:
                in_rows = send_cotangent(CHUNKS - 1, in_rows)
            partial, gate_tok = combine(layout, c, table, pos, in_rows, dgate)
            if c == 0:
                partial, m_tok[-1] = after(partial, m_tok[-1])
            in_raw.append(scatter(partial))
            gate_part.append(gate_tok[:, :num_experts])
            d_rows.append(d)
            mg_rows.append(mg)
        *wide_grads, helped_gate, helped_up = weight_grad(layout, table, x_rows, d_rows, local_experts, 2)
        back = [lax.ppermute(g, "ep", swap) for g in (helped_gate, helped_up)]
        mg_rows[0], _ = after(mg_rows[0], wide_grads[0])
        down_grad, helped_down = weight_grad(layout, table, hidden, mg_rows, local_experts, 1)
        back.append(lax.ppermute(helped_down, "ep", swap))

        moe_all = jnp.concatenate(moe_out, axis=0)
        y = (x_float + moe_all).astype(jnp.bfloat16)
        gate_part[0], _ = after(gate_part[0], (wide_grads[0], in_raw))
        sums = jnp.concatenate([g.reshape(dev_count, -1) for g in gate_part], axis=1)
        gate_weight_grad = lax.psum_scatter(sums, rows_axes, scatter_dimension=0, tiled=False)
        prob_grad = gate_weight_grad.reshape(tokens, num_experts) + balance_scale * counts[None, :]
        logit_grad = (route_prob * (prob_grad - jnp.sum(route_prob * prob_grad, axis=-1, keepdims=True))).astype(jnp.bfloat16)
        x_norm_grad = jnp.concatenate(in_raw, axis=0).astype(jnp.float32)
        x_norm_grad = x_norm_grad + jnp.einsum("se,de->sd", logit_grad, w_router, preferred_element_type=jnp.float32)
        unit_grad = x_norm_grad * gain
        x_grad = y_grad.astype(jnp.float32) + inv_rms * (unit_grad - unit * jnp.mean(unit_grad * unit, axis=-1, keepdims=True))
        gain_sum, router_sum, act_sum = lax.psum(
            (
                jnp.sum(x_norm_grad * unit, axis=0),
                jnp.einsum("sd,se->de", x_norm, logit_grad, preferred_element_type=jnp.float32),
                jnp.sum(moe_all * moe_all),
            ),
            ("tp", "ep"),
        )
        table, _ = after(table, (x_grad, gain_sum))
        act_loss = ACT_COEF * act_sum / (total_tokens * model_dim)
        gate_grad, up_grad, down_grad = insert(layout, table, back, (*wide_grads, down_grad))
        return (y, x_grad.astype(jnp.bfloat16), gain_sum.astype(jnp.bfloat16), router_sum.astype(jnp.bfloat16), gate_grad, up_grad, down_grad, balance_loss, act_loss)

    return jax.shard_map(body, mesh=mesh, in_specs=(row_spec, row_spec, row_spec, P(), P(), wide_spec, wide_spec, down_spec), out_specs=(row_spec, row_spec, P(), P(), wide_spec, wide_spec, down_spec, P(), P()), check_vma=False)
```

```python
import functools

import jax
import jax.numpy as jnp
from jax import lax
from jax.experimental import pallas as pl
from jax.experimental.pallas import tpu as pltpu
from jax.sharding import PartitionSpec as P


NORM_EPS = 1e-6
ACT_COEF = 1e-5
BALANCE_COEF = 1e-3
TILE = 256
LANES = 128
GROUP = 4
PARTS = (384, 256, 384)
CHUNKS = len(PARTS)
WINDOWS = (1, 2, 3, 4)
STATS_SIZE = 65536
VMEM_LIMIT = 67_043_328


def call(kernel, table, operands, in_specs, out_shape, out_specs, scratch, cost, grid=()):
    return pl.pallas_call(
        kernel,
        grid_spec=pltpu.PrefetchScalarGridSpec(
            num_scalar_prefetch=1, grid=grid, in_specs=in_specs, out_specs=out_specs, scratch_shapes=scratch
        ),
        out_shape=out_shape,
        compiler_params=pltpu.CompilerParams(vmem_limit_bytes=VMEM_LIMIT),
        cost_estimate=pl.CostEstimate(flops=cost[0], bytes_accessed=cost[1], transcendentals=0),
    )(table, *operands)


ANY = pl.BlockSpec(memory_space=pl.ANY)
WHOLE = pl.BlockSpec(memory_space=pltpu.VMEM)


def row_block(width):
    return pl.BlockSpec((TILE, width), lambda t: (t, 0))


class Dispatch:
    def __init__(self, at, table_ref, pos_ref, prob_ref, tok_hbm, scratch):
        self.at, self.table_ref, self.pos_ref, self.prob_ref, self.tok_hbm = at, table_ref, pos_ref, prob_ref, tok_hbm
        self.tok, self.waited, self.sems = scratch
        self.first, self.spans = at["spans"]

    def block_copy(self, index):
        rows = pl.ds(index * TILE if isinstance(index, int) else pl.multiple_of(index * TILE, TILE), TILE)
        return pltpu.make_async_copy(self.tok_hbm.at[rows, :], self.tok.at[rows, :], self.sems.at[index])

    def begin(self):
        self.waited[0] = 0
        for index in range(self.spans * LANES // TILE):
            self.block_copy(index).start()

    def await_tokens(self, stop_span):
        need = (stop_span * LANES + TILE - 1) // TILE

        @pl.loop(self.waited[0], need)
        def _(index):
            self.block_copy(index).wait()

        self.waited[0] = jnp.maximum(self.waited[0], need)

    def end(self):
        self.await_tokens(self.spans)

    def tile(self, x_ref, gate_ref=None):
        tile = pl.program_id(0)
        group = self.table_ref[self.at["group"] + tile]
        width = self.table_ref[self.at["width"] + tile]

        def window(half, count, start):
            row_id = lax.broadcasted_iota(jnp.int32, (LANES, LANES), 0) + (tile * TILE + half * LANES)
            into = pl.ds(half * LANES if isinstance(half, int) else pl.multiple_of(half * LANES, LANES), LANES)
            hot, gate = [], jnp.zeros((LANES, LANES), jnp.float32)
            for q in range(count):
                span = pl.ds(self.first + start + q, 1)
                match = self.pos_ref[group, span, :] == row_id
                hot.append(jnp.where(match, 1.0, 0.0).astype(jnp.bfloat16))
                if gate_ref is not None:
                    gate = gate + jnp.where(match, self.prob_ref[group, span, :], 0.0)
            rows = self.tok[pl.ds(pl.multiple_of(start * LANES, LANES), count * LANES), :]
            out = jnp.dot(jnp.concatenate(hot, axis=1), rows, preferred_element_type=jnp.float32)
            x_ref[into, :] = out.astype(x_ref.dtype)
            if gate_ref is not None:
                gate_ref[into, :] = jnp.broadcast_to(jnp.sum(gate, axis=1, keepdims=True), (LANES, LANES))

        @pl.when(width > WINDOWS[-1])
        def _():
            self.await_tokens(self.spans)

            @pl.loop(0, 2)
            def _(half):
                window(half, self.spans, 0)

        for k in WINDOWS:
            @pl.when(width == k)
            def _(k=k):
                starts = [jnp.minimum(self.table_ref[self.at["lo"] + 2 * tile + half], self.spans - 2 * k) for half in range(2)]
                self.await_tokens(jnp.maximum(starts[0], starts[1]) + 2 * k)
                for half in range(2):
                    window(half, 2 * k, starts[half])


def dispatch_scratch(tok):
    return [pltpu.VMEM(tok.shape, tok.dtype), pltpu.SMEM((1,), jnp.int32), pltpu.SemaphoreType.DMA((tok.shape[0] // TILE,))]


def combine_kernel(at, spans, groups, with_gate, table_ref, pos_ref, rows_hbm, *rest):
    if with_gate:
        gate_hbm, out_ref, gout_ref, rows, gates, waited, sems = rest
    else:
        out_ref, rows, waited, sems = rest
    step = pl.program_id(0)
    steps = pl.num_programs(0)
    row_iota = lax.broadcasted_iota(jnp.int32, (LANES, LANES), 0)
    over = table_ref[at["over"] + step]

    def region(g):
        return table_ref[at["first"] + g], table_ref[at["first"] + g + 1]

    def start_of(g, span):
        return pl.multiple_of(table_ref[at["start"][g] + span], 16)

    def block_copies(index):
        into = pl.ds(pl.multiple_of(index * TILE, TILE), TILE)
        copies = [pltpu.make_async_copy(rows_hbm.at[into, :], rows.at[into, :], sems.at[0, index])]
        if with_gate:
            copies.append(pltpu.make_async_copy(gate_hbm.at[into, :], gates.at[into, :], sems.at[1, index]))
        return copies

    @pl.when(step == 0)
    def _():
        for g in range(groups):
            waited[g] = region(g)[0]
        longest = region(0)[1] - region(0)[0]
        for g in range(1, groups):
            longest = jnp.maximum(longest, region(g)[1] - region(g)[0])

        @pl.loop(0, longest)
        def _(index):
            for g in range(groups):
                begin, stop = region(g)

                @pl.when(begin + index < stop)
                def _(begin=begin):
                    for copy in block_copies(begin + index):
                        copy.start()

    for g in range(groups):
        stop = region(g)[1]
        need = jnp.minimum((start_of(g, (step + 1) * GROUP - 1) + LANES + over * LANES + TILE - 1) // TILE, stop)
        need = jnp.where(step == steps - 1, stop, need)

        @pl.loop(waited[g], need)
        def _(index):
            for copy in block_copies(index):
                copy.wait()

        waited[g] = jnp.maximum(waited[g], need)

    def window(q, second):
        span = step * GROUP + q
        hot, data, gdata = [], [], []
        for g in range(groups):
            begin = place = start_of(g, span)
            if second:
                first, stop = region(g)
                place = pl.multiple_of(jnp.where(first == stop, begin, jnp.minimum(begin + LANES, stop * TILE - LANES)), 16)
                begin = begin + LANES
            row = row_iota + place
            match = pos_ref[g, pl.ds(spans[0] + span, 1), :] == row
            if second:
                match = jnp.logical_and(match, row >= begin)
            hot.append(jnp.where(match, 1.0, 0.0).astype(jnp.bfloat16))
            data.append(rows[pl.ds(place, LANES), :])
            if with_gate:
                gdata.append(gates[pl.ds(place, LANES), :])
        hot = jnp.concatenate(hot, axis=0)
        dims = (((0,), (0,)), ((), ()))
        out = lax.dot_general(hot, jnp.concatenate(data, axis=0), dims, preferred_element_type=jnp.float32)
        if not with_gate:
            return out, None
        exact = jnp.concatenate(gdata, axis=0)
        high = exact.astype(jnp.bfloat16)
        low = (exact - high.astype(jnp.float32)).astype(jnp.bfloat16)
        pair = lax.dot_general(hot, jnp.concatenate([high, low], axis=1), dims, preferred_element_type=jnp.float32)
        return out, pair[:, :LANES] + pair[:, LANES:]

    def put(q, wide):
        out, gate = window(q, False)
        if wide:
            out2, gate2 = window(q, True)
            out = out + out2
            gate = gate + gate2 if with_gate else None
        into = pl.ds(q * LANES if isinstance(q, int) else pl.multiple_of(q * LANES, LANES), LANES)
        out_ref[into, :] = out.astype(out_ref.dtype)
        if with_gate:
            gout_ref[into, :] = gate

    @pl.when(over == 0)
    def _():
        for q in range(GROUP):
            put(q, False)

    @pl.when(over != 0)
    def _():
        @pl.loop(0, GROUP)
        def _(q):
            put(q, True)


def combine(layout, chunk, table, pos, rows, gate_rows=None):
    rows_max, dim = rows.shape
    groups = pos.shape[0]
    spans = layout[chunk]["spans"]
    tokens = spans[1] * LANES
    with_gate = gate_rows is not None
    block = GROUP * LANES
    operands, in_specs = [pos, rows], [WHOLE, ANY]
    out_shape = [jax.ShapeDtypeStruct((tokens, dim), jnp.bfloat16)]
    out_specs = [pl.BlockSpec((block, dim), lambda t, *_: (t, 0))]
    scratch = [pltpu.VMEM((rows_max, dim), jnp.bfloat16)]
    if with_gate:
        operands.append(gate_rows)
        in_specs.append(ANY)
        out_shape.append(jax.ShapeDtypeStruct((tokens, LANES), jnp.float32))
        out_specs.append(pl.BlockSpec((block, LANES), lambda t, *_: (t, 0)))
        scratch.append(pltpu.VMEM((rows_max, LANES), jnp.float32))
    scratch += [pltpu.SMEM((groups,), jnp.int32), pltpu.SemaphoreType.DMA((2, rows_max // TILE))]
    kernel = functools.partial(combine_kernel, layout[chunk], spans, groups, with_gate)
    return call(kernel, table, operands, in_specs, out_shape, out_specs, scratch, (9 * 10**9, 35 * 10**6), (tokens // block,))


class WeightStream:
    def __init__(self, at, table_ref, weights, scratch):
        self.at, self.table_ref, self.own, self.helped = at, table_ref, weights[:3], weights[3:]
        self.wide, self.down, self.sems = scratch
        self.experts, _, self.ffn = weights[0].shape

    def copies(self, sources, s):
        wg, wu, wd = sources
        return (
            pltpu.make_async_copy(wg, self.wide.at[s, :, pl.ds(0, self.ffn)], self.sems.at[s, 0]),
            pltpu.make_async_copy(wu, self.wide.at[s, :, pl.ds(self.ffn, self.ffn)], self.sems.at[s, 1]),
            pltpu.make_async_copy(wd, self.down.at[s], self.sems.at[s, 2]),
        )

    def start(self, group, s):
        @pl.when(jnp.logical_and(group >= 0, group < self.experts))
        def _():
            for copy in self.copies([w.at[group] for w in self.own], s):
                copy.start()

        @pl.when(group == self.experts)
        def _():
            for copy in self.copies([w.at[0] for w in self.helped], s):
                copy.start()

    def begin(self):
        self.start(self.table_ref[self.at["group"]], 0)

    def slot(self):
        tile = pl.program_id(0)
        s = table_slot = self.table_ref[self.at["slot"] + tile]

        @pl.when(self.table_ref[self.at["fresh"] + tile] != 0)
        def _():
            self.start(self.table_ref[self.at["next"] + tile], 1 - table_slot)
            for copy in self.copies([w.at[0] for w in self.own], table_slot):
                copy.wait()

        return s


def run_tiles(at, table_ref, tile_body, piped_in, piped_out):
    pltpu.emit_pipeline(
        tile_body, grid=(table_ref[at["count"]],),
        in_specs=[row_block(ref.shape[1]) for ref in piped_in],
        out_specs=[row_block(ref.shape[1]) for ref in piped_out],
    )(*piped_in, *piped_out)


def forward_kernel(at, table_ref, pos_ref, prob_ref, tok_hbm, *rest):
    stream = WeightStream(at, table_ref, rest[:6], rest[11:14])
    dispatch = Dispatch(at, table_ref, pos_ref, prob_ref, tok_hbm, rest[14:])
    wide, down, ffn = stream.wide, stream.down, stream.ffn
    dispatch.begin()
    stream.begin()

    def tile_body(x_ref, gate_ref, ab_ref, h_ref, out_ref):
        dispatch.tile(x_ref, gate_ref)
        slot = stream.slot()
        x = x_ref[...]
        for j in range(ffn // LANES):
            cols = slice(j * LANES, (j + 1) * LANES)
            ucols = slice(ffn + j * LANES, ffn + (j + 1) * LANES)
            both = jnp.dot(x, jnp.concatenate([wide[slot, :, cols], wide[slot, :, ucols]], axis=1), preferred_element_type=jnp.float32)
            a, b = both[:, :LANES], both[:, LANES:]
            ab_ref[:, cols] = a
            ab_ref[:, ucols] = b
            h_ref[:, cols] = (a * jax.nn.sigmoid(a) * b).astype(h_ref.dtype)
        out = jnp.dot(h_ref[...], down[slot], preferred_element_type=jnp.float32)
        gate = gate_ref[...]
        for j in range(out.shape[1] // LANES):
            cols = slice(j * LANES, (j + 1) * LANES)
            out_ref[:, cols] = (out[:, cols] * gate).astype(out_ref.dtype)

    run_tiles(at, table_ref, tile_body, (), rest[6:11])
    dispatch.end()


def backward_kernel(at, table_ref, pos_ref, tok_hbm, ab_hbm, h_hbm, gate_hbm, *rest):
    stream = WeightStream(at, table_ref, rest[:6], rest[10:13])
    m_ref = rest[13]
    dispatch = Dispatch(at, table_ref, pos_ref, None, tok_hbm, rest[14:])
    wide, down, ffn = stream.wide, stream.down, stream.ffn
    trans = (((1,), (1,)), ((), ()))
    dispatch.begin()
    stream.begin()

    def tile_body(ab_ref, h_ref, gate_ref, d_ref, in_ref, mg_ref, dgate_ref):
        dispatch.tile(m_ref)
        slot = stream.slot()
        m = m_ref[...]
        gate = gate_ref[...]
        dgate = jnp.zeros(gate.shape, jnp.float32)
        for c in range(0, ffn, 2 * LANES):
            width = min(2 * LANES, ffn - c)
            raw = lax.dot_general(m, down[slot, c:c + width, :], trans, preferred_element_type=jnp.float32)
            for k in range(width // LANES):
                lo = c + k * LANES
                cols = slice(lo, lo + LANES)
                ucols = slice(ffn + lo, ffn + lo + LANES)
                g = raw[:, k * LANES:(k + 1) * LANES]
                a, b = ab_ref[:, cols], ab_ref[:, ucols]
                sig = jax.nn.sigmoid(a)
                hidden_grad = g * gate
                d_ref[:, cols] = (hidden_grad * b * sig * (1.0 + a * (1.0 - sig))).astype(d_ref.dtype)
                d_ref[:, ucols] = (hidden_grad * (a * sig)).astype(d_ref.dtype)
                dgate = dgate + g * h_ref[:, cols].astype(jnp.float32)
        in_ref[...] = lax.dot_general(d_ref[...], wide[slot], trans, preferred_element_type=jnp.float32).astype(in_ref.dtype)
        for j in range(m.shape[1] // LANES):
            cols = slice(j * LANES, (j + 1) * LANES)
            mg_ref[:, cols] = (m[:, cols].astype(jnp.float32) * gate).astype(mg_ref.dtype)
        lane = lax.broadcasted_iota(jnp.int32, gate.shape, 1)
        expert = table_ref[at["expert"] + table_ref[at["group"] + pl.program_id(0)]]
        dgate_ref[...] = jnp.where(lane == expert, jnp.sum(dgate, axis=1, keepdims=True), 0.0)

    run_tiles(at, table_ref, tile_body, (ab_hbm, h_hbm, gate_hbm), rest[6:10])
    dispatch.end()


def weight_scratch(wg):
    _, dim, ffn = wg.shape
    return [
        pltpu.VMEM((2, dim, 2 * ffn), wg.dtype),
        pltpu.VMEM((2, ffn, dim), wg.dtype),
        pltpu.SemaphoreType.DMA((2, 3)),
    ]


def shapes(rows_max, *kinds):
    return [jax.ShapeDtypeStruct((rows_max, width), dtype) for width, dtype in kinds]


def forward(layout, chunk, table, pos, prob, tok, weights):
    _, dim, ffn = weights[0].shape
    kinds = ((dim, jnp.bfloat16), (LANES, jnp.float32), (2 * ffn, jnp.float32), (ffn, jnp.bfloat16), (dim, jnp.bfloat16))
    at = layout[chunk]
    return call(
        functools.partial(forward_kernel, at), table, (pos, prob, tok, *weights), [WHOLE, WHOLE] + [ANY] * 7,
        shapes(at["rows_max"], *kinds), [ANY] * 5, weight_scratch(weights[0]) + dispatch_scratch(tok), (75 * 10**9, 150 * 10**6),
    )


def backward(layout, chunk, table, pos, tok, ab, hidden, gates, weights):
    _, dim, ffn = weights[0].shape
    kinds = ((2 * ffn, jnp.bfloat16), (dim, jnp.bfloat16), (dim, jnp.bfloat16), (LANES, jnp.float32))
    at = layout[chunk]
    scratch = [*weight_scratch(weights[0]), pltpu.VMEM((TILE, dim), jnp.bfloat16), *dispatch_scratch(tok)]
    return call(
        functools.partial(backward_kernel, at), table, (pos, tok, ab, hidden, gates, *weights), [WHOLE] + [ANY] * 10,
        shapes(at["rows_max"], *kinds), [ANY] * 4, scratch, (75 * 10**9, 150 * 10**6),
    )


def weight_grad_kernel(at, tiles_max, outs, table_ref, *rest):
    lhs_hbm, rhs_hbm = rest[:CHUNKS], rest[CHUNKS:2 * CHUNKS]
    own_out, helped_out = rest[2 * CHUNKS:2 * CHUNKS + outs], rest[2 * CHUNKS + outs:2 * CHUNKS + 2 * outs]
    lhs, rhs, lhs_t, acc, staged, pending, sems, out_sems = rest[2 * CHUNKS + 2 * outs:]
    experts = own_out[0].shape[0]
    steps = table_ref[at["steps"]]

    def copies(chunk, row, s, half):
        source = pl.ds(pl.multiple_of(row, TILE), TILE)
        into = pl.ds(half * TILE, TILE)
        return (
            pltpu.make_async_copy(lhs_hbm[chunk].at[source, :], lhs.at[s, into, :], sems.at[s, half, 0]),
            pltpu.make_async_copy(rhs_hbm[chunk].at[source, :], rhs.at[s, into, :], sems.at[s, half, 1]),
        )

    def start(index, s):
        for half in range(2):
            src = table_ref[at["src"] + 2 * index + half]
            for chunk in range(CHUNKS):
                @pl.when(jnp.logical_and(src >= chunk * tiles_max, src < (chunk + 1) * tiles_max))
                def _(chunk=chunk, src=src, half=half):
                    for copy in copies(chunk, (src - chunk * tiles_max) * TILE, s, half):
                        copy.start()

    def out_copies(targets):
        return [pltpu.make_async_copy(staged.at[i], target, out_sems.at[i]) for i, target in enumerate(targets)]

    def drain():
        @pl.when(pending[0] != 0)
        def _():
            for copy in out_copies([out.at[0] for out in own_out]):
                copy.wait()

        pending[0] = 0

    pending[0] = 0
    start(0, 0)

    def accumulate(slot, fresh, depth):
        lhs_t[:, :depth] = jnp.transpose(lhs[slot, :depth, :], (1, 0))
        block = 2 * LANES
        for c in range(0, acc.shape[1], block):
            part = jnp.dot(lhs_t[:, :depth], rhs[slot, :depth, c:c + block], preferred_element_type=jnp.float32)
            acc[:, c:c + block] = jnp.where(fresh, 0.0, acc[:, c:c + block]) + part

    @pl.loop(0, steps)
    def _(step):
        slot = lax.rem(step, 2)
        group = table_ref[at["owner"] + step]

        @pl.when(step + 1 < steps)
        def _():
            start(step + 1, 1 - slot)

        fresh = jnp.logical_or(step == 0, group != table_ref[at["owner"] + jnp.maximum(step - 1, 0)])
        last = jnp.logical_or(step == steps - 1, group != table_ref[at["owner"] + step + 1])
        pair = table_ref[at["src"] + 2 * step + 1] >= 0
        for copy in copies(0, 0, slot, 0):
            copy.wait()

        @pl.when(pair)
        def _():
            for copy in copies(0, 0, slot, 1):
                copy.wait()
            accumulate(slot, fresh, 2 * TILE)

        @pl.when(jnp.logical_not(pair))
        def _():
            accumulate(slot, fresh, TILE)

        @pl.when(last)
        def _():
            drain()
            width = acc.shape[1] // outs
            for i in range(outs):
                staged[i, :, :] = acc[:, i * width:(i + 1) * width].astype(staged.dtype)

            @pl.when(group < experts)
            def _():
                for copy in out_copies([out.at[group] for out in own_out]):
                    copy.start()

            @pl.when(group == experts)
            def _():
                for copy in out_copies([out.at[0] for out in helped_out]):
                    copy.start()

            pending[0] = 1

    drain()


def weight_grad(layout, table, lhs, rhs, experts, outs):
    left, right = lhs[0].shape[1], rhs[0].shape[1]
    width = right // outs
    kernel = functools.partial(weight_grad_kernel, layout["grad"], layout["tiles_max"], outs)
    scratch = [
        pltpu.VMEM((2, 2 * TILE, left), jnp.bfloat16),
        pltpu.VMEM((2, 2 * TILE, right), jnp.bfloat16),
        pltpu.VMEM((left, 2 * TILE), jnp.bfloat16),
        pltpu.VMEM((left, right), jnp.float32),
        pltpu.VMEM((outs, left, width), jnp.bfloat16),
        pltpu.SMEM((1,), jnp.int32),
        pltpu.SemaphoreType.DMA((2, 2, 2)),
        pltpu.SemaphoreType.DMA((outs,)),
    ]
    out_shape = [jax.ShapeDtypeStruct((n, left, width), jnp.bfloat16) for n in [experts] * outs + [1] * outs]
    return call(
        kernel, table, (*lhs, *rhs), [ANY] * (2 * CHUNKS), out_shape, [ANY] * len(out_shape),
        scratch, (2 * 9000 * left * right, 100 * 10**6),
    )


def insert_kernel(at, size, table_ref, *rest):
    back, outs, staged, sems = rest[:size], rest[2 * size:3 * size], rest[3 * size:4 * size], rest[4 * size]
    place = table_ref[at]

    @pl.when(place >= 0)
    def _():
        fetch = [pltpu.make_async_copy(b.at[0], s, sems.at[0, i]) for i, (b, s) in enumerate(zip(back, staged))]
        store = [pltpu.make_async_copy(s, out.at[place], sems.at[1, i]) for i, (s, out) in enumerate(zip(staged, outs))]
        for copy in fetch:
            copy.start()
        for i in range(size):
            fetch[i].wait()
            store[i].start()
        for copy in store:
            copy.wait()


def insert(layout, table, back, grads):
    size = len(grads)
    return pl.pallas_call(
        functools.partial(insert_kernel, layout["insert"], size),
        grid_spec=pltpu.PrefetchScalarGridSpec(
            num_scalar_prefetch=1,
            in_specs=[ANY] * (2 * size),
            out_specs=[ANY] * size,
            scratch_shapes=[pltpu.VMEM(g.shape[1:], g.dtype) for g in grads] + [pltpu.SemaphoreType.DMA((2, size))],
        ),
        out_shape=[jax.ShapeDtypeStruct(g.shape, g.dtype) for g in grads],
        input_output_aliases={1 + size + i: i for i in range(size)},
        compiler_params=pltpu.CompilerParams(vmem_limit_bytes=VMEM_LIMIT),
        cost_estimate=pl.CostEstimate(flops=10**9, bytes_accessed=15 * 10**6 * size, transcendentals=0),
        name="insert",
    )(table, *back, *grads)


def below(size, strict):
    i = lax.broadcasted_iota(jnp.int32, (size, size), 0)
    j = lax.broadcasted_iota(jnp.int32, (size, size), 1)
    return (i < j if strict else i <= j).astype(jnp.float32)


def running(values):
    size = values.shape[-1]
    i = lax.broadcasted_iota(jnp.int32, (size, size), 0)
    j = lax.broadcasted_iota(jnp.int32, (size, size), 1)
    return jnp.sum(jnp.where(i <= j, values[..., :, None], 0), axis=-2)


def count(condition, axis):
    return jnp.sum(condition.astype(jnp.int32), axis=axis)


def choose_swap(tiles, experts):
    none = jnp.zeros((1,), jnp.int32)
    options = [jnp.concatenate([none, tiles[:experts]]), jnp.concatenate([none, tiles[experts:]])]
    gap = jnp.sum(tiles[:experts]) - jnp.sum(tiles[experts:])
    left = jnp.abs(gap - 2 * options[0][:, None] + 2 * options[1][None, :])
    index = lax.broadcasted_iota(jnp.int32, left.shape, 0) * (experts + 1) + lax.broadcasted_iota(jnp.int32, left.shape, 1)
    best = jnp.min(jnp.where(left == jnp.min(left), index, left.size))
    return best // (experts + 1) - 1, best % (experts + 1) - 1


def routing(hot, experts_of, place):
    groups, span_total, _ = hot.shape
    spans_of = [part * (span_total * LANES // sum(PARTS)) // LANES for part in PARTS]
    firsts = [sum(spans_of[:c]) for c in range(CHUNKS)]
    chunk_of = jnp.concatenate([jnp.full((n,), c, jnp.int32) for c, n in enumerate(spans_of)])
    member = chunk_of[:, None] == jnp.arange(CHUNKS, dtype=jnp.int32)[None, :]
    same = chunk_of[:, None] == chunk_of[None, :]
    tiles_of = [2 * n * LANES // TILE + groups for n in spans_of]
    tiles_max = max(tiles_of)

    within = jnp.einsum("gsi,ij->gsj", hot, below(LANES, False), preferred_element_type=jnp.float32)
    span_count = jnp.sum(hot, axis=-1)
    before = jnp.einsum("gi,ij->gj", span_count, jnp.where(same, below(span_total, True), 0.0), preferred_element_type=jnp.float32)
    total = jnp.sum(jnp.where(member[:, None, :], span_count.T[:, :, None], 0.0), axis=0).T.astype(jnp.int32)
    tiles = (total + TILE - 1) // TILE
    none = jnp.logical_and(jnp.sum(tiles, axis=1, keepdims=True) == 0, jnp.arange(groups, dtype=jnp.int32) == 0)
    tiles = jnp.where(none, 1, tiles)
    stop = running(tiles)
    begin = stop - tiles

    def to_spans(values):
        return jnp.sum(jnp.where(member[None], values.T[:, None, :], 0), axis=2)

    span_first = to_spans(begin) * TILE + before.astype(jnp.int32)
    span_stop = span_first + span_count.astype(jnp.int32)
    pos = jnp.where(hot > 0, span_first[:, :, None] + within.astype(jnp.int32) - 1, -1)

    index = jnp.arange(groups, dtype=jnp.int32)
    tile = jnp.arange(tiles_max, dtype=jnp.int32)
    group = jnp.minimum(count(tile[None, :, None] >= stop[:, None, :], 2), groups - 1)
    mine = group[:, :, None] == index
    ordinal = running((tiles > 0).astype(jnp.int32)) - 1
    later = jnp.logical_and(index[None, None, :] > group[:, :, None], tiles[:, None, :] > 0)
    follow = jnp.min(jnp.where(later, index, groups), axis=2)
    follow = jnp.where(follow == groups, -1, follow)
    fresh = jnp.sum(jnp.where(mine, begin[:, None, :], 0), axis=2) == tile
    slot = jnp.sum(jnp.where(mine, ordinal[:, None, :], 0), axis=2) % 2

    half_mine = jnp.repeat(mine, 2, axis=1)
    stops = jnp.sum(jnp.where(half_mine[..., None], span_stop[None, None], 0), axis=2)
    row0 = jnp.arange(2 * tiles_max, dtype=jnp.int32)[None, :, None] * LANES
    inside = member.T[:, None, :]
    lo = count(jnp.logical_and(inside, stops <= row0), 2)
    hi = jnp.minimum(count(jnp.logical_and(inside, stops < row0 + LANES), 2), jnp.array(spans_of, jnp.int32)[:, None] - 1)
    width = jnp.maximum(jnp.max(((hi - lo + 2) // 2).reshape(CHUNKS, tiles_max, 2), axis=2), 1)
    start = jnp.minimum(span_first // 16 * 16, to_spans(stop) * TILE - LANES)
    empty = to_spans(tiles) == 0
    leading = jnp.logical_and(jnp.logical_not(empty), to_spans(ordinal) == 0)
    start = jnp.where(empty, jnp.sum(jnp.where(leading, start, 0), axis=0), start)
    over = jnp.any(jnp.logical_and(jnp.logical_not(empty), span_stop - start > LANES), axis=0)
    over = jnp.any(over.reshape(-1, GROUP), axis=1)

    in_chunks = running(tiles.T)
    both = in_chunks[:, -1]
    step_stop = running((both + 1) // 2)
    step_first = step_stop - (both + 1) // 2
    steps = CHUNKS * tiles_max // 2 + groups
    step = jnp.arange(steps, dtype=jnp.int32)
    owner = jnp.minimum(count(step[:, None] >= step_stop[None, :], 1), groups - 1)
    step_mine = owner[:, None] == index

    def of_step(values):
        return jnp.sum(jnp.where(step_mine[:, :, None], values[None], 0), axis=1)[:, None, :]

    local = 2 * (step - of_step(step_first[:, None])[:, 0, 0])[:, None, None] + jnp.arange(2, dtype=jnp.int32)[None, :, None]
    ends, sizes = of_step(in_chunks), of_step(tiles.T)
    offset = local - (ends - sizes)
    found = jnp.logical_and(offset >= 0, local < ends)
    chunk_at = jnp.arange(CHUNKS, dtype=jnp.int32) * tiles_max
    src = jnp.sum(jnp.where(found, of_step(begin.T) + offset + chunk_at + 1, 0), axis=2) - 1

    sections = (
        ("expert", experts_of), ("insert", place.reshape(1)), ("steps", step_stop[-1:]), ("owner", owner), ("src", src),
        ("count", stop[:, -1:]), ("group", group), ("slot", slot), ("fresh", fresh), ("next", follow), ("lo", lo), ("width", width),
        ("first", jnp.concatenate([jnp.zeros((CHUNKS, 1), jnp.int32), stop], axis=1)), ("start", start), ("over", over),
    )
    table = jnp.concatenate([values.reshape(-1).astype(jnp.int32) for _, values in sections])
    places, sizes_of, at = {}, {}, 0
    for name, values in sections:
        places[name], sizes_of[name] = at, values.size
        at += values.size
    layout = {}
    for c in range(CHUNKS):
        layout[c] = {name: places[name] + c * (sizes_of[name] // CHUNKS) for name in ("count", "group", "slot", "fresh", "next", "lo", "width", "first")}
        layout[c] |= {
            "expert": places["expert"], "spans": (firsts[c], spans_of[c]), "rows_max": tiles_of[c] * TILE,
            "start": [places["start"] + g * span_total + firsts[c] for g in range(groups)],
            "over": places["over"] + firsts[c] // GROUP,
        }
    layout |= {"grad": {name: places[name] for name in ("steps", "owner", "src")}, "insert": places["insert"], "tiles_max": tiles_max}
    return pos, table, layout


def solution(mesh):
    tp_size = mesh.shape["tp"]
    ep_size = mesh.shape["ep"]
    dev_count = tp_size * ep_size
    rows_axes = ("ep", "tp")
    row_spec = P(rows_axes, None)
    wide_spec = P("ep", None, "tp")
    down_spec = P("ep", "tp", None)
    swap = [(0, 1), (1, 0)]

    def body(x, y_grad, expert_ids, norm_gain, w_router, w_gate, w_up, w_down):
        tokens, model_dim = x.shape
        top_k = expert_ids.shape[1]
        num_experts = w_router.shape[1]
        local_experts = w_gate.shape[0]
        total_tokens = tokens * dev_count
        my_ep = lax.axis_index("ep").astype(jnp.int32)
        firsts = [sum(PARTS[:c]) for c in range(CHUNKS)]

        def of_chunk(rows, c, axis=0):
            return lax.slice_in_dim(rows, firsts[c], firsts[c] + PARTS[c], axis=axis)

        def gather(rows):
            return lax.all_gather(rows, rows_axes, axis=0, tiled=True)

        def scatter(rows):
            return lax.psum_scatter(rows, rows_axes, scatter_dimension=0, tiled=True)

        def after(values, first):
            return lax.optimization_barrier((values, first))

        x_float = x.astype(jnp.float32)
        inv_rms = lax.rsqrt(jnp.mean(x_float * x_float, axis=-1, keepdims=True) + NORM_EPS)
        unit = x_float * inv_rms
        gain = norm_gain.astype(jnp.float32)
        x_norm = (unit * gain).astype(jnp.bfloat16)
        tok = [gather(of_chunk(x_norm, c)) for c in range(CHUNKS)]

        route_prob = jax.nn.softmax(jnp.dot(x_norm, w_router, preferred_element_type=jnp.float32), axis=-1)
        expert_range = jnp.arange(num_experts, dtype=jnp.int32)
        choice = jnp.sum((expert_ids[:, :, None] == expert_range[None, None, :]).astype(jnp.float32), axis=1)
        small = lax.all_gather(jnp.concatenate([choice, route_prob], axis=1).T, rows_axes, axis=0, tiled=False)
        counts = jnp.sum(small[:, :num_experts], axis=(0, 2))
        balance_scale = BALANCE_COEF * num_experts / (total_tokens * total_tokens * top_k)
        balance_loss = balance_scale * jnp.sum(counts * jnp.sum(small[:, num_experts:], axis=(0, 2)))

        rows_in = jnp.stack([jnp.sum(of_chunk(small[:, :num_experts], c, 2), axis=(0, 2)) for c in range(CHUNKS)])
        tiles_in = jnp.sum((rows_in.astype(jnp.int32) + TILE - 1) // TILE, axis=0)
        gives = choose_swap(tiles_in, local_experts)
        given = jnp.where(my_ep == 0, gives[0], gives[1])
        taken = jnp.where(my_ep == 0, gives[1], gives[0])
        my_base = my_ep * local_experts
        local = jnp.arange(local_experts, dtype=jnp.int32)
        group_experts = jnp.concatenate([my_base + local, (local_experts - my_base + jnp.maximum(taken, 0)).reshape(1)])
        active = jnp.concatenate([local != given, (taken >= 0).reshape(1)])
        take = jnp.logical_and(group_experts[:, None] == expert_range, active[:, None])
        spread = jnp.concatenate([of_chunk(small, c, 2).transpose(1, 0, 2).reshape(2 * num_experts, -1) for c in range(CHUNKS)], axis=1)
        spread = spread.reshape(2, 1, num_experts, -1, LANES)
        own = jnp.sum(jnp.where(take[None, :, :, None, None], spread, 0.0), axis=2)
        prob = own[1]
        pos, table, layout = routing(own[0], group_experts, given)
        helped = [lax.ppermute(lax.dynamic_slice_in_dim(w, jnp.maximum(given, 0), 1, axis=0), "ep", swap) for w in (w_gate, w_up, w_down)]
        weights = (w_gate, w_up, w_down, *helped)

        grad_scale = 2.0 * ACT_COEF / (total_tokens * model_dim)
        x_rows, gate_rows, pre, hidden, d_rows, mg_rows = [], [], [], [], [], []
        out_raw, moe_out, m_own, m_tok, in_raw, gate_part = [], [], [], [], [], []

        def send_cotangent(c, gate):
            raw, (gate, _) = after(out_raw[c], (gate, m_own[-1:]))
            moe_out.append(raw.astype(jnp.float32))
            moe_grad = of_chunk(y_grad, c).astype(jnp.float32) + grad_scale * moe_out[c]
            m_own.append(moe_grad.astype(jnp.bfloat16))
            m_tok.append(gather(m_own[c]))
            return gate

        for c in range(CHUNKS):
            rows, gates, ab, h, out_rows = forward(layout, c, table, pos, prob, tok[c], weights)
            (partial,) = combine(layout, c, table, pos, out_rows)
            if c == 0:
                partial, tok[1:] = after(partial, tok[1:])
            else:
                partial = send_cotangent(c - 1, partial)
            out_raw.append(scatter(partial))
            x_rows.append(rows)
            gate_rows.append(gates)
            pre.append(ab)
            hidden.append(h)
        for c in range(CHUNKS):
            d, in_rows, mg, dgate = backward(layout, c, table, pos, m_tok[c], pre[c], hidden[c], gate_rows[c], weights)
            if c == 0:
                in_rows = send_cotangent(CHUNKS - 1, in_rows)
            partial, gate_tok = combine(layout, c, table, pos, in_rows, dgate)
            if c == 0:
                partial, m_tok[-1] = after(partial, m_tok[-1])
            in_raw.append(scatter(partial))
            gate_part.append(gate_tok[:, :num_experts])
            d_rows.append(d)
            mg_rows.append(mg)
        *wide_grads, helped_gate, helped_up = weight_grad(layout, table, x_rows, d_rows, local_experts, 2)
        back = [lax.ppermute(g, "ep", swap) for g in (helped_gate, helped_up)]

        sums = jnp.concatenate([g.reshape(dev_count, -1) for g in gate_part], axis=1)
        sums, _ = after(sums, in_raw[:CHUNKS - 1])
        gate_weight_grad = lax.psum_scatter(sums, rows_axes, scatter_dimension=0, tiled=False)
        gate_weight_grad, (wide_grads, in_raw) = after(gate_weight_grad, (wide_grads, in_raw))
        moe_all = jnp.concatenate(moe_out, axis=0)
        y = (x_float + moe_all).astype(jnp.bfloat16)
        prob_grad = gate_weight_grad.reshape(tokens, num_experts) + balance_scale * counts[None, :]
        logit_grad = (route_prob * (prob_grad - jnp.sum(route_prob * prob_grad, axis=-1, keepdims=True))).astype(jnp.bfloat16)
        x_norm_grad = jnp.concatenate(in_raw, axis=0).astype(jnp.float32)
        x_norm_grad = x_norm_grad + jnp.einsum("se,de->sd", logit_grad, w_router, preferred_element_type=jnp.float32)
        unit_grad = x_norm_grad * gain
        x_grad = y_grad.astype(jnp.float32) + inv_rms * (unit_grad - unit * jnp.mean(unit_grad * unit, axis=-1, keepdims=True))
        x_grad = x_grad.astype(jnp.bfloat16)
        stats = (
            jnp.sum(x_norm_grad * unit, axis=0),
            jnp.einsum("sd,se->de", x_norm, logit_grad, preferred_element_type=jnp.float32).reshape(-1),
            jnp.sum(moe_all * moe_all).reshape(1),
        )
        size = sum(s.size for s in stats)
        stats = jnp.concatenate([*stats, jnp.zeros((STATS_SIZE - size,), jnp.float32)]).reshape(dev_count, -1)
        gate_grad, up_grad = insert(layout, table, back, wide_grads)
        stats, (mg_rows[0], x_grad, gate_grad) = after(stats, (mg_rows[0], x_grad, gate_grad))
        down_grad, helped_down = weight_grad(layout, table, hidden, mg_rows, local_experts, 1)
        (down_grad,) = insert(layout, table, [lax.ppermute(helped_down, "ep", swap)], [down_grad])
        stats = lax.psum(stats, ("tp", "ep"))
        stats = stats.reshape(-1)
        gain_sum = stats[:model_dim]
        router_sum = stats[model_dim:size - 1].reshape(model_dim, num_experts)
        act_loss = ACT_COEF * stats[size - 1] / (total_tokens * model_dim)
        return (y, x_grad, gain_sum.astype(jnp.bfloat16), router_sum.astype(jnp.bfloat16), gate_grad, up_grad, down_grad, balance_loss, act_loss)

    return jax.shard_map(body, mesh=mesh, in_specs=(row_spec, row_spec, row_spec, P(), P(), wide_spec, wide_spec, down_spec), out_specs=(row_spec, row_spec, P(), P(), wide_spec, wide_spec, down_spec, P(), P()), check_vma=False)
```

```python
import functools

import jax
import jax.numpy as jnp
from jax import lax
from jax.experimental import pallas as pl
from jax.experimental.pallas import tpu as pltpu
from jax.sharding import PartitionSpec as P


NORM_EPS = 1e-6
ACT_COEF = 1e-5
BALANCE_COEF = 1e-3
TILE = 256
LANES = 128
GROUP = 4
REACH = 96
PARTS = (384, 256, 384)
CHUNKS = len(PARTS)
WINDOWS = (1, 2, 3, 4)
VMEM_LIMIT = 67_043_328


def call(kernel, table, operands, in_specs, out_shape, out_specs, scratch, cost, grid=()):
    return pl.pallas_call(
        kernel,
        grid_spec=pltpu.PrefetchScalarGridSpec(
            num_scalar_prefetch=1, grid=grid, in_specs=in_specs, out_specs=out_specs, scratch_shapes=scratch
        ),
        out_shape=out_shape,
        compiler_params=pltpu.CompilerParams(vmem_limit_bytes=VMEM_LIMIT),
        cost_estimate=pl.CostEstimate(flops=cost[0], bytes_accessed=cost[1], transcendentals=0),
    )(table, *operands)


ANY = pl.BlockSpec(memory_space=pl.ANY)
WHOLE = pl.BlockSpec(memory_space=pltpu.VMEM)


def row_block(width):
    return pl.BlockSpec((TILE, width), lambda t: (t, 0))


class Dispatch:
    def __init__(self, at, place, table_ref, pos_ref, prob_ref, tok_hbm, scratch):
        self.at, self.table_ref, self.pos_ref, self.prob_ref, self.tok_hbm = at, table_ref, pos_ref, prob_ref, tok_hbm
        self.tok, self.waited, self.sems = scratch
        self.first, self.spans = at["spans"]
        self.offset, self.stride = place
        self.part = at["part"]

    def span_copy(self, index, row):
        into = pl.ds(index * LANES if isinstance(index, int) else pl.multiple_of(index * LANES, LANES), LANES)
        return pltpu.make_async_copy(self.tok_hbm.at[pl.ds(row, LANES), :], self.tok.at[into, :], self.sems.at[index])

    def begin(self):
        self.waited[0] = 0
        for index in range(self.spans):
            device, token = divmod(index * LANES, self.part)
            self.span_copy(index, device * self.stride + self.offset + token).start()

    def await_tokens(self, stop_span):
        @pl.loop(self.waited[0], stop_span)
        def _(index):
            self.span_copy(index, 0).wait()

        self.waited[0] = jnp.maximum(self.waited[0], stop_span)

    def end(self):
        self.await_tokens(self.spans)

    def tile(self, x_ref, gate_ref=None):
        tile = pl.program_id(0)
        group = self.table_ref[self.at["group"] + tile]
        width = self.table_ref[self.at["width"] + tile]

        def window(half, count, start):
            row_id = lax.broadcasted_iota(jnp.int32, (LANES, LANES), 0) + (tile * TILE + half * LANES)
            into = pl.ds(half * LANES if isinstance(half, int) else pl.multiple_of(half * LANES, LANES), LANES)
            hot, gate = [], jnp.zeros((LANES, LANES), jnp.float32)
            for q in range(count):
                span = pl.ds(self.first + start + q, 1)
                match = self.pos_ref[group, span, :] == row_id
                hot.append(jnp.where(match, 1.0, 0.0).astype(jnp.bfloat16))
                if gate_ref is not None:
                    gate = gate + jnp.where(match, self.prob_ref[group, span, :], 0.0)
            rows = self.tok[pl.ds(pl.multiple_of(start * LANES, LANES), count * LANES), :]
            out = jnp.dot(jnp.concatenate(hot, axis=1), rows, preferred_element_type=jnp.float32)
            x_ref[into, :] = out.astype(x_ref.dtype)
            if gate_ref is not None:
                gate_ref[into, :] = jnp.broadcast_to(jnp.sum(gate, axis=1, keepdims=True), (LANES, LANES))

        @pl.when(width > WINDOWS[-1])
        def _():
            self.await_tokens(self.spans)

            @pl.loop(0, 2)
            def _(half):
                window(half, self.spans, 0)

        for k in WINDOWS:
            @pl.when(width == k)
            def _(k=k):
                starts = [jnp.minimum(self.table_ref[self.at["lo"] + 2 * tile + half], self.spans - 2 * k) for half in range(2)]
                self.await_tokens(jnp.maximum(starts[0], starts[1]) + 2 * k)
                for half in range(2):
                    window(half, 2 * k, starts[half])


def dispatch_scratch(at, tok):
    spans = at["spans"][1]
    return [pltpu.VMEM((spans * LANES, tok.shape[1]), tok.dtype), pltpu.SMEM((1,), jnp.int32), pltpu.SemaphoreType.DMA((spans,))]


def combine_kernel(at, spans, groups, with_gate, table_ref, pos_ref, rows_hbm, *rest):
    if with_gate:
        gate_hbm, out_ref, gout_ref, rows, gates, waited, sems = rest
    else:
        out_ref, rows, waited, sems = rest
    step = pl.program_id(0)
    steps = pl.num_programs(0)
    row_iota = lax.broadcasted_iota(jnp.int32, (REACH, LANES), 0)
    over = table_ref[at["over"] + step]

    def region(g):
        return table_ref[at["first"] + g], table_ref[at["first"] + g + 1]

    def start_of(g, span):
        return pl.multiple_of(table_ref[at["start"][g] + span], 16)

    def block_copies(index):
        into = pl.ds(pl.multiple_of(index * TILE, TILE), TILE)
        copies = [pltpu.make_async_copy(rows_hbm.at[into, :], rows.at[into, :], sems.at[0, index])]
        if with_gate:
            copies.append(pltpu.make_async_copy(gate_hbm.at[into, :], gates.at[into, :], sems.at[1, index]))
        return copies

    @pl.when(step == 0)
    def _():
        for g in range(groups):
            waited[g] = region(g)[0]
        longest = region(0)[1] - region(0)[0]
        for g in range(1, groups):
            longest = jnp.maximum(longest, region(g)[1] - region(g)[0])

        @pl.loop(0, longest)
        def _(index):
            for g in range(groups):
                begin, stop = region(g)

                @pl.when(begin + index < stop)
                def _(begin=begin):
                    for copy in block_copies(begin + index):
                        copy.start()

    for g in range(groups):
        stop = region(g)[1]
        need = jnp.minimum((start_of(g, (step + 1) * GROUP - 1) + REACH + over * REACH + TILE - 1) // TILE, stop)
        need = jnp.where(step == steps - 1, stop, need)

        @pl.loop(waited[g], need)
        def _(index):
            for copy in block_copies(index):
                copy.wait()

        waited[g] = jnp.maximum(waited[g], need)

    def window(q, second):
        span = step * GROUP + q
        hot, data, gdata = [], [], []
        for g in range(groups):
            begin = place = start_of(g, span)
            if second:
                first, stop = region(g)
                place = pl.multiple_of(jnp.where(first == stop, begin, jnp.minimum(begin + REACH, stop * TILE - REACH)), 16)
                begin = begin + REACH
            row = row_iota + place
            match = pos_ref[g, pl.ds(spans[0] + span, 1), :] == row
            if second:
                match = jnp.logical_and(match, row >= begin)
            hot.append(jnp.where(match, 1.0, 0.0).astype(jnp.bfloat16))
            data.append(rows[pl.ds(place, REACH), :])
            if with_gate:
                gdata.append(gates[pl.ds(place, REACH), :])
        hot = jnp.concatenate(hot, axis=0)
        dims = (((0,), (0,)), ((), ()))
        out = lax.dot_general(hot, jnp.concatenate(data, axis=0), dims, preferred_element_type=jnp.float32)
        if not with_gate:
            return out, None
        exact = jnp.concatenate(gdata, axis=0)
        high = exact.astype(jnp.bfloat16)
        low = (exact - high.astype(jnp.float32)).astype(jnp.bfloat16)
        pair = lax.dot_general(hot, jnp.concatenate([high, low], axis=1), dims, preferred_element_type=jnp.float32)
        return out, pair[:, :LANES] + pair[:, LANES:]

    def put(q, wide):
        out, gate = window(q, False)
        if wide:
            out2, gate2 = window(q, True)
            out = out + out2
            gate = gate + gate2 if with_gate else None
        into = pl.ds(q * LANES if isinstance(q, int) else pl.multiple_of(q * LANES, LANES), LANES)
        out_ref[into, :] = out.astype(out_ref.dtype)
        if with_gate:
            gout_ref[into, :] = gate

    @pl.when(over == 0)
    def _():
        for q in range(GROUP):
            put(q, False)

    @pl.when(over != 0)
    def _():
        @pl.loop(0, GROUP)
        def _(q):
            put(q, True)


def combine(layout, chunk, table, pos, rows, gate_rows=None):
    rows_max, dim = rows.shape
    groups = pos.shape[0]
    spans = layout[chunk]["spans"]
    tokens = spans[1] * LANES
    with_gate = gate_rows is not None
    block = GROUP * LANES
    operands, in_specs = [pos, rows], [WHOLE, ANY]
    out_shape = [jax.ShapeDtypeStruct((tokens, dim), jnp.bfloat16)]
    out_specs = [pl.BlockSpec((block, dim), lambda t, *_: (t, 0))]
    scratch = [pltpu.VMEM((rows_max, dim), jnp.bfloat16)]
    if with_gate:
        operands.append(gate_rows)
        in_specs.append(ANY)
        out_shape.append(jax.ShapeDtypeStruct((tokens, LANES), jnp.float32))
        out_specs.append(pl.BlockSpec((block, LANES), lambda t, *_: (t, 0)))
        scratch.append(pltpu.VMEM((rows_max, LANES), jnp.float32))
    scratch += [pltpu.SMEM((groups,), jnp.int32), pltpu.SemaphoreType.DMA((2, rows_max // TILE))]
    kernel = functools.partial(combine_kernel, layout[chunk], spans, groups, with_gate)
    return call(kernel, table, operands, in_specs, out_shape, out_specs, scratch, (9 * 10**9, 35 * 10**6), (tokens // block,))


class WeightStream:
    def __init__(self, at, table_ref, weights, scratch):
        self.at, self.table_ref, self.own, self.helped = at, table_ref, weights[:3], weights[3:]
        self.wide, self.down, self.sems = scratch
        self.experts, _, self.ffn = weights[0].shape

    def copies(self, sources, s):
        wg, wu, wd = sources
        return (
            pltpu.make_async_copy(wg, self.wide.at[s, :, pl.ds(0, self.ffn)], self.sems.at[s, 0]),
            pltpu.make_async_copy(wu, self.wide.at[s, :, pl.ds(self.ffn, self.ffn)], self.sems.at[s, 1]),
            pltpu.make_async_copy(wd, self.down.at[s], self.sems.at[s, 2]),
        )

    def start(self, group, s):
        @pl.when(jnp.logical_and(group >= 0, group < self.experts))
        def _():
            for copy in self.copies([w.at[group] for w in self.own], s):
                copy.start()

        @pl.when(group == self.experts)
        def _():
            for copy in self.copies([w.at[0] for w in self.helped], s):
                copy.start()

    def begin(self):
        self.start(self.table_ref[self.at["group"]], 0)

    def slot(self):
        tile = pl.program_id(0)
        s = table_slot = self.table_ref[self.at["slot"] + tile]

        @pl.when(self.table_ref[self.at["fresh"] + tile] != 0)
        def _():
            self.start(self.table_ref[self.at["next"] + tile], 1 - table_slot)
            for copy in self.copies([w.at[0] for w in self.own], table_slot):
                copy.wait()

        return s


def run_tiles(at, table_ref, tile_body, piped_in, piped_out):
    pltpu.emit_pipeline(
        tile_body, grid=(table_ref[at["count"]],),
        in_specs=[row_block(ref.shape[1]) for ref in piped_in],
        out_specs=[row_block(ref.shape[1]) for ref in piped_out],
    )(*piped_in, *piped_out)


def forward_kernel(at, place, table_ref, pos_ref, prob_ref, tok_hbm, *rest):
    stream = WeightStream(at, table_ref, rest[:6], rest[11:14])
    dispatch = Dispatch(at, place, table_ref, pos_ref, prob_ref, tok_hbm, rest[14:])
    wide, down, ffn = stream.wide, stream.down, stream.ffn
    dispatch.begin()
    stream.begin()

    def tile_body(x_ref, gate_ref, ab_ref, h_ref, out_ref):
        dispatch.tile(x_ref, gate_ref)
        slot = stream.slot()

        def matmuls(height):
            used = slice(0, height)
            x = x_ref[used, :]
            for j in range(ffn // LANES):
                cols = slice(j * LANES, (j + 1) * LANES)
                ucols = slice(ffn + j * LANES, ffn + (j + 1) * LANES)
                both = jnp.dot(x, jnp.concatenate([wide[slot, :, cols], wide[slot, :, ucols]], axis=1), preferred_element_type=jnp.float32)
                a, b = both[:, :LANES], both[:, LANES:]
                ab_ref[used, cols] = a
                ab_ref[used, ucols] = b
                h_ref[used, cols] = (a * jax.nn.sigmoid(a) * b).astype(h_ref.dtype)
            out = jnp.dot(h_ref[used, :], down[slot], preferred_element_type=jnp.float32)
            gate = gate_ref[used, :]
            for j in range(out.shape[1] // LANES):
                cols = slice(j * LANES, (j + 1) * LANES)
                out_ref[used, cols] = (out[:, cols] * gate).astype(out_ref.dtype)

        half = table_ref[at["half"] + pl.program_id(0)] != 0

        @pl.when(jnp.logical_not(half))
        def _():
            matmuls(TILE)

        @pl.when(half)
        def _():
            matmuls(TILE // 2)
            for ref in (ab_ref, h_ref, out_ref):
                ref[TILE // 2:, :] = jnp.zeros((TILE // 2, ref.shape[1]), ref.dtype)

    run_tiles(at, table_ref, tile_body, (), rest[6:11])
    dispatch.end()


def backward_kernel(at, place, table_ref, pos_ref, tok_hbm, ab_hbm, h_hbm, gate_hbm, *rest):
    stream = WeightStream(at, table_ref, rest[:6], rest[10:13])
    m_ref = rest[13]
    dispatch = Dispatch(at, place, table_ref, pos_ref, None, tok_hbm, rest[14:])
    wide, down, ffn = stream.wide, stream.down, stream.ffn
    trans = (((1,), (1,)), ((), ()))
    dispatch.begin()
    stream.begin()

    def tile_body(ab_ref, h_ref, gate_ref, d_ref, in_ref, mg_ref, dgate_ref):
        dispatch.tile(m_ref)
        slot = stream.slot()
        m = m_ref[...]
        gate = gate_ref[...]
        dgate = jnp.zeros(gate.shape, jnp.float32)
        for c in range(0, ffn, 2 * LANES):
            width = min(2 * LANES, ffn - c)
            raw = lax.dot_general(m, down[slot, c:c + width, :], trans, preferred_element_type=jnp.float32)
            for k in range(width // LANES):
                lo = c + k * LANES
                cols = slice(lo, lo + LANES)
                ucols = slice(ffn + lo, ffn + lo + LANES)
                g = raw[:, k * LANES:(k + 1) * LANES]
                a, b = ab_ref[:, cols], ab_ref[:, ucols]
                sig = jax.nn.sigmoid(a)
                hidden_grad = g * gate
                d_ref[:, cols] = (hidden_grad * b * sig * (1.0 + a * (1.0 - sig))).astype(d_ref.dtype)
                d_ref[:, ucols] = (hidden_grad * (a * sig)).astype(d_ref.dtype)
                dgate = dgate + g * h_ref[:, cols].astype(jnp.float32)
        in_ref[...] = lax.dot_general(d_ref[...], wide[slot], trans, preferred_element_type=jnp.float32).astype(in_ref.dtype)
        for j in range(m.shape[1] // LANES):
            cols = slice(j * LANES, (j + 1) * LANES)
            mg_ref[:, cols] = (m[:, cols].astype(jnp.float32) * gate).astype(mg_ref.dtype)
        lane = lax.broadcasted_iota(jnp.int32, gate.shape, 1)
        expert = table_ref[at["expert"] + table_ref[at["group"] + pl.program_id(0)]]
        dgate_ref[...] = jnp.where(lane == expert, jnp.sum(dgate, axis=1, keepdims=True), 0.0)

    run_tiles(at, table_ref, tile_body, (ab_hbm, h_hbm, gate_hbm), rest[6:10])
    dispatch.end()


def weight_scratch(wg):
    _, dim, ffn = wg.shape
    return [
        pltpu.VMEM((2, dim, 2 * ffn), wg.dtype),
        pltpu.VMEM((2, ffn, dim), wg.dtype),
        pltpu.SemaphoreType.DMA((2, 3)),
    ]


def shapes(rows_max, *kinds):
    return [jax.ShapeDtypeStruct((rows_max, width), dtype) for width, dtype in kinds]


def forward(layout, chunk, table, pos, prob, tokens, weights):
    _, dim, ffn = weights[0].shape
    kinds = ((dim, jnp.bfloat16), (LANES, jnp.float32), (2 * ffn, jnp.float32), (ffn, jnp.bfloat16), (dim, jnp.bfloat16))
    at = layout[chunk]
    tok, place = tokens
    return call(
        functools.partial(forward_kernel, at, place), table, (pos, prob, tok, *weights), [WHOLE, WHOLE] + [ANY] * 7,
        shapes(at["rows_max"], *kinds), [ANY] * 5, weight_scratch(weights[0]) + dispatch_scratch(at, tok), (75 * 10**9, 150 * 10**6),
    )


def backward(layout, chunk, table, pos, tok, ab, hidden, gates, weights):
    _, dim, ffn = weights[0].shape
    kinds = ((2 * ffn, jnp.bfloat16), (dim, jnp.bfloat16), (dim, jnp.bfloat16), (LANES, jnp.float32))
    at = layout[chunk]
    scratch = [*weight_scratch(weights[0]), pltpu.VMEM((TILE, dim), jnp.bfloat16), *dispatch_scratch(at, tok)]
    return call(
        functools.partial(backward_kernel, at, (0, at["part"])), table, (pos, tok, ab, hidden, gates, *weights), [WHOLE] + [ANY] * 10,
        shapes(at["rows_max"], *kinds), [ANY] * 4, scratch, (75 * 10**9, 150 * 10**6),
    )


def weight_grad_kernel(at, tiles_max, outs, table_ref, *rest):
    lhs_hbm, rhs_hbm = rest[:CHUNKS], rest[CHUNKS:2 * CHUNKS]
    own_out, helped_out = rest[2 * CHUNKS:2 * CHUNKS + outs], rest[2 * CHUNKS + outs:2 * CHUNKS + 2 * outs]
    lhs, rhs, lhs_t, acc, staged, pending, sems, out_sems = rest[2 * CHUNKS + 2 * outs:]
    experts = own_out[0].shape[0]
    steps = table_ref[at["steps"]]

    def copies(chunk, row, s, half):
        source = pl.ds(pl.multiple_of(row, TILE), TILE)
        into = pl.ds(half * TILE, TILE)
        return (
            pltpu.make_async_copy(lhs_hbm[chunk].at[source, :], lhs.at[s, into, :], sems.at[s, half, 0]),
            pltpu.make_async_copy(rhs_hbm[chunk].at[source, :], rhs.at[s, into, :], sems.at[s, half, 1]),
        )

    def start(index, s):
        for half in range(2):
            src = table_ref[at["src"] + 2 * index + half]
            for chunk in range(CHUNKS):
                @pl.when(jnp.logical_and(src >= chunk * tiles_max, src < (chunk + 1) * tiles_max))
                def _(chunk=chunk, src=src, half=half):
                    for copy in copies(chunk, (src - chunk * tiles_max) * TILE, s, half):
                        copy.start()

    def out_copies(targets):
        return [pltpu.make_async_copy(staged.at[i], target, out_sems.at[i]) for i, target in enumerate(targets)]

    def drain():
        @pl.when(pending[0] != 0)
        def _():
            for copy in out_copies([out.at[0] for out in own_out]):
                copy.wait()

        pending[0] = 0

    pending[0] = 0
    start(0, 0)

    def accumulate(slot, fresh, depth):
        lhs_t[:, :depth] = jnp.transpose(lhs[slot, :depth, :], (1, 0))
        block = 2 * LANES
        for c in range(0, acc.shape[1], block):
            part = jnp.dot(lhs_t[:, :depth], rhs[slot, :depth, c:c + block], preferred_element_type=jnp.float32)
            acc[:, c:c + block] = jnp.where(fresh, 0.0, acc[:, c:c + block]) + part

    @pl.loop(0, steps)
    def _(step):
        slot = lax.rem(step, 2)
        group = table_ref[at["owner"] + step]

        @pl.when(step + 1 < steps)
        def _():
            start(step + 1, 1 - slot)

        fresh = jnp.logical_or(step == 0, group != table_ref[at["owner"] + jnp.maximum(step - 1, 0)])
        last = jnp.logical_or(step == steps - 1, group != table_ref[at["owner"] + step + 1])
        pair = table_ref[at["src"] + 2 * step + 1] >= 0
        for copy in copies(0, 0, slot, 0):
            copy.wait()

        @pl.when(pair)
        def _():
            for copy in copies(0, 0, slot, 1):
                copy.wait()
            accumulate(slot, fresh, 2 * TILE)

        @pl.when(jnp.logical_not(pair))
        def _():
            accumulate(slot, fresh, TILE)

        @pl.when(last)
        def _():
            drain()
            width = acc.shape[1] // outs
            for i in range(outs):
                staged[i, :, :] = acc[:, i * width:(i + 1) * width].astype(staged.dtype)

            @pl.when(group < experts)
            def _():
                for copy in out_copies([out.at[group] for out in own_out]):
                    copy.start()

            @pl.when(group == experts)
            def _():
                for copy in out_copies([out.at[0] for out in helped_out]):
                    copy.start()

            pending[0] = 1

    drain()


def weight_grad(layout, table, lhs, rhs, experts, outs):
    left, right = lhs[0].shape[1], rhs[0].shape[1]
    width = right // outs
    kernel = functools.partial(weight_grad_kernel, layout["grad"], layout["tiles_max"], outs)
    scratch = [
        pltpu.VMEM((2, 2 * TILE, left), jnp.bfloat16),
        pltpu.VMEM((2, 2 * TILE, right), jnp.bfloat16),
        pltpu.VMEM((left, 2 * TILE), jnp.bfloat16),
        pltpu.VMEM((left, right), jnp.float32),
        pltpu.VMEM((outs, left, width), jnp.bfloat16),
        pltpu.SMEM((1,), jnp.int32),
        pltpu.SemaphoreType.DMA((2, 2, 2)),
        pltpu.SemaphoreType.DMA((outs,)),
    ]
    out_shape = [jax.ShapeDtypeStruct((n, left, width), jnp.bfloat16) for n in [experts] * outs + [1] * outs]
    return call(
        kernel, table, (*lhs, *rhs), [ANY] * (2 * CHUNKS), out_shape, [ANY] * len(out_shape),
        scratch, (2 * 9000 * left * right, 100 * 10**6),
    )


def insert_kernel(at, size, table_ref, *rest):
    back, outs, staged, sems = rest[:size], rest[2 * size:3 * size], rest[3 * size:4 * size], rest[4 * size]
    place = table_ref[at]

    @pl.when(place >= 0)
    def _():
        fetch = [pltpu.make_async_copy(b.at[0], s, sems.at[0, i]) for i, (b, s) in enumerate(zip(back, staged))]
        store = [pltpu.make_async_copy(s, out.at[place], sems.at[1, i]) for i, (s, out) in enumerate(zip(staged, outs))]
        for copy in fetch:
            copy.start()
        for i in range(size):
            fetch[i].wait()
            store[i].start()
        for copy in store:
            copy.wait()


def insert(layout, table, back, grads):
    size = len(grads)
    return pl.pallas_call(
        functools.partial(insert_kernel, layout["insert"], size),
        grid_spec=pltpu.PrefetchScalarGridSpec(
            num_scalar_prefetch=1,
            in_specs=[ANY] * (2 * size),
            out_specs=[ANY] * size,
            scratch_shapes=[pltpu.VMEM(g.shape[1:], g.dtype) for g in grads] + [pltpu.SemaphoreType.DMA((2, size))],
        ),
        out_shape=[jax.ShapeDtypeStruct(g.shape, g.dtype) for g in grads],
        input_output_aliases={1 + size + i: i for i in range(size)},
        compiler_params=pltpu.CompilerParams(vmem_limit_bytes=VMEM_LIMIT),
        cost_estimate=pl.CostEstimate(flops=10**9, bytes_accessed=15 * 10**6 * size, transcendentals=0),
        name="insert",
    )(table, *back, *grads)


def row_blocks(height, dim):
    specs, first = [], 0
    for part in PARTS:
        blocks = part // height
        specs.append(pl.BlockSpec((height, dim), lambda t, *_, first=first, last=blocks - 1: (jnp.clip(t - first, 0, last), 0)))
        first += blocks
    return specs


def of_this_chunk(height, refs):
    step, first, value = pl.program_id(0), 0, None
    for part, ref in zip(PARTS, refs):
        value = ref[...] if value is None else jnp.where(step >= first, ref[...], value)
        first += part // height
    return value


def norm_kernel(x_ref, gain_ref, head_ref, tail_ref):
    step = pl.program_id(0)
    x = x_ref[...].astype(jnp.float32)
    inv_rms = lax.rsqrt(jnp.mean(x * x, axis=-1, keepdims=True) + NORM_EPS)
    x_norm = (x * inv_rms * gain_ref[...]).astype(jnp.bfloat16)
    head = PARTS[0] // x.shape[0]

    @pl.when(step < head)
    def _():
        head_ref[...] = x_norm

    @pl.when(step >= head)
    def _():
        tail_ref[...] = x_norm


def normalize(x, gain):
    tokens, dim = x.shape
    height, head = LANES, PARTS[0] // LANES
    return pl.pallas_call(
        norm_kernel,
        grid=(tokens // height,),
        in_specs=[pl.BlockSpec((height, dim), lambda t: (t, 0)), pl.BlockSpec((1, dim), lambda t: (0, 0))],
        out_specs=[
            pl.BlockSpec((height, dim), lambda t: (jnp.minimum(t, head - 1), 0)),
            pl.BlockSpec((height, dim), lambda t: (jnp.maximum(t - head, 0), 0)),
        ],
        out_shape=[jax.ShapeDtypeStruct((n, dim), jnp.bfloat16) for n in (PARTS[0], tokens - PARTS[0])],
        cost_estimate=pl.CostEstimate(flops=10**7, bytes_accessed=8 * 10**6, transcendentals=0),
        name="normalize",
    )(x, gain.reshape(1, dim))


def finish_kernel(x_ref, y_grad_ref, logit_ref, gain_ref, router_ref, *rest):
    in_refs, out_refs, (y_ref, x_grad_ref, stats_ref) = rest[:CHUNKS], rest[CHUNKS:2 * CHUNKS], rest[2 * CHUNKS:]
    height = x_ref.shape[0]
    x = x_ref[...].astype(jnp.float32)
    inv_rms = lax.rsqrt(jnp.mean(x * x, axis=-1, keepdims=True) + NORM_EPS)
    unit = x * inv_rms
    gain = gain_ref[...]
    moe_out = of_this_chunk(height, out_refs).astype(jnp.float32)
    y_ref[...] = (x + moe_out).astype(y_ref.dtype)
    logit_grad = logit_ref[...]
    routed = lax.dot_general(logit_grad, router_ref[...], (((1,), (1,)), ((), ())), preferred_element_type=jnp.float32)
    x_norm_grad = of_this_chunk(height, in_refs).astype(jnp.float32) + routed
    unit_grad = x_norm_grad * gain
    x_grad = y_grad_ref[...].astype(jnp.float32) + inv_rms * (unit_grad - unit * jnp.mean(unit_grad * unit, axis=-1, keepdims=True))
    x_grad_ref[...] = x_grad.astype(x_grad_ref.dtype)
    x_norm = (unit * gain).astype(jnp.bfloat16)
    by_expert = lax.dot_general(logit_grad, x_norm, (((0,), (0,)), ((), ())), preferred_element_type=jnp.float32)

    @pl.when(pl.program_id(0) == 0)
    def _():
        stats_ref[...] = jnp.zeros_like(stats_ref)

    def folded(values):
        return jnp.sum(values.reshape(height // 8, 8, values.shape[1]), axis=0)

    stats_ref[0:8, :] += by_expert[0:8, :]
    stats_ref[8:16, :] += folded(x_norm_grad * unit)
    stats_ref[16:24, :] += folded(moe_out * moe_out)


def finish(x, y_grad, logit_grad, gain, w_router, in_raw, out_raw):
    tokens, dim = x.shape
    height = LANES
    rows = pl.BlockSpec((height, dim), lambda t: (t, 0))
    wide = jnp.pad(logit_grad, ((0, 0), (0, LANES - logit_grad.shape[1])))
    router = jnp.pad(w_router, ((0, 0), (0, LANES - w_router.shape[1])))
    return pl.pallas_call(
        finish_kernel,
        grid=(tokens // height,),
        in_specs=[
            rows, rows, pl.BlockSpec((height, LANES), lambda t: (t, 0)), pl.BlockSpec((1, dim), lambda t: (0, 0)),
            pl.BlockSpec((dim, LANES), lambda t: (0, 0)), *row_blocks(height, dim), *row_blocks(height, dim),
        ],
        out_specs=[rows, rows, pl.BlockSpec((32, dim), lambda t: (0, 0))],
        out_shape=[
            jax.ShapeDtypeStruct((tokens, dim), jnp.bfloat16), jax.ShapeDtypeStruct((tokens, dim), jnp.bfloat16),
            jax.ShapeDtypeStruct((32, dim), jnp.float32),
        ],
        compiler_params=pltpu.CompilerParams(vmem_limit_bytes=VMEM_LIMIT),
        cost_estimate=pl.CostEstimate(flops=10**9, bytes_accessed=25 * 10**6, transcendentals=0),
        name="finish",
    )(x, y_grad, wide, gain.reshape(1, dim), router, *in_raw, *out_raw)


def below(size, strict):
    i = lax.broadcasted_iota(jnp.int32, (size, size), 0)
    j = lax.broadcasted_iota(jnp.int32, (size, size), 1)
    return (i < j if strict else i <= j).astype(jnp.float32)


def running(values):
    size = values.shape[-1]
    i = lax.broadcasted_iota(jnp.int32, (size, size), 0)
    j = lax.broadcasted_iota(jnp.int32, (size, size), 1)
    return jnp.sum(jnp.where(i <= j, values[..., :, None], 0), axis=-2)


def count(condition, axis):
    return jnp.sum(condition.astype(jnp.int32), axis=axis)


def choose_swap(tiles, experts):
    none = jnp.zeros((1,), jnp.int32)
    options = [jnp.concatenate([none, tiles[:experts]]), jnp.concatenate([none, tiles[experts:]])]
    gap = jnp.sum(tiles[:experts]) - jnp.sum(tiles[experts:])
    left = jnp.abs(gap - 2 * options[0][:, None] + 2 * options[1][None, :])
    index = lax.broadcasted_iota(jnp.int32, left.shape, 0) * (experts + 1) + lax.broadcasted_iota(jnp.int32, left.shape, 1)
    best = jnp.min(jnp.where(left == jnp.min(left), index, left.size))
    return best // (experts + 1) - 1, best % (experts + 1) - 1


def routing(hot, experts_of, place):
    groups, span_total, _ = hot.shape
    spans_of = [part * (span_total * LANES // sum(PARTS)) // LANES for part in PARTS]
    firsts = [sum(spans_of[:c]) for c in range(CHUNKS)]
    chunk_of = jnp.concatenate([jnp.full((n,), c, jnp.int32) for c, n in enumerate(spans_of)])
    member = chunk_of[:, None] == jnp.arange(CHUNKS, dtype=jnp.int32)[None, :]
    same = chunk_of[:, None] == chunk_of[None, :]
    tiles_of = [2 * n * LANES // TILE + groups for n in spans_of]
    tiles_max = max(tiles_of)

    within = jnp.einsum("gsi,ij->gsj", hot, below(LANES, False), preferred_element_type=jnp.float32)
    span_count = jnp.sum(hot, axis=-1)
    before = jnp.einsum("gi,ij->gj", span_count, jnp.where(same, below(span_total, True), 0.0), preferred_element_type=jnp.float32)
    total = jnp.sum(jnp.where(member[:, None, :], span_count.T[:, :, None], 0.0), axis=0).T.astype(jnp.int32)
    tiles = (total + TILE - 1) // TILE
    none = jnp.logical_and(jnp.sum(tiles, axis=1, keepdims=True) == 0, jnp.arange(groups, dtype=jnp.int32) == 0)
    tiles = jnp.where(none, 1, tiles)
    stop = running(tiles)
    begin = stop - tiles

    def to_spans(values):
        return jnp.sum(jnp.where(member[None], values.T[:, None, :], 0), axis=2)

    span_first = to_spans(begin) * TILE + before.astype(jnp.int32)
    span_stop = span_first + span_count.astype(jnp.int32)
    pos = jnp.where(hot > 0, span_first[:, :, None] + within.astype(jnp.int32) - 1, -1)

    index = jnp.arange(groups, dtype=jnp.int32)
    tile = jnp.arange(tiles_max, dtype=jnp.int32)
    group = jnp.minimum(count(tile[None, :, None] >= stop[:, None, :], 2), groups - 1)
    mine = group[:, :, None] == index
    ordinal = running((tiles > 0).astype(jnp.int32)) - 1
    later = jnp.logical_and(index[None, None, :] > group[:, :, None], tiles[:, None, :] > 0)
    follow = jnp.min(jnp.where(later, index, groups), axis=2)
    follow = jnp.where(follow == groups, -1, follow)
    fresh = jnp.sum(jnp.where(mine, begin[:, None, :], 0), axis=2) == tile
    slot = jnp.sum(jnp.where(mine, ordinal[:, None, :], 0), axis=2) % 2
    rows_left = jnp.sum(jnp.where(mine, (total + begin * TILE)[:, None, :], 0), axis=2) - tile * TILE
    half = rows_left <= TILE // 2

    half_mine = jnp.repeat(mine, 2, axis=1)
    stops = jnp.sum(jnp.where(half_mine[..., None], span_stop[None, None], 0), axis=2)
    row0 = jnp.arange(2 * tiles_max, dtype=jnp.int32)[None, :, None] * LANES
    inside = member.T[:, None, :]
    lo = count(jnp.logical_and(inside, stops <= row0), 2)
    hi = jnp.minimum(count(jnp.logical_and(inside, stops < row0 + LANES), 2), jnp.array(spans_of, jnp.int32)[:, None] - 1)
    width = jnp.maximum(jnp.max(((hi - lo + 2) // 2).reshape(CHUNKS, tiles_max, 2), axis=2), 1)
    start = jnp.minimum(span_first // 16 * 16, to_spans(stop) * TILE - REACH)
    empty = to_spans(tiles) == 0
    leading = jnp.logical_and(jnp.logical_not(empty), to_spans(ordinal) == 0)
    start = jnp.where(empty, jnp.sum(jnp.where(leading, start, 0), axis=0), start)
    over = jnp.any(jnp.logical_and(jnp.logical_not(empty), span_stop - start > REACH), axis=0)
    over = jnp.any(over.reshape(-1, GROUP), axis=1)

    in_chunks = running(tiles.T)
    both = in_chunks[:, -1]
    step_stop = running((both + 1) // 2)
    step_first = step_stop - (both + 1) // 2
    steps = CHUNKS * tiles_max // 2 + groups
    step = jnp.arange(steps, dtype=jnp.int32)
    owner = jnp.minimum(count(step[:, None] >= step_stop[None, :], 1), groups - 1)
    step_mine = owner[:, None] == index

    def of_step(values):
        return jnp.sum(jnp.where(step_mine[:, :, None], values[None], 0), axis=1)[:, None, :]

    local = 2 * (step - of_step(step_first[:, None])[:, 0, 0])[:, None, None] + jnp.arange(2, dtype=jnp.int32)[None, :, None]
    ends, sizes = of_step(in_chunks), of_step(tiles.T)
    offset = local - (ends - sizes)
    found = jnp.logical_and(offset >= 0, local < ends)
    chunk_at = jnp.arange(CHUNKS, dtype=jnp.int32) * tiles_max
    src = jnp.sum(jnp.where(found, of_step(begin.T) + offset + chunk_at + 1, 0), axis=2) - 1

    sections = (
        ("expert", experts_of), ("insert", place.reshape(1)), ("steps", step_stop[-1:]), ("owner", owner), ("src", src),
        ("count", stop[:, -1:]), ("group", group), ("slot", slot), ("fresh", fresh), ("half", half), ("next", follow), ("lo", lo), ("width", width),
        ("first", jnp.concatenate([jnp.zeros((CHUNKS, 1), jnp.int32), stop], axis=1)), ("start", start), ("over", over),
    )
    table = jnp.concatenate([values.reshape(-1).astype(jnp.int32) for _, values in sections])
    places, sizes_of, at = {}, {}, 0
    for name, values in sections:
        places[name], sizes_of[name] = at, values.size
        at += values.size
    layout = {}
    for c in range(CHUNKS):
        layout[c] = {name: places[name] + c * (sizes_of[name] // CHUNKS) for name in ("count", "group", "slot", "fresh", "half", "next", "lo", "width", "first")}
        layout[c] |= {
            "expert": places["expert"], "spans": (firsts[c], spans_of[c]), "part": PARTS[c], "rows_max": tiles_of[c] * TILE,
            "start": [places["start"] + g * span_total + firsts[c] for g in range(groups)],
            "over": places["over"] + firsts[c] // GROUP,
        }
    layout |= {"grad": {name: places[name] for name in ("steps", "owner", "src")}, "insert": places["insert"], "tiles_max": tiles_max}
    return pos, table, layout


def solution(mesh):
    tp_size = mesh.shape["tp"]
    ep_size = mesh.shape["ep"]
    dev_count = tp_size * ep_size
    rows_axes = ("ep", "tp")
    row_spec = P(rows_axes, None)
    wide_spec = P("ep", None, "tp")
    down_spec = P("ep", "tp", None)
    swap = [(0, 1), (1, 0)]

    def body(x, y_grad, expert_ids, norm_gain, w_router, w_gate, w_up, w_down):
        tokens, model_dim = x.shape
        top_k = expert_ids.shape[1]
        num_experts = w_router.shape[1]
        local_experts = w_gate.shape[0]
        total_tokens = tokens * dev_count
        my_ep = lax.axis_index("ep").astype(jnp.int32)
        firsts = [sum(PARTS[:c]) for c in range(CHUNKS)]

        def of_chunk(rows, c, axis=0):
            return lax.slice_in_dim(rows, firsts[c], firsts[c] + PARTS[c], axis=axis)

        def gather(rows):
            return lax.all_gather(rows, rows_axes, axis=0, tiled=True)

        def scatter(rows):
            return lax.psum_scatter(rows, rows_axes, scatter_dimension=0, tiled=True)

        def after(values, first):
            return lax.optimization_barrier((values, first))

        gain = norm_gain.astype(jnp.float32)
        head, tail = normalize(x, gain)
        rest = tokens - PARTS[0]
        gathered = [gather(head), gather(tail)]
        tok = [(gathered[0], (0, PARTS[0]))] + [(gathered[1], (firsts[c] - PARTS[0], rest)) for c in range(1, CHUNKS)]

        x_norm = jnp.concatenate([head, tail], axis=0)
        route_prob = jax.nn.softmax(jnp.dot(x_norm, w_router, preferred_element_type=jnp.float32), axis=-1)
        expert_range = jnp.arange(num_experts, dtype=jnp.int32)
        choice = jnp.sum((expert_ids[:, :, None] == expert_range[None, None, :]).astype(jnp.float32), axis=1)
        small = lax.all_gather(jnp.concatenate([choice, route_prob], axis=1).T, rows_axes, axis=0, tiled=False)
        counts = jnp.sum(small[:, :num_experts], axis=(0, 2))
        balance_scale = BALANCE_COEF * num_experts / (total_tokens * total_tokens * top_k)
        balance_loss = balance_scale * jnp.sum(counts * jnp.sum(small[:, num_experts:], axis=(0, 2)))

        rows_in = jnp.stack([jnp.sum(of_chunk(small[:, :num_experts], c, 2), axis=(0, 2)) for c in range(CHUNKS)])
        tiles_in = jnp.sum((rows_in.astype(jnp.int32) + TILE - 1) // TILE, axis=0)
        gives = choose_swap(tiles_in, local_experts)
        given = jnp.where(my_ep == 0, gives[0], gives[1])
        taken = jnp.where(my_ep == 0, gives[1], gives[0])
        my_base = my_ep * local_experts
        local = jnp.arange(local_experts, dtype=jnp.int32)
        group_experts = jnp.concatenate([my_base + local, (local_experts - my_base + jnp.maximum(taken, 0)).reshape(1)])
        active = jnp.concatenate([local != given, (taken >= 0).reshape(1)])
        take = jnp.logical_and(group_experts[:, None] == expert_range, active[:, None])
        spread = jnp.concatenate([of_chunk(small, c, 2).transpose(1, 0, 2).reshape(2 * num_experts, -1) for c in range(CHUNKS)], axis=1)
        spread = spread.reshape(2, 1, num_experts, -1, LANES)
        own = jnp.sum(jnp.where(take[None, :, :, None, None], spread, 0.0), axis=2)
        prob = own[1]
        pos, table, layout = routing(own[0], group_experts, given)
        helped = [lax.ppermute(lax.dynamic_slice_in_dim(w, jnp.maximum(given, 0), 1, axis=0), "ep", swap) for w in (w_gate, w_up, w_down)]
        weights = (w_gate, w_up, w_down, *helped)

        grad_scale = 2.0 * ACT_COEF / (total_tokens * model_dim)
        x_rows, gate_rows, pre, hidden, d_rows, mg_rows = [], [], [], [], [], []
        out_raw, moe_out, m_own, m_tok, in_raw, gate_part = [], [], [], [], [], []

        def send_cotangent(c, gate):
            raw, (gate, _) = after(out_raw[c], (gate, m_own[-1:]))
            moe_out.append(raw)
            moe_grad = of_chunk(y_grad, c).astype(jnp.float32) + grad_scale * raw.astype(jnp.float32)
            m_own.append(moe_grad.astype(jnp.bfloat16))
            m_tok.append(gather(m_own[c]))
            return gate

        for c in range(CHUNKS):
            rows, gates, ab, h, out_rows = forward(layout, c, table, pos, prob, tok[c], weights)
            (partial,) = combine(layout, c, table, pos, out_rows)
            if c == 0:
                partial, later = after(partial, gathered[1])
                tok[1:] = [(later, place) for _, place in tok[1:]]
            else:
                partial = send_cotangent(c - 1, partial)
            out_raw.append(scatter(partial))
            x_rows.append(rows)
            gate_rows.append(gates)
            pre.append(ab)
            hidden.append(h)
        for c in range(CHUNKS):
            d, in_rows, mg, dgate = backward(layout, c, table, pos, m_tok[c], pre[c], hidden[c], gate_rows[c], weights)
            if c == 0:
                in_rows = send_cotangent(CHUNKS - 1, in_rows)
            partial, gate_tok = combine(layout, c, table, pos, in_rows, dgate)
            if c == 0:
                m_tok[1], partial = after(m_tok[1], partial)
                partial, m_tok[-1] = after(partial, m_tok[-1])
            in_raw.append(scatter(partial))
            gate_part.append(gate_tok[:, :num_experts])
            d_rows.append(d)
            mg_rows.append(mg)
        *wide_grads, helped_gate, helped_up = weight_grad(layout, table, x_rows, d_rows, local_experts, 2)
        back = [lax.ppermute(g, "ep", swap) for g in (helped_gate, helped_up)]

        sums = jnp.concatenate([g.reshape(dev_count, -1) for g in gate_part], axis=1)
        gate_weight_grad = lax.psum(sums, ("tp", "ep"))
        gate_weight_grad = lax.dynamic_index_in_dim(gate_weight_grad, my_ep * tp_size + lax.axis_index("tp"), axis=0, keepdims=False)
        gate_weight_grad, (wide_grads, in_raw) = after(gate_weight_grad, (wide_grads, in_raw))
        prob_grad = gate_weight_grad.reshape(tokens, num_experts) + balance_scale * counts[None, :]
        logit_grad = (route_prob * (prob_grad - jnp.sum(route_prob * prob_grad, axis=-1, keepdims=True))).astype(jnp.bfloat16)
        y, x_grad, stats = finish(x, y_grad, logit_grad, gain, w_router, in_raw, moe_out)
        gate_grad, up_grad = insert(layout, table, back, wide_grads)
        stats, (mg_rows[0], x_grad, gate_grad) = after(stats, (mg_rows[0], x_grad, gate_grad))
        down_grad, helped_down = weight_grad(layout, table, hidden, mg_rows, local_experts, 1)
        (down_grad,) = insert(layout, table, [lax.ppermute(helped_down, "ep", swap)], [down_grad])
        stats = lax.psum(stats, ("tp", "ep"))
        router_sum = stats[:num_experts].T
        gain_sum = jnp.sum(stats[8:16], axis=0)
        act_loss = ACT_COEF * jnp.sum(stats[16:24]) / (total_tokens * model_dim)
        return (y, x_grad, gain_sum.astype(jnp.bfloat16), router_sum.astype(jnp.bfloat16), gate_grad, up_grad, down_grad, balance_loss, act_loss)

    return jax.shard_map(body, mesh=mesh, in_specs=(row_spec, row_spec, row_spec, P(), P(), wide_spec, wide_spec, down_spec), out_specs=(row_spec, row_spec, P(), P(), wide_spec, wide_spec, down_spec, P(), P()), check_vma=False)
```

```python
import functools

import jax
import jax.numpy as jnp
from jax import lax
from jax.experimental import pallas as pl
from jax.experimental.pallas import tpu as pltpu
from jax.sharding import PartitionSpec as P


NORM_EPS = 1e-6
ACT_COEF = 1e-5
BALANCE_COEF = 1e-3
TILE = 256
LANES = 128
GROUP = 4
REACH = 96
PARTS = (384, 256, 384)
CHUNKS = len(PARTS)
WINDOWS = (1, 2, 3, 4)
VMEM_LIMIT = 67_043_328


def call(kernel, table, operands, in_specs, out_shape, out_specs, scratch, cost, grid=()):
    return pl.pallas_call(
        kernel,
        grid_spec=pltpu.PrefetchScalarGridSpec(
            num_scalar_prefetch=1, grid=grid, in_specs=in_specs, out_specs=out_specs, scratch_shapes=scratch
        ),
        out_shape=out_shape,
        compiler_params=pltpu.CompilerParams(vmem_limit_bytes=VMEM_LIMIT),
        cost_estimate=pl.CostEstimate(flops=cost[0], bytes_accessed=cost[1], transcendentals=0),
    )(table, *operands)


ANY = pl.BlockSpec(memory_space=pl.ANY)
WHOLE = pl.BlockSpec(memory_space=pltpu.VMEM)


def row_block(width):
    return pl.BlockSpec((TILE, width), lambda t: (t, 0))


class Dispatch:
    def __init__(self, at, place, table_ref, pos_ref, prob_ref, tok_hbm, scratch):
        self.at, self.table_ref, self.pos_ref, self.prob_ref, self.tok_hbm = at, table_ref, pos_ref, prob_ref, tok_hbm
        self.tok, self.waited, self.sems = scratch
        self.first, self.spans = at["spans"]
        self.offset, self.stride = place
        self.part = at["part"]

    def span_copy(self, index, row):
        into = pl.ds(index * LANES if isinstance(index, int) else pl.multiple_of(index * LANES, LANES), LANES)
        return pltpu.make_async_copy(self.tok_hbm.at[pl.ds(row, LANES), :], self.tok.at[into, :], self.sems.at[index])

    def begin(self, stream):
        self.waited[0] = 0
        for index in range(self.spans):
            if index == 2 * WINDOWS[-1]:
                stream.begin()
            device, token = divmod(index * LANES, self.part)
            self.span_copy(index, device * self.stride + self.offset + token).start()

    def await_tokens(self, stop_span):
        @pl.loop(self.waited[0], stop_span)
        def _(index):
            self.span_copy(index, 0).wait()

        self.waited[0] = jnp.maximum(self.waited[0], stop_span)

    def end(self):
        self.await_tokens(self.spans)

    def tile(self, x_ref, gate_ref=None):
        tile = pl.program_id(0)
        group = self.table_ref[self.at["group"] + tile]
        width = self.table_ref[self.at["width"] + tile]

        def window(half, count, start):
            row_id = lax.broadcasted_iota(jnp.int32, (LANES, LANES), 0) + (tile * TILE + half * LANES)
            into = pl.ds(half * LANES if isinstance(half, int) else pl.multiple_of(half * LANES, LANES), LANES)
            hot, gate = [], jnp.zeros((LANES, LANES), jnp.float32)
            for q in range(count):
                span = pl.ds(self.first + start + q, 1)
                match = self.pos_ref[group, span, :] == row_id
                hot.append(jnp.where(match, 1.0, 0.0).astype(jnp.bfloat16))
                if gate_ref is not None:
                    gate = gate + jnp.where(match, self.prob_ref[group, span, :], 0.0)
            rows = self.tok[pl.ds(pl.multiple_of(start * LANES, LANES), count * LANES), :]
            out = jnp.dot(jnp.concatenate(hot, axis=1), rows, preferred_element_type=jnp.float32)
            x_ref[into, :] = out.astype(x_ref.dtype)
            if gate_ref is not None:
                gate_ref[into, :] = jnp.broadcast_to(jnp.sum(gate, axis=1, keepdims=True), (LANES, LANES))

        @pl.when(width > WINDOWS[-1])
        def _():
            self.await_tokens(self.spans)

            @pl.loop(0, 2)
            def _(half):
                window(half, self.spans, 0)

        for k in WINDOWS:
            @pl.when(width == k)
            def _(k=k):
                starts = [jnp.minimum(self.table_ref[self.at["lo"] + 2 * tile + half], self.spans - 2 * k) for half in range(2)]
                self.await_tokens(jnp.maximum(starts[0], starts[1]) + 2 * k)
                for half in range(2):
                    window(half, 2 * k, starts[half])


def dispatch_scratch(at, tok):
    spans = at["spans"][1]
    return [pltpu.VMEM((spans * LANES, tok.shape[1]), tok.dtype), pltpu.SMEM((1,), jnp.int32), pltpu.SemaphoreType.DMA((spans,))]


def combine_kernel(at, spans, groups, with_gate, table_ref, pos_ref, rows_hbm, *rest):
    if with_gate:
        gate_hbm, out_ref, gout_ref, rows, gates, waited, sems = rest
    else:
        out_ref, rows, waited, sems = rest
    step = pl.program_id(0)
    steps = pl.num_programs(0)
    row_iota = lax.broadcasted_iota(jnp.int32, (REACH, LANES), 0)
    over = table_ref[at["over"] + step]

    def region(g):
        return table_ref[at["first"] + g], table_ref[at["first"] + g + 1]

    def start_of(g, span):
        return pl.multiple_of(table_ref[at["start"][g] + span], 16)

    def block_copies(index):
        into = pl.ds(pl.multiple_of(index * TILE, TILE), TILE)
        copies = [pltpu.make_async_copy(rows_hbm.at[into, :], rows.at[into, :], sems.at[0, index])]
        if with_gate:
            copies.append(pltpu.make_async_copy(gate_hbm.at[into, :], gates.at[into, :], sems.at[1, index]))
        return copies

    @pl.when(step == 0)
    def _():
        for g in range(groups):
            waited[g] = region(g)[0]
        longest = region(0)[1] - region(0)[0]
        for g in range(1, groups):
            longest = jnp.maximum(longest, region(g)[1] - region(g)[0])

        @pl.loop(0, longest)
        def _(index):
            for g in range(groups):
                begin, stop = region(g)

                @pl.when(begin + index < stop)
                def _(begin=begin):
                    for copy in block_copies(begin + index):
                        copy.start()

    for g in range(groups):
        stop = region(g)[1]
        need = jnp.minimum((start_of(g, (step + 1) * GROUP - 1) + REACH + over * REACH + TILE - 1) // TILE, stop)
        need = jnp.where(step == steps - 1, stop, need)

        @pl.loop(waited[g], need)
        def _(index):
            for copy in block_copies(index):
                copy.wait()

        waited[g] = jnp.maximum(waited[g], need)

    def window(q, second):
        span = step * GROUP + q
        hot, data, gdata = [], [], []
        for g in range(groups):
            begin = place = start_of(g, span)
            if second:
                first, stop = region(g)
                place = pl.multiple_of(jnp.where(first == stop, begin, jnp.minimum(begin + REACH, stop * TILE - REACH)), 16)
                begin = begin + REACH
            row = row_iota + place
            match = pos_ref[g, pl.ds(spans[0] + span, 1), :] == row
            if second:
                match = jnp.logical_and(match, row >= begin)
            hot.append(jnp.where(match, 1.0, 0.0).astype(jnp.bfloat16))
            data.append(rows[pl.ds(place, REACH), :])
            if with_gate:
                gdata.append(gates[pl.ds(place, REACH), :])
        hot = jnp.concatenate(hot, axis=0)
        dims = (((0,), (0,)), ((), ()))
        out = lax.dot_general(hot, jnp.concatenate(data, axis=0), dims, preferred_element_type=jnp.float32)
        if not with_gate:
            return out, None
        exact = jnp.concatenate(gdata, axis=0)
        high = exact.astype(jnp.bfloat16)
        low = (exact - high.astype(jnp.float32)).astype(jnp.bfloat16)
        pair = lax.dot_general(hot, jnp.concatenate([high, low], axis=1), dims, preferred_element_type=jnp.float32)
        return out, pair[:, :LANES] + pair[:, LANES:]

    def put(q, wide):
        out, gate = window(q, False)
        if wide:
            out2, gate2 = window(q, True)
            out = out + out2
            gate = gate + gate2 if with_gate else None
        into = pl.ds(q * LANES if isinstance(q, int) else pl.multiple_of(q * LANES, LANES), LANES)
        out_ref[into, :] = out.astype(out_ref.dtype)
        if with_gate:
            gout_ref[into, :] = gate

    @pl.when(over == 0)
    def _():
        for q in range(GROUP):
            put(q, False)

    @pl.when(over != 0)
    def _():
        @pl.loop(0, GROUP)
        def _(q):
            put(q, True)


def combine(layout, chunk, table, pos, rows, gate_rows=None):
    rows_max, dim = rows.shape
    groups = pos.shape[0]
    spans = layout[chunk]["spans"]
    tokens = spans[1] * LANES
    with_gate = gate_rows is not None
    block = GROUP * LANES
    operands, in_specs = [pos, rows], [WHOLE, ANY]
    out_shape = [jax.ShapeDtypeStruct((tokens, dim), jnp.bfloat16)]
    out_specs = [pl.BlockSpec((block, dim), lambda t, *_: (t, 0))]
    scratch = [pltpu.VMEM((rows_max, dim), jnp.bfloat16)]
    if with_gate:
        operands.append(gate_rows)
        in_specs.append(ANY)
        out_shape.append(jax.ShapeDtypeStruct((tokens, LANES), jnp.float32))
        out_specs.append(pl.BlockSpec((block, LANES), lambda t, *_: (t, 0)))
        scratch.append(pltpu.VMEM((rows_max, LANES), jnp.float32))
    scratch += [pltpu.SMEM((groups,), jnp.int32), pltpu.SemaphoreType.DMA((2, rows_max // TILE))]
    kernel = functools.partial(combine_kernel, layout[chunk], spans, groups, with_gate)
    return call(kernel, table, operands, in_specs, out_shape, out_specs, scratch, (9 * 10**9, 35 * 10**6), (tokens // block,))


class WeightStream:
    def __init__(self, at, table_ref, weights, scratch):
        self.at, self.table_ref, self.own, self.helped = at, table_ref, weights[:3], weights[3:]
        self.wide, self.down, self.sems = scratch
        self.experts, _, self.ffn = weights[0].shape

    def copies(self, sources, s):
        wg, wu, wd = sources
        return (
            pltpu.make_async_copy(wg, self.wide.at[s, :, pl.ds(0, self.ffn)], self.sems.at[s, 0]),
            pltpu.make_async_copy(wu, self.wide.at[s, :, pl.ds(self.ffn, self.ffn)], self.sems.at[s, 1]),
            pltpu.make_async_copy(wd, self.down.at[s], self.sems.at[s, 2]),
        )

    def start(self, group, s):
        @pl.when(jnp.logical_and(group >= 0, group < self.experts))
        def _():
            for copy in self.copies([w.at[group] for w in self.own], s):
                copy.start()

        @pl.when(group == self.experts)
        def _():
            for copy in self.copies([w.at[0] for w in self.helped], s):
                copy.start()

    def begin(self):
        self.start(self.table_ref[self.at["group"]], 0)

    def slot(self):
        tile = pl.program_id(0)
        s = table_slot = self.table_ref[self.at["slot"] + tile]

        @pl.when(self.table_ref[self.at["fresh"] + tile] != 0)
        def _():
            self.start(self.table_ref[self.at["next"] + tile], 1 - table_slot)
            for copy in self.copies([w.at[0] for w in self.own], table_slot):
                copy.wait()

        return s


def run_tiles(at, table_ref, tile_body, piped_in, piped_out):
    pltpu.emit_pipeline(
        tile_body, grid=(table_ref[at["count"]],),
        in_specs=[row_block(ref.shape[1]) for ref in piped_in],
        out_specs=[row_block(ref.shape[1]) for ref in piped_out],
    )(*piped_in, *piped_out)


def forward_kernel(at, place, table_ref, pos_ref, prob_ref, tok_hbm, *rest):
    stream = WeightStream(at, table_ref, rest[:6], rest[11:14])
    dispatch = Dispatch(at, place, table_ref, pos_ref, prob_ref, tok_hbm, rest[14:])
    wide, down, ffn = stream.wide, stream.down, stream.ffn
    dispatch.begin(stream)

    def tile_body(x_ref, gate_ref, ab_ref, h_ref, out_ref):
        dispatch.tile(x_ref, gate_ref)
        slot = stream.slot()

        def matmuls(height):
            used = slice(0, height)
            x = x_ref[used, :]
            for j in range(ffn // LANES):
                cols = slice(j * LANES, (j + 1) * LANES)
                ucols = slice(ffn + j * LANES, ffn + (j + 1) * LANES)
                both = jnp.dot(x, jnp.concatenate([wide[slot, :, cols], wide[slot, :, ucols]], axis=1), preferred_element_type=jnp.float32)
                a, b = both[:, :LANES], both[:, LANES:]
                ab_ref[used, cols] = a
                ab_ref[used, ucols] = b
                h_ref[used, cols] = (a * jax.nn.sigmoid(a) * b).astype(h_ref.dtype)
            out = jnp.dot(h_ref[used, :], down[slot], preferred_element_type=jnp.float32)
            gate = gate_ref[used, :]
            for j in range(out.shape[1] // LANES):
                cols = slice(j * LANES, (j + 1) * LANES)
                out_ref[used, cols] = (out[:, cols] * gate).astype(out_ref.dtype)

        half = table_ref[at["half"] + pl.program_id(0)] != 0

        @pl.when(jnp.logical_not(half))
        def _():
            matmuls(TILE)

        @pl.when(half)
        def _():
            matmuls(TILE // 2)
            for ref in (ab_ref, h_ref, out_ref):
                ref[TILE // 2:, :] = jnp.zeros((TILE // 2, ref.shape[1]), ref.dtype)

    run_tiles(at, table_ref, tile_body, (), rest[6:11])
    dispatch.end()


def backward_kernel(at, place, table_ref, pos_ref, tok_hbm, ab_hbm, h_hbm, gate_hbm, *rest):
    stream = WeightStream(at, table_ref, rest[:6], rest[10:13])
    m_ref = rest[13]
    dispatch = Dispatch(at, place, table_ref, pos_ref, None, tok_hbm, rest[14:])
    wide, down, ffn = stream.wide, stream.down, stream.ffn
    trans = (((1,), (1,)), ((), ()))
    dispatch.begin(stream)

    def tile_body(ab_ref, h_ref, gate_ref, d_ref, in_ref, mg_ref, dgate_ref):
        dispatch.tile(m_ref)
        slot = stream.slot()
        m = m_ref[...]
        gate = gate_ref[...]
        dgate = jnp.zeros(gate.shape, jnp.float32)
        for c in range(0, ffn, 2 * LANES):
            width = min(2 * LANES, ffn - c)
            raw = lax.dot_general(m, down[slot, c:c + width, :], trans, preferred_element_type=jnp.float32)
            for k in range(width // LANES):
                lo = c + k * LANES
                cols = slice(lo, lo + LANES)
                ucols = slice(ffn + lo, ffn + lo + LANES)
                g = raw[:, k * LANES:(k + 1) * LANES]
                a, b = ab_ref[:, cols], ab_ref[:, ucols]
                sig = jax.nn.sigmoid(a)
                hidden_grad = g * gate
                d_ref[:, cols] = (hidden_grad * b * sig * (1.0 + a * (1.0 - sig))).astype(d_ref.dtype)
                d_ref[:, ucols] = (hidden_grad * (a * sig)).astype(d_ref.dtype)
                dgate = dgate + g * h_ref[:, cols].astype(jnp.float32)
        in_ref[...] = lax.dot_general(d_ref[...], wide[slot], trans, preferred_element_type=jnp.float32).astype(in_ref.dtype)
        for j in range(m.shape[1] // LANES):
            cols = slice(j * LANES, (j + 1) * LANES)
            mg_ref[:, cols] = (m[:, cols].astype(jnp.float32) * gate).astype(mg_ref.dtype)
        lane = lax.broadcasted_iota(jnp.int32, gate.shape, 1)
        expert = table_ref[at["expert"] + table_ref[at["group"] + pl.program_id(0)]]
        dgate_ref[...] = jnp.where(lane == expert, jnp.sum(dgate, axis=1, keepdims=True), 0.0)

    run_tiles(at, table_ref, tile_body, (ab_hbm, h_hbm, gate_hbm), rest[6:10])
    dispatch.end()


def weight_scratch(wg):
    _, dim, ffn = wg.shape
    return [
        pltpu.VMEM((2, dim, 2 * ffn), wg.dtype),
        pltpu.VMEM((2, ffn, dim), wg.dtype),
        pltpu.SemaphoreType.DMA((2, 3)),
    ]


def shapes(rows_max, *kinds):
    return [jax.ShapeDtypeStruct((rows_max, width), dtype) for width, dtype in kinds]


def forward(layout, chunk, table, pos, prob, tokens, weights):
    _, dim, ffn = weights[0].shape
    kinds = ((dim, jnp.bfloat16), (LANES, jnp.float32), (2 * ffn, jnp.float32), (ffn, jnp.bfloat16), (dim, jnp.bfloat16))
    at = layout[chunk]
    tok, place = tokens
    return call(
        functools.partial(forward_kernel, at, place), table, (pos, prob, tok, *weights), [WHOLE, WHOLE] + [ANY] * 7,
        shapes(at["rows_max"], *kinds), [ANY] * 5, weight_scratch(weights[0]) + dispatch_scratch(at, tok), (75 * 10**9, 150 * 10**6),
    )


def backward(layout, chunk, table, pos, tok, ab, hidden, gates, weights):
    _, dim, ffn = weights[0].shape
    kinds = ((2 * ffn, jnp.bfloat16), (dim, jnp.bfloat16), (dim, jnp.bfloat16), (LANES, jnp.float32))
    at = layout[chunk]
    scratch = [*weight_scratch(weights[0]), pltpu.VMEM((TILE, dim), jnp.bfloat16), *dispatch_scratch(at, tok)]
    return call(
        functools.partial(backward_kernel, at, (0, at["part"])), table, (pos, tok, ab, hidden, gates, *weights), [WHOLE] + [ANY] * 10,
        shapes(at["rows_max"], *kinds), [ANY] * 4, scratch, (75 * 10**9, 150 * 10**6),
    )


def weight_grad_kernel(at, tiles_max, outs, carried, table_ref, *rest):
    lhs_hbm, rhs_hbm, back, rest = rest[:CHUNKS], rest[CHUNKS:2 * CHUNKS], rest[2 * CHUNKS:2 * CHUNKS + carried], rest[2 * CHUNKS + 2 * carried:]
    own_out, helped_out, filled, rest = rest[:outs], rest[outs:2 * outs], rest[2 * outs:2 * outs + carried], rest[2 * outs + carried:]
    lhs, rhs, lhs_t, acc, staged, pending, sems, out_sems = rest[:8]
    experts = own_out[0].shape[0]
    steps = table_ref[at["steps"]]

    def copies(chunk, row, s, half):
        source = pl.ds(pl.multiple_of(row, TILE), TILE)
        into = pl.ds(half * TILE, TILE)
        return (
            pltpu.make_async_copy(lhs_hbm[chunk].at[source, :], lhs.at[s, into, :], sems.at[s, half, 0]),
            pltpu.make_async_copy(rhs_hbm[chunk].at[source, :], rhs.at[s, into, :], sems.at[s, half, 1]),
        )

    def start(index, s):
        for half in range(2):
            src = table_ref[at["src"] + 2 * index + half]
            for chunk in range(CHUNKS):
                @pl.when(jnp.logical_and(src >= chunk * tiles_max, src < (chunk + 1) * tiles_max))
                def _(chunk=chunk, src=src, half=half):
                    for copy in copies(chunk, (src - chunk * tiles_max) * TILE, s, half):
                        copy.start()

    def out_copies(targets):
        return [pltpu.make_async_copy(staged.at[i], target, out_sems.at[i]) for i, target in enumerate(targets)]

    def drain():
        @pl.when(pending[0] != 0)
        def _():
            for copy in out_copies([out.at[0] for out in own_out]):
                copy.wait()

        pending[0] = 0

    pending[0] = 0
    start(0, 0)

    place = table_ref[at["insert"]]
    if carried:
        bounce, fetch_sems, store_sems = rest[8:]
        fetch = [pltpu.make_async_copy(back[i].at[0], bounce.at[i], fetch_sems.at[i]) for i in range(carried)]
        store = [pltpu.make_async_copy(bounce.at[i], filled[i].at[jnp.maximum(place, 0)], store_sems.at[i]) for i in range(carried)]

        @pl.when(place >= 0)
        def _():
            for copy in fetch:
                copy.start()

    def accumulate(slot, fresh, depth):
        lhs_t[:, :depth] = jnp.transpose(lhs[slot, :depth, :], (1, 0))
        block = 2 * LANES
        for c in range(0, acc.shape[1], block):
            part = jnp.dot(lhs_t[:, :depth], rhs[slot, :depth, c:c + block], preferred_element_type=jnp.float32)
            acc[:, c:c + block] = jnp.where(fresh, 0.0, acc[:, c:c + block]) + part

    @pl.loop(0, steps)
    def _(step):
        slot = lax.rem(step, 2)
        group = table_ref[at["owner"] + step]

        @pl.when(step + 1 < steps)
        def _():
            start(step + 1, 1 - slot)

        if carried:
            @pl.when(jnp.logical_and(place >= 0, step == steps // 2))
            def _():
                for one, other in zip(fetch, store):
                    one.wait()
                    other.start()

        fresh = jnp.logical_or(step == 0, group != table_ref[at["owner"] + jnp.maximum(step - 1, 0)])
        last = jnp.logical_or(step == steps - 1, group != table_ref[at["owner"] + step + 1])
        pair = table_ref[at["src"] + 2 * step + 1] >= 0
        for copy in copies(0, 0, slot, 0):
            copy.wait()

        @pl.when(pair)
        def _():
            for copy in copies(0, 0, slot, 1):
                copy.wait()
            accumulate(slot, fresh, 2 * TILE)

        @pl.when(jnp.logical_not(pair))
        def _():
            accumulate(slot, fresh, TILE)

        @pl.when(last)
        def _():
            drain()
            width = acc.shape[1] // outs
            for i in range(outs):
                staged[i, :, :] = acc[:, i * width:(i + 1) * width].astype(staged.dtype)

            @pl.when(group < experts)
            def _():
                for copy in out_copies([out.at[group] for out in own_out]):
                    copy.start()

            @pl.when(group == experts)
            def _():
                for copy in out_copies([out.at[0] for out in helped_out]):
                    copy.start()

            pending[0] = 1

    drain()
    if carried:
        @pl.when(place >= 0)
        def _():
            for copy in store:
                copy.wait()


def weight_grad(layout, table, lhs, rhs, experts, outs, back=(), grads=()):
    left, right = lhs[0].shape[1], rhs[0].shape[1]
    width = right // outs
    carried = len(grads)
    scratch = [
        pltpu.VMEM((2, 2 * TILE, left), jnp.bfloat16),
        pltpu.VMEM((2, 2 * TILE, right), jnp.bfloat16),
        pltpu.VMEM((left, 2 * TILE), jnp.bfloat16),
        pltpu.VMEM((left, right), jnp.float32),
        pltpu.VMEM((outs, left, width), jnp.bfloat16),
        pltpu.SMEM((1,), jnp.int32),
        pltpu.SemaphoreType.DMA((2, 2, 2)),
        pltpu.SemaphoreType.DMA((outs,)),
    ]
    if carried:
        scratch += [pltpu.VMEM((carried, *grads[0].shape[1:]), jnp.bfloat16), pltpu.SemaphoreType.DMA((carried,)), pltpu.SemaphoreType.DMA((carried,))]
    out_shape = [jax.ShapeDtypeStruct((n, left, width), jnp.bfloat16) for n in [experts] * outs + [1] * outs]
    out_shape += [jax.ShapeDtypeStruct(g.shape, g.dtype) for g in grads]
    operands = (*lhs, *rhs, *back, *grads)
    return pl.pallas_call(
        functools.partial(weight_grad_kernel, layout["grad"], layout["tiles_max"], outs, carried),
        grid_spec=pltpu.PrefetchScalarGridSpec(
            num_scalar_prefetch=1, in_specs=[ANY] * len(operands), out_specs=[ANY] * len(out_shape), scratch_shapes=scratch
        ),
        out_shape=out_shape,
        input_output_aliases={1 + 2 * CHUNKS + carried + i: 2 * outs + i for i in range(carried)},
        compiler_params=pltpu.CompilerParams(vmem_limit_bytes=VMEM_LIMIT),
        cost_estimate=pl.CostEstimate(flops=2 * 9000 * left * right, bytes_accessed=100 * 10**6, transcendentals=0),
        name="weight_grad",
    )(table, *operands)


def insert_kernel(at, size, table_ref, *rest):
    back, outs, staged, sems = rest[:size], rest[2 * size:3 * size], rest[3 * size:4 * size], rest[4 * size]
    place = table_ref[at]

    @pl.when(place >= 0)
    def _():
        fetch = [pltpu.make_async_copy(b.at[0], s, sems.at[0, i]) for i, (b, s) in enumerate(zip(back, staged))]
        store = [pltpu.make_async_copy(s, out.at[place], sems.at[1, i]) for i, (s, out) in enumerate(zip(staged, outs))]
        for copy in fetch:
            copy.start()
        for i in range(size):
            fetch[i].wait()
            store[i].start()
        for copy in store:
            copy.wait()


def insert(layout, table, back, grads):
    size = len(grads)
    return pl.pallas_call(
        functools.partial(insert_kernel, layout["insert"], size),
        grid_spec=pltpu.PrefetchScalarGridSpec(
            num_scalar_prefetch=1,
            in_specs=[ANY] * (2 * size),
            out_specs=[ANY] * size,
            scratch_shapes=[pltpu.VMEM(g.shape[1:], g.dtype) for g in grads] + [pltpu.SemaphoreType.DMA((2, size))],
        ),
        out_shape=[jax.ShapeDtypeStruct(g.shape, g.dtype) for g in grads],
        input_output_aliases={1 + size + i: i for i in range(size)},
        compiler_params=pltpu.CompilerParams(vmem_limit_bytes=VMEM_LIMIT),
        cost_estimate=pl.CostEstimate(flops=10**9, bytes_accessed=15 * 10**6 * size, transcendentals=0),
        name="insert",
    )(table, *back, *grads)


def row_blocks(height, dim):
    specs, first = [], 0
    for part in PARTS:
        blocks = part // height
        specs.append(pl.BlockSpec((height, dim), lambda t, *_, first=first, last=blocks - 1: (jnp.clip(t - first, 0, last), 0)))
        first += blocks
    return specs


def of_this_chunk(height, refs):
    step, first, value = pl.program_id(0), 0, None
    for part, ref in zip(PARTS, refs):
        value = ref[...] if value is None else jnp.where(step >= first, ref[...], value)
        first += part // height
    return value


def norm_kernel(x_ref, gain_ref, out_ref):
    x = x_ref[...].astype(jnp.float32)
    inv_rms = lax.rsqrt(jnp.mean(x * x, axis=-1, keepdims=True) + NORM_EPS)
    out_ref[...] = (x * inv_rms * gain_ref[...]).astype(out_ref.dtype)


def normalize(x, gain, first, count):
    dim = x.shape[1]
    height = LANES
    return pl.pallas_call(
        norm_kernel,
        grid=(count // height,),
        in_specs=[pl.BlockSpec((height, dim), lambda t: (t + first // height, 0)), pl.BlockSpec((1, dim), lambda t: (0, 0))],
        out_specs=pl.BlockSpec((height, dim), lambda t: (t, 0)),
        out_shape=jax.ShapeDtypeStruct((count, dim), jnp.bfloat16),
        cost_estimate=pl.CostEstimate(flops=10**7, bytes_accessed=4 * 10**6, transcendentals=0),
        name="normalize",
    )(x, gain.reshape(1, dim))


def finish_kernel(x_ref, y_grad_ref, logit_ref, gain_ref, router_ref, *rest):
    in_refs, out_refs, (y_ref, x_grad_ref, stats_ref) = rest[:CHUNKS], rest[CHUNKS:2 * CHUNKS], rest[2 * CHUNKS:]
    height = x_ref.shape[0]
    x = x_ref[...].astype(jnp.float32)
    inv_rms = lax.rsqrt(jnp.mean(x * x, axis=-1, keepdims=True) + NORM_EPS)
    unit = x * inv_rms
    gain = gain_ref[...]
    moe_out = of_this_chunk(height, out_refs).astype(jnp.float32)
    y_ref[...] = (x + moe_out).astype(y_ref.dtype)
    logit_grad = logit_ref[...]
    routed = lax.dot_general(logit_grad, router_ref[...], (((1,), (1,)), ((), ())), preferred_element_type=jnp.float32)
    x_norm_grad = of_this_chunk(height, in_refs).astype(jnp.float32) + routed
    unit_grad = x_norm_grad * gain
    x_grad = y_grad_ref[...].astype(jnp.float32) + inv_rms * (unit_grad - unit * jnp.mean(unit_grad * unit, axis=-1, keepdims=True))
    x_grad_ref[...] = x_grad.astype(x_grad_ref.dtype)
    x_norm = (unit * gain).astype(jnp.bfloat16)
    by_expert = lax.dot_general(logit_grad, x_norm, (((0,), (0,)), ((), ())), preferred_element_type=jnp.float32)

    @pl.when(pl.program_id(0) == 0)
    def _():
        stats_ref[...] = jnp.zeros_like(stats_ref)

    def folded(values):
        return jnp.sum(values.reshape(height // 8, 8, values.shape[1]), axis=0)

    stats_ref[0:8, :] += by_expert[0:8, :]
    stats_ref[8:16, :] += folded(x_norm_grad * unit)
    stats_ref[16:24, :] += folded(moe_out * moe_out)


def finish(x, y_grad, logit_grad, gain, w_router, in_raw, out_raw):
    tokens, dim = x.shape
    height = LANES
    rows = pl.BlockSpec((height, dim), lambda t: (t, 0))
    wide = jnp.pad(logit_grad, ((0, 0), (0, LANES - logit_grad.shape[1])))
    router = jnp.pad(w_router, ((0, 0), (0, LANES - w_router.shape[1])))
    return pl.pallas_call(
        finish_kernel,
        grid=(tokens // height,),
        in_specs=[
            rows, rows, pl.BlockSpec((height, LANES), lambda t: (t, 0)), pl.BlockSpec((1, dim), lambda t: (0, 0)),
            pl.BlockSpec((dim, LANES), lambda t: (0, 0)), *row_blocks(height, dim), *row_blocks(height, dim),
        ],
        out_specs=[rows, rows, pl.BlockSpec((32, dim), lambda t: (0, 0))],
        out_shape=[
            jax.ShapeDtypeStruct((tokens, dim), jnp.bfloat16), jax.ShapeDtypeStruct((tokens, dim), jnp.bfloat16),
            jax.ShapeDtypeStruct((32, dim), jnp.float32),
        ],
        compiler_params=pltpu.CompilerParams(vmem_limit_bytes=VMEM_LIMIT),
        cost_estimate=pl.CostEstimate(flops=10**9, bytes_accessed=25 * 10**6, transcendentals=0),
        name="finish",
    )(x, y_grad, wide, gain.reshape(1, dim), router, *in_raw, *out_raw)


def below(size, strict):
    i = lax.broadcasted_iota(jnp.int32, (size, size), 0)
    j = lax.broadcasted_iota(jnp.int32, (size, size), 1)
    return (i < j if strict else i <= j).astype(jnp.float32)


def running(values):
    size = values.shape[-1]
    i = lax.broadcasted_iota(jnp.int32, (size, size), 0)
    j = lax.broadcasted_iota(jnp.int32, (size, size), 1)
    return jnp.sum(jnp.where(i <= j, values[..., :, None], 0), axis=-2)


def count(condition, axis):
    return jnp.sum(condition.astype(jnp.int32), axis=axis)


def choose_swap(rows, experts):
    work = 4 * ((rows + TILE - 1) // TILE) + (rows + TILE // 2 - 1) // (TILE // 2)
    none = jnp.zeros((rows.shape[0], 1), jnp.int32)
    sides = [work[:, :experts], work[:, experts:]]
    options = [jnp.concatenate([none, side], axis=1) for side in sides]
    moved = options[1][:, None, :] - options[0][:, :, None]
    loads = [jnp.sum(side, axis=1)[:, None, None] for side in sides]
    cost = jnp.sum(jnp.maximum(loads[0] + moved, loads[1] - moved), axis=0)
    index = lax.broadcasted_iota(jnp.int32, cost.shape, 0) * (experts + 1) + lax.broadcasted_iota(jnp.int32, cost.shape, 1)
    best = jnp.min(jnp.where(cost == jnp.min(cost), index, cost.size))
    return best // (experts + 1) - 1, best % (experts + 1) - 1


def routing(hot, experts_of, place):
    groups, span_total, _ = hot.shape
    spans_of = [part * (span_total * LANES // sum(PARTS)) // LANES for part in PARTS]
    firsts = [sum(spans_of[:c]) for c in range(CHUNKS)]
    chunk_of = jnp.concatenate([jnp.full((n,), c, jnp.int32) for c, n in enumerate(spans_of)])
    member = chunk_of[:, None] == jnp.arange(CHUNKS, dtype=jnp.int32)[None, :]
    same = chunk_of[:, None] == chunk_of[None, :]
    tiles_of = [2 * n * LANES // TILE + groups for n in spans_of]
    tiles_max = max(tiles_of)

    within = jnp.einsum("gsi,ij->gsj", hot, below(LANES, False), preferred_element_type=jnp.float32)
    span_count = jnp.sum(hot, axis=-1)
    before = jnp.einsum("gi,ij->gj", span_count, jnp.where(same, below(span_total, True), 0.0), preferred_element_type=jnp.float32)
    total = jnp.sum(jnp.where(member[:, None, :], span_count.T[:, :, None], 0.0), axis=0).T.astype(jnp.int32)
    tiles = (total + TILE - 1) // TILE
    none = jnp.logical_and(jnp.sum(tiles, axis=1, keepdims=True) == 0, jnp.arange(groups, dtype=jnp.int32) == 0)
    tiles = jnp.where(none, 1, tiles)
    stop = running(tiles)
    begin = stop - tiles

    def to_spans(values):
        return jnp.sum(jnp.where(member[None], values.T[:, None, :], 0), axis=2)

    span_first = to_spans(begin) * TILE + before.astype(jnp.int32)
    span_stop = span_first + span_count.astype(jnp.int32)
    pos = jnp.where(hot > 0, span_first[:, :, None] + within.astype(jnp.int32) - 1, -1)

    index = jnp.arange(groups, dtype=jnp.int32)
    tile = jnp.arange(tiles_max, dtype=jnp.int32)
    group = jnp.minimum(count(tile[None, :, None] >= stop[:, None, :], 2), groups - 1)
    mine = group[:, :, None] == index
    ordinal = running((tiles > 0).astype(jnp.int32)) - 1
    later = jnp.logical_and(index[None, None, :] > group[:, :, None], tiles[:, None, :] > 0)
    follow = jnp.min(jnp.where(later, index, groups), axis=2)
    follow = jnp.where(follow == groups, -1, follow)
    fresh = jnp.sum(jnp.where(mine, begin[:, None, :], 0), axis=2) == tile
    slot = jnp.sum(jnp.where(mine, ordinal[:, None, :], 0), axis=2) % 2
    rows_left = jnp.sum(jnp.where(mine, (total + begin * TILE)[:, None, :], 0), axis=2) - tile * TILE
    half = rows_left <= TILE // 2

    half_mine = jnp.repeat(mine, 2, axis=1)
    stops = jnp.sum(jnp.where(half_mine[..., None], span_stop[None, None], 0), axis=2)
    row0 = jnp.arange(2 * tiles_max, dtype=jnp.int32)[None, :, None] * LANES
    inside = member.T[:, None, :]
    lo = count(jnp.logical_and(inside, stops <= row0), 2)
    hi = jnp.minimum(count(jnp.logical_and(inside, stops < row0 + LANES), 2), jnp.array(spans_of, jnp.int32)[:, None] - 1)
    width = jnp.maximum(jnp.max(((hi - lo + 2) // 2).reshape(CHUNKS, tiles_max, 2), axis=2), 1)
    start = jnp.minimum(span_first // 16 * 16, to_spans(stop) * TILE - REACH)
    empty = to_spans(tiles) == 0
    leading = jnp.logical_and(jnp.logical_not(empty), to_spans(ordinal) == 0)
    start = jnp.where(empty, jnp.sum(jnp.where(leading, start, 0), axis=0), start)
    over = jnp.any(jnp.logical_and(jnp.logical_not(empty), span_stop - start > REACH), axis=0)
    over = jnp.any(over.reshape(-1, GROUP), axis=1)

    in_chunks = running(tiles.T)
    both = in_chunks[:, -1]
    step_stop = running((both + 1) // 2)
    step_first = step_stop - (both + 1) // 2
    steps = CHUNKS * tiles_max // 2 + groups
    step = jnp.arange(steps, dtype=jnp.int32)
    owner = jnp.minimum(count(step[:, None] >= step_stop[None, :], 1), groups - 1)
    step_mine = owner[:, None] == index

    def of_step(values):
        return jnp.sum(jnp.where(step_mine[:, :, None], values[None], 0), axis=1)[:, None, :]

    local = 2 * (step - of_step(step_first[:, None])[:, 0, 0])[:, None, None] + jnp.arange(2, dtype=jnp.int32)[None, :, None]
    ends, sizes = of_step(in_chunks), of_step(tiles.T)
    offset = local - (ends - sizes)
    found = jnp.logical_and(offset >= 0, local < ends)
    chunk_at = jnp.arange(CHUNKS, dtype=jnp.int32) * tiles_max
    src = jnp.sum(jnp.where(found, of_step(begin.T) + offset + chunk_at + 1, 0), axis=2) - 1

    sections = (
        ("expert", experts_of), ("insert", place.reshape(1)), ("steps", step_stop[-1:]), ("owner", owner), ("src", src),
        ("count", stop[:, -1:]), ("group", group), ("slot", slot), ("fresh", fresh), ("half", half), ("next", follow), ("lo", lo), ("width", width),
        ("first", jnp.concatenate([jnp.zeros((CHUNKS, 1), jnp.int32), stop], axis=1)), ("start", start), ("over", over),
    )
    table = jnp.concatenate([values.reshape(-1).astype(jnp.int32) for _, values in sections])
    places, sizes_of, at = {}, {}, 0
    for name, values in sections:
        places[name], sizes_of[name] = at, values.size
        at += values.size
    layout = {}
    for c in range(CHUNKS):
        layout[c] = {name: places[name] + c * (sizes_of[name] // CHUNKS) for name in ("count", "group", "slot", "fresh", "half", "next", "lo", "width", "first")}
        layout[c] |= {
            "expert": places["expert"], "spans": (firsts[c], spans_of[c]), "part": PARTS[c], "rows_max": tiles_of[c] * TILE,
            "start": [places["start"] + g * span_total + firsts[c] for g in range(groups)],
            "over": places["over"] + firsts[c] // GROUP,
        }
    layout |= {"grad": {name: places[name] for name in ("steps", "owner", "src", "insert")}, "insert": places["insert"], "tiles_max": tiles_max}
    return pos, table, layout


def solution(mesh):
    tp_size = mesh.shape["tp"]
    ep_size = mesh.shape["ep"]
    dev_count = tp_size * ep_size
    rows_axes = ("ep", "tp")
    row_spec = P(rows_axes, None)
    wide_spec = P("ep", None, "tp")
    down_spec = P("ep", "tp", None)
    swap = [(0, 1), (1, 0)]

    def body(x, y_grad, expert_ids, norm_gain, w_router, w_gate, w_up, w_down):
        tokens, model_dim = x.shape
        top_k = expert_ids.shape[1]
        num_experts = w_router.shape[1]
        local_experts = w_gate.shape[0]
        total_tokens = tokens * dev_count
        my_ep = lax.axis_index("ep").astype(jnp.int32)
        firsts = [sum(PARTS[:c]) for c in range(CHUNKS)]

        def of_chunk(rows, c, axis=0):
            return lax.slice_in_dim(rows, firsts[c], firsts[c] + PARTS[c], axis=axis)

        def gather(rows):
            return lax.all_gather(rows, rows_axes, axis=0, tiled=True)

        def scatter(rows):
            return lax.psum_scatter(rows, rows_axes, scatter_dimension=0, tiled=True)

        def after(values, first):
            return lax.optimization_barrier((values, first))

        gain = norm_gain.astype(jnp.float32)
        rest = tokens - PARTS[0]
        head, tail = normalize(x, gain, 0, PARTS[0]), normalize(x, gain, PARTS[0], rest)
        gathered = [gather(head), gather(tail)]
        tok = [(gathered[0], (0, PARTS[0]))] + [(gathered[1], (firsts[c] - PARTS[0], rest)) for c in range(1, CHUNKS)]

        x_norm = jnp.concatenate([head, tail], axis=0)
        route_prob = jax.nn.softmax(jnp.dot(x_norm, w_router, preferred_element_type=jnp.float32), axis=-1)
        expert_range = jnp.arange(num_experts, dtype=jnp.int32)
        choice = jnp.sum((expert_ids[:, :, None] == expert_range[None, None, :]).astype(jnp.float32), axis=1)
        small = lax.all_gather(jnp.concatenate([choice, route_prob], axis=1).T, rows_axes, axis=0, tiled=False)
        counts = jnp.sum(small[:, :num_experts], axis=(0, 2))
        balance_scale = BALANCE_COEF * num_experts / (total_tokens * total_tokens * top_k)
        balance_loss = balance_scale * jnp.sum(counts * jnp.sum(small[:, num_experts:], axis=(0, 2)))

        rows_in = jnp.stack([jnp.sum(of_chunk(small[:, :num_experts], c, 2), axis=(0, 2)) for c in range(CHUNKS)])
        gives = choose_swap(rows_in.astype(jnp.int32), local_experts)
        given = jnp.where(my_ep == 0, gives[0], gives[1])
        taken = jnp.where(my_ep == 0, gives[1], gives[0])
        my_base = my_ep * local_experts
        local = jnp.arange(local_experts, dtype=jnp.int32)
        group_experts = jnp.concatenate([my_base + local, (local_experts - my_base + jnp.maximum(taken, 0)).reshape(1)])
        active = jnp.concatenate([local != given, (taken >= 0).reshape(1)])
        take = jnp.logical_and(group_experts[:, None] == expert_range, active[:, None])
        spread = jnp.concatenate([of_chunk(small, c, 2).transpose(1, 0, 2).reshape(2 * num_experts, -1) for c in range(CHUNKS)], axis=1)
        spread = spread.reshape(2, 1, num_experts, -1, LANES)
        own = jnp.sum(jnp.where(take[None, :, :, None, None], spread, 0.0), axis=2)
        prob = own[1]
        pos, table, layout = routing(own[0], group_experts, given)
        helped = [lax.ppermute(lax.dynamic_slice_in_dim(w, jnp.maximum(given, 0), 1, axis=0), "ep", swap) for w in (w_gate, w_up, w_down)]
        weights = (w_gate, w_up, w_down, *helped)

        grad_scale = 2.0 * ACT_COEF / (total_tokens * model_dim)
        x_rows, gate_rows, pre, hidden, d_rows, mg_rows = [], [], [], [], [], []
        out_raw, moe_out, m_own, m_tok, in_raw, gate_part = [], [], [], [], [], []

        def send_cotangent(c, gate):
            raw, (gate, _) = after(out_raw[c], (gate, m_own[-1:]))
            moe_out.append(raw)
            moe_grad = of_chunk(y_grad, c).astype(jnp.float32) + grad_scale * raw.astype(jnp.float32)
            m_own.append(moe_grad.astype(jnp.bfloat16))
            m_tok.append(gather(m_own[c]))
            return gate

        for c in range(CHUNKS):
            rows, gates, ab, h, out_rows = forward(layout, c, table, pos, prob, tok[c], weights)
            (partial,) = combine(layout, c, table, pos, out_rows)
            if c == 0:
                partial, later = after(partial, gathered[1])
                tok[1:] = [(later, place) for _, place in tok[1:]]
            else:
                partial = send_cotangent(c - 1, partial)
            out_raw.append(scatter(partial))
            x_rows.append(rows)
            gate_rows.append(gates)
            pre.append(ab)
            hidden.append(h)
        for c in range(CHUNKS):
            d, in_rows, mg, dgate = backward(layout, c, table, pos, m_tok[c], pre[c], hidden[c], gate_rows[c], weights)
            if c == 0:
                in_rows = send_cotangent(CHUNKS - 1, in_rows)
            partial, gate_tok = combine(layout, c, table, pos, in_rows, dgate)
            if c == 0:
                m_tok[1], partial = after(m_tok[1], partial)
            in_raw.append(scatter(partial))
            gate_part.append(gate_tok[:, :num_experts])
            d_rows.append(d)
            mg_rows.append(mg)
        *wide_grads, helped_gate, helped_up = weight_grad(layout, table, x_rows, d_rows, local_experts, 2)
        back = [lax.ppermute(g, "ep", swap) for g in (helped_gate, helped_up)]

        sums = jnp.concatenate([g.reshape(dev_count, -1) for g in gate_part], axis=1)
        gate_weight_grad = lax.psum(sums, ("tp", "ep"))
        gate_weight_grad = lax.dynamic_index_in_dim(gate_weight_grad, my_ep * tp_size + lax.axis_index("tp"), axis=0, keepdims=False)
        gate_weight_grad, (wide_grads, in_raw) = after(gate_weight_grad, (wide_grads, in_raw))
        prob_grad = gate_weight_grad.reshape(tokens, num_experts) + balance_scale * counts[None, :]
        logit_grad = (route_prob * (prob_grad - jnp.sum(route_prob * prob_grad, axis=-1, keepdims=True))).astype(jnp.bfloat16)
        y, x_grad, stats = finish(x, y_grad, logit_grad, gain, w_router, in_raw, moe_out)
        stats, (mg_rows[0], x_grad, back) = after(stats, (mg_rows[0], x_grad, back))
        down_grad, helped_down, gate_grad, up_grad = weight_grad(layout, table, hidden, mg_rows, local_experts, 1, back, wide_grads)
        (down_grad,) = insert(layout, table, [lax.ppermute(helped_down, "ep", swap)], [down_grad])
        stats = lax.psum(stats, ("tp", "ep"))
        router_sum = stats[:num_experts].T
        gain_sum = jnp.sum(stats[8:16], axis=0)
        act_loss = ACT_COEF * jnp.sum(stats[16:24]) / (total_tokens * model_dim)
        return (y, x_grad, gain_sum.astype(jnp.bfloat16), router_sum.astype(jnp.bfloat16), gate_grad, up_grad, down_grad, balance_loss, act_loss)

    return jax.shard_map(body, mesh=mesh, in_specs=(row_spec, row_spec, row_spec, P(), P(), wide_spec, wide_spec, down_spec), out_specs=(row_spec, row_spec, P(), P(), wide_spec, wide_spec, down_spec, P(), P()), check_vma=False)
```

```python
import functools

import jax
import jax.numpy as jnp
from jax import lax
from jax.experimental import pallas as pl
from jax.experimental.pallas import tpu as pltpu
from jax.sharding import PartitionSpec as P


NORM_EPS = 1e-6
ACT_COEF = 1e-5
BALANCE_COEF = 1e-3
TILE = 256
LANES = 128
GROUP = 4
REACH = 96
PARTS = (384, 256, 384)
CHUNKS = len(PARTS)
WINDOWS = (1, 2, 3, 4)
VMEM_LIMIT = 67_043_328


def call(kernel, table, operands, in_specs, out_shape, out_specs, scratch, cost, grid=()):
    return pl.pallas_call(
        kernel,
        grid_spec=pltpu.PrefetchScalarGridSpec(
            num_scalar_prefetch=1, grid=grid, in_specs=in_specs, out_specs=out_specs, scratch_shapes=scratch
        ),
        out_shape=out_shape,
        compiler_params=pltpu.CompilerParams(vmem_limit_bytes=VMEM_LIMIT),
        cost_estimate=pl.CostEstimate(flops=cost[0], bytes_accessed=cost[1], transcendentals=0),
    )(table, *operands)


ANY = pl.BlockSpec(memory_space=pl.ANY)
WHOLE = pl.BlockSpec(memory_space=pltpu.VMEM)


def row_block(width):
    return pl.BlockSpec((TILE, width), lambda t: (t, 0))


class Dispatch:
    def __init__(self, at, place, table_ref, pos_ref, prob_ref, tok_hbm, scratch):
        self.at, self.table_ref, self.pos_ref, self.prob_ref, self.tok_hbm = at, table_ref, pos_ref, prob_ref, tok_hbm
        self.tok, self.waited, self.sems = scratch
        self.first, self.spans = at["spans"]
        self.offset, self.stride = place
        self.part = at["part"]

    def span_copy(self, index, row):
        into = pl.ds(index * LANES if isinstance(index, int) else pl.multiple_of(index * LANES, LANES), LANES)
        return pltpu.make_async_copy(self.tok_hbm.at[pl.ds(row, LANES), :], self.tok.at[into, :], self.sems.at[index])

    def begin(self, stream):
        self.waited[0] = 0
        for index in range(self.spans):
            if index == 2 * WINDOWS[-1]:
                stream.begin()
            device, token = divmod(index * LANES, self.part)
            self.span_copy(index, device * self.stride + self.offset + token).start()

    def await_tokens(self, stop_span):
        @pl.loop(self.waited[0], stop_span)
        def _(index):
            self.span_copy(index, 0).wait()

        self.waited[0] = jnp.maximum(self.waited[0], stop_span)

    def end(self):
        self.await_tokens(self.spans)

    def tile(self, x_ref, gate_ref=None):
        tile = pl.program_id(0)
        group = self.table_ref[self.at["group"] + tile]
        width = self.table_ref[self.at["width"] + tile]

        def window(half, count, start):
            row_id = lax.broadcasted_iota(jnp.int32, (LANES, LANES), 0) + (tile * TILE + half * LANES)
            into = pl.ds(half * LANES if isinstance(half, int) else pl.multiple_of(half * LANES, LANES), LANES)
            hot, gate = [], jnp.zeros((LANES, LANES), jnp.float32)
            for q in range(count):
                span = pl.ds(self.first + start + q, 1)
                match = self.pos_ref[group, span, :] == row_id
                hot.append(jnp.where(match, 1.0, 0.0).astype(jnp.bfloat16))
                if gate_ref is not None:
                    gate = gate + jnp.where(match, self.prob_ref[group, span, :], 0.0)
            rows = self.tok[pl.ds(pl.multiple_of(start * LANES, LANES), count * LANES), :]
            out = jnp.dot(jnp.concatenate(hot, axis=1), rows, preferred_element_type=jnp.float32)
            x_ref[into, :] = out.astype(x_ref.dtype)
            if gate_ref is not None:
                gate_ref[into, :] = jnp.broadcast_to(jnp.sum(gate, axis=1, keepdims=True), (LANES, LANES))

        @pl.when(width > WINDOWS[-1])
        def _():
            self.await_tokens(self.spans)

            @pl.loop(0, 2)
            def _(half):
                window(half, self.spans, 0)

        for k in WINDOWS:
            @pl.when(width == k)
            def _(k=k):
                starts = [jnp.minimum(self.table_ref[self.at["lo"] + 2 * tile + half], self.spans - 2 * k) for half in range(2)]
                self.await_tokens(jnp.maximum(starts[0], starts[1]) + 2 * k)
                for half in range(2):
                    window(half, 2 * k, starts[half])


def dispatch_scratch(at, tok):
    spans = at["spans"][1]
    return [pltpu.VMEM((spans * LANES, tok.shape[1]), tok.dtype), pltpu.SMEM((1,), jnp.int32), pltpu.SemaphoreType.DMA((spans,))]


def combine_kernel(at, spans, groups, with_gate, table_ref, pos_ref, rows_hbm, *rest):
    if with_gate:
        gate_hbm, out_ref, gout_ref, rows, gates, waited, sems = rest
    else:
        out_ref, rows, waited, sems = rest
    step = pl.program_id(0)
    steps = pl.num_programs(0)
    row_iota = lax.broadcasted_iota(jnp.int32, (REACH, LANES), 0)
    over = table_ref[at["over"] + step]

    def region(g):
        return table_ref[at["first"] + g], table_ref[at["first"] + g + 1]

    def start_of(g, span):
        return pl.multiple_of(table_ref[at["start"][g] + span], 16)

    def block_copies(index):
        into = pl.ds(pl.multiple_of(index * TILE, TILE), TILE)
        copies = [pltpu.make_async_copy(rows_hbm.at[into, :], rows.at[into, :], sems.at[0, index])]
        if with_gate:
            copies.append(pltpu.make_async_copy(gate_hbm.at[into, :], gates.at[into, :], sems.at[1, index]))
        return copies

    @pl.when(step == 0)
    def _():
        for g in range(groups):
            waited[g] = region(g)[0]
        longest = region(0)[1] - region(0)[0]
        for g in range(1, groups):
            longest = jnp.maximum(longest, region(g)[1] - region(g)[0])

        @pl.loop(0, longest)
        def _(index):
            for g in range(groups):
                begin, stop = region(g)

                @pl.when(begin + index < stop)
                def _(begin=begin):
                    for copy in block_copies(begin + index):
                        copy.start()

    for g in range(groups):
        stop = region(g)[1]
        need = jnp.minimum((start_of(g, (step + 1) * GROUP - 1) + REACH + over * REACH + TILE - 1) // TILE, stop)
        need = jnp.where(step == steps - 1, stop, need)

        @pl.loop(waited[g], need)
        def _(index):
            for copy in block_copies(index):
                copy.wait()

        waited[g] = jnp.maximum(waited[g], need)

    def window(q, second):
        span = step * GROUP + q
        hot, data, gdata = [], [], []
        for g in range(groups):
            begin = place = start_of(g, span)
            if second:
                first, stop = region(g)
                place = pl.multiple_of(jnp.where(first == stop, begin, jnp.minimum(begin + REACH, stop * TILE - REACH)), 16)
                begin = begin + REACH
            row = row_iota + place
            match = pos_ref[g, pl.ds(spans[0] + span, 1), :] == row
            if second:
                match = jnp.logical_and(match, row >= begin)
            hot.append(jnp.where(match, 1.0, 0.0).astype(jnp.bfloat16))
            data.append(rows[pl.ds(place, REACH), :])
            if with_gate:
                gdata.append(gates[pl.ds(place, REACH), :])
        hot = jnp.concatenate(hot, axis=0)
        dims = (((0,), (0,)), ((), ()))
        out = lax.dot_general(hot, jnp.concatenate(data, axis=0), dims, preferred_element_type=jnp.float32)
        if not with_gate:
            return out, None
        exact = jnp.concatenate(gdata, axis=0)
        high = exact.astype(jnp.bfloat16)
        low = (exact - high.astype(jnp.float32)).astype(jnp.bfloat16)
        pair = lax.dot_general(hot, jnp.concatenate([high, low], axis=1), dims, preferred_element_type=jnp.float32)
        return out, pair[:, :LANES] + pair[:, LANES:]

    def put(q, wide):
        out, gate = window(q, False)
        if wide:
            out2, gate2 = window(q, True)
            out = out + out2
            gate = gate + gate2 if with_gate else None
        into = pl.ds(q * LANES if isinstance(q, int) else pl.multiple_of(q * LANES, LANES), LANES)
        out_ref[into, :] = out.astype(out_ref.dtype)
        if with_gate:
            gout_ref[:, into] = jnp.transpose(gate, (1, 0))[:8, :]

    @pl.when(over == 0)
    def _():
        for q in range(GROUP):
            put(q, False)

    @pl.when(over != 0)
    def _():
        @pl.loop(0, GROUP)
        def _(q):
            put(q, True)


def combine(layout, chunk, table, pos, rows, gate_rows=None):
    rows_max, dim = rows.shape
    groups = pos.shape[0]
    spans = layout[chunk]["spans"]
    tokens = spans[1] * LANES
    with_gate = gate_rows is not None
    block = GROUP * LANES
    operands, in_specs = [pos, rows], [WHOLE, ANY]
    out_shape = [jax.ShapeDtypeStruct((tokens, dim), jnp.bfloat16)]
    out_specs = [pl.BlockSpec((block, dim), lambda t, *_: (t, 0))]
    scratch = [pltpu.VMEM((rows_max, dim), jnp.bfloat16)]
    if with_gate:
        operands.append(gate_rows)
        in_specs.append(ANY)
        out_shape.append(jax.ShapeDtypeStruct((8, tokens), jnp.float32))
        out_specs.append(pl.BlockSpec((8, block), lambda t, *_: (0, t)))
        scratch.append(pltpu.VMEM((rows_max, LANES), jnp.float32))
    scratch += [pltpu.SMEM((groups,), jnp.int32), pltpu.SemaphoreType.DMA((2, rows_max // TILE))]
    kernel = functools.partial(combine_kernel, layout[chunk], spans, groups, with_gate)
    return call(kernel, table, operands, in_specs, out_shape, out_specs, scratch, (9 * 10**9, 35 * 10**6), (tokens // block,))


class WeightStream:
    def __init__(self, at, table_ref, weights, scratch):
        self.at, self.table_ref, self.own, self.helped = at, table_ref, weights[:3], weights[3:]
        self.wide, self.down, self.sems = scratch
        self.experts, _, self.ffn = weights[0].shape

    def copies(self, sources, s):
        wg, wu, wd = sources
        return (
            pltpu.make_async_copy(wg, self.wide.at[s, :, pl.ds(0, self.ffn)], self.sems.at[s, 0]),
            pltpu.make_async_copy(wu, self.wide.at[s, :, pl.ds(self.ffn, self.ffn)], self.sems.at[s, 1]),
            pltpu.make_async_copy(wd, self.down.at[s], self.sems.at[s, 2]),
        )

    def start(self, group, s):
        @pl.when(jnp.logical_and(group >= 0, group < self.experts))
        def _():
            for copy in self.copies([w.at[group] for w in self.own], s):
                copy.start()

        @pl.when(group == self.experts)
        def _():
            for copy in self.copies([w.at[0] for w in self.helped], s):
                copy.start()

    def begin(self):
        self.start(self.table_ref[self.at["group"]], 0)

    def slot(self):
        tile = pl.program_id(0)
        s = table_slot = self.table_ref[self.at["slot"] + tile]

        @pl.when(self.table_ref[self.at["fresh"] + tile] != 0)
        def _():
            self.start(self.table_ref[self.at["next"] + tile], 1 - table_slot)
            for copy in self.copies([w.at[0] for w in self.own], table_slot):
                copy.wait()

        return s


def run_tiles(at, table_ref, tile_body, piped_in, piped_out):
    pltpu.emit_pipeline(
        tile_body, grid=(table_ref[at["count"]],),
        in_specs=[row_block(ref.shape[1]) for ref in piped_in],
        out_specs=[row_block(ref.shape[1]) for ref in piped_out],
    )(*piped_in, *piped_out)


def forward_kernel(at, place, table_ref, pos_ref, prob_ref, tok_hbm, *rest):
    stream = WeightStream(at, table_ref, rest[:6], rest[11:14])
    dispatch = Dispatch(at, place, table_ref, pos_ref, prob_ref, tok_hbm, rest[14:])
    wide, down, ffn = stream.wide, stream.down, stream.ffn
    dispatch.begin(stream)

    def tile_body(x_ref, gate_ref, ab_ref, h_ref, out_ref):
        dispatch.tile(x_ref, gate_ref)
        slot = stream.slot()

        def matmuls(height):
            used = slice(0, height)
            x = x_ref[used, :]
            for j in range(ffn // LANES):
                cols = slice(j * LANES, (j + 1) * LANES)
                ucols = slice(ffn + j * LANES, ffn + (j + 1) * LANES)
                both = jnp.dot(x, jnp.concatenate([wide[slot, :, cols], wide[slot, :, ucols]], axis=1), preferred_element_type=jnp.float32)
                a, b = both[:, :LANES], both[:, LANES:]
                ab_ref[used, cols] = a
                ab_ref[used, ucols] = b
                h_ref[used, cols] = (a * jax.nn.sigmoid(a) * b).astype(h_ref.dtype)
            out = jnp.dot(h_ref[used, :], down[slot], preferred_element_type=jnp.float32)
            gate = gate_ref[used, :]
            for j in range(out.shape[1] // LANES):
                cols = slice(j * LANES, (j + 1) * LANES)
                out_ref[used, cols] = (out[:, cols] * gate).astype(out_ref.dtype)

        half = table_ref[at["half"] + pl.program_id(0)] != 0

        @pl.when(jnp.logical_not(half))
        def _():
            matmuls(TILE)

        @pl.when(half)
        def _():
            matmuls(TILE // 2)
            for ref in (ab_ref, h_ref, out_ref):
                ref[TILE // 2:, :] = jnp.zeros((TILE // 2, ref.shape[1]), ref.dtype)

    run_tiles(at, table_ref, tile_body, (), rest[6:11])
    dispatch.end()


def backward_kernel(at, place, table_ref, pos_ref, tok_hbm, ab_hbm, h_hbm, gate_hbm, *rest):
    stream = WeightStream(at, table_ref, rest[:6], rest[10:13])
    m_ref = rest[13]
    dispatch = Dispatch(at, place, table_ref, pos_ref, None, tok_hbm, rest[14:])
    wide, down, ffn = stream.wide, stream.down, stream.ffn
    trans = (((1,), (1,)), ((), ()))
    dispatch.begin(stream)

    def tile_body(ab_ref, h_ref, gate_ref, d_ref, in_ref, mg_ref, dgate_ref):
        dispatch.tile(m_ref)
        slot = stream.slot()
        m = m_ref[...]
        gate = gate_ref[...]
        dgate = jnp.zeros(gate.shape, jnp.float32)
        for c in range(0, ffn, 2 * LANES):
            width = min(2 * LANES, ffn - c)
            raw = lax.dot_general(m, down[slot, c:c + width, :], trans, preferred_element_type=jnp.float32)
            for k in range(width // LANES):
                lo = c + k * LANES
                cols = slice(lo, lo + LANES)
                ucols = slice(ffn + lo, ffn + lo + LANES)
                g = raw[:, k * LANES:(k + 1) * LANES]
                a, b = ab_ref[:, cols], ab_ref[:, ucols]
                sig = jax.nn.sigmoid(a)
                hidden_grad = g * gate
                d_ref[:, cols] = (hidden_grad * b * sig * (1.0 + a * (1.0 - sig))).astype(d_ref.dtype)
                d_ref[:, ucols] = (hidden_grad * (a * sig)).astype(d_ref.dtype)
                dgate = dgate + g * h_ref[:, cols].astype(jnp.float32)
        in_ref[...] = lax.dot_general(d_ref[...], wide[slot], trans, preferred_element_type=jnp.float32).astype(in_ref.dtype)
        for j in range(m.shape[1] // LANES):
            cols = slice(j * LANES, (j + 1) * LANES)
            mg_ref[:, cols] = (m[:, cols].astype(jnp.float32) * gate).astype(mg_ref.dtype)
        lane = lax.broadcasted_iota(jnp.int32, gate.shape, 1)
        expert = table_ref[at["expert"] + table_ref[at["group"] + pl.program_id(0)]]
        dgate_ref[...] = jnp.where(lane == expert, jnp.sum(dgate, axis=1, keepdims=True), 0.0)

    run_tiles(at, table_ref, tile_body, (ab_hbm, h_hbm, gate_hbm), rest[6:10])
    dispatch.end()


def weight_scratch(wg):
    _, dim, ffn = wg.shape
    return [
        pltpu.VMEM((2, dim, 2 * ffn), wg.dtype),
        pltpu.VMEM((2, ffn, dim), wg.dtype),
        pltpu.SemaphoreType.DMA((2, 3)),
    ]


def shapes(rows_max, *kinds):
    return [jax.ShapeDtypeStruct((rows_max, width), dtype) for width, dtype in kinds]


def forward(layout, chunk, table, pos, prob, tokens, weights):
    _, dim, ffn = weights[0].shape
    kinds = ((dim, jnp.bfloat16), (LANES, jnp.float32), (2 * ffn, jnp.float32), (ffn, jnp.bfloat16), (dim, jnp.bfloat16))
    at = layout[chunk]
    tok, place = tokens
    return call(
        functools.partial(forward_kernel, at, place), table, (pos, prob, tok, *weights), [WHOLE, WHOLE] + [ANY] * 7,
        shapes(at["rows_max"], *kinds), [ANY] * 5, weight_scratch(weights[0]) + dispatch_scratch(at, tok), (75 * 10**9, 150 * 10**6),
    )


def backward(layout, chunk, table, pos, tok, ab, hidden, gates, weights):
    _, dim, ffn = weights[0].shape
    kinds = ((2 * ffn, jnp.bfloat16), (dim, jnp.bfloat16), (dim, jnp.bfloat16), (LANES, jnp.float32))
    at = layout[chunk]
    scratch = [*weight_scratch(weights[0]), pltpu.VMEM((TILE, dim), jnp.bfloat16), *dispatch_scratch(at, tok)]
    return call(
        functools.partial(backward_kernel, at, (0, at["part"])), table, (pos, tok, ab, hidden, gates, *weights), [WHOLE] + [ANY] * 10,
        shapes(at["rows_max"], *kinds), [ANY] * 4, scratch, (75 * 10**9, 150 * 10**6),
    )


def weight_grad_kernel(at, tiles_max, outs, groups, carried, table_ref, *rest):
    lhs_hbm, rhs_hbm, back, rest = rest[:CHUNKS], rest[CHUNKS:2 * CHUNKS], rest[2 * CHUNKS:2 * CHUNKS + carried], rest[2 * CHUNKS + 2 * carried - bool(carried):]
    own_out, rest = (rest[:outs], rest[outs:]) if groups != "helped" else ((), rest)
    helped_out, rest = (rest[:outs], rest[outs:]) if groups != "own" else ((), rest)
    filled, rest = ((*rest[:carried - 1], own_out[0]), rest[carried - 1:]) if carried else ((), rest)
    lhs, rhs, lhs_t, acc, staged, pending, sems, out_sems = rest[:8]
    experts = at["experts"]
    begin = table_ref[at["own_steps"]] if groups == "helped" else 0
    steps = table_ref[at["own_steps" if groups == "own" else "steps"]]

    def copies(chunk, row, s, half):
        source = pl.ds(pl.multiple_of(row, TILE), TILE)
        into = pl.ds(half * TILE, TILE)
        return (
            pltpu.make_async_copy(lhs_hbm[chunk].at[source, :], lhs.at[s, into, :], sems.at[s, half, 0]),
            pltpu.make_async_copy(rhs_hbm[chunk].at[source, :], rhs.at[s, into, :], sems.at[s, half, 1]),
        )

    def start(index, s):
        for half in range(2):
            src = table_ref[at["src"] + 2 * index + half]
            for chunk in range(CHUNKS):
                @pl.when(jnp.logical_and(src >= chunk * tiles_max, src < (chunk + 1) * tiles_max))
                def _(chunk=chunk, src=src, half=half):
                    for copy in copies(chunk, (src - chunk * tiles_max) * TILE, s, half):
                        copy.start()

    def out_copies(targets):
        return [pltpu.make_async_copy(staged.at[i], target, out_sems.at[i]) for i, target in enumerate(targets)]

    def drain():
        @pl.when(pending[0] != 0)
        def _():
            for copy in out_copies([out.at[0] for out in (own_out or helped_out)]):
                copy.wait()

        pending[0] = 0

    pending[0] = 0

    @pl.when(begin < steps)
    def _():
        start(begin, lax.rem(begin, 2))

    place = table_ref[at["insert"]]
    if carried:
        *bounce, fetch_sems, store_sems = rest[8:]
        fetch = [pltpu.make_async_copy(back[i].at[0], bounce[i], fetch_sems.at[i]) for i in range(carried)]
        store = [pltpu.make_async_copy(bounce[i], filled[i].at[jnp.maximum(place, 0)], store_sems.at[i]) for i in range(carried)]

        @pl.when(place >= 0)
        def _():
            for copy in fetch:
                copy.start()

    def accumulate(slot, fresh, depth):
        lhs_t[:, :depth] = jnp.transpose(lhs[slot, :depth, :], (1, 0))
        block = 2 * LANES
        for c in range(0, acc.shape[1], block):
            part = jnp.dot(lhs_t[:, :depth], rhs[slot, :depth, c:c + block], preferred_element_type=jnp.float32)
            acc[:, c:c + block] = jnp.where(fresh, 0.0, acc[:, c:c + block]) + part

    @pl.loop(begin, steps)
    def _(step):
        slot = lax.rem(step, 2)
        group = table_ref[at["owner"] + step]

        @pl.when(step + 1 < steps)
        def _():
            start(step + 1, 1 - slot)

        if carried:
            @pl.when(jnp.logical_and(place >= 0, step == begin + (steps - begin) // 2))
            def _():
                for one, other in zip(fetch, store):
                    one.wait()
                    other.start()

        fresh = jnp.logical_or(step == begin, group != table_ref[at["owner"] + jnp.maximum(step - 1, 0)])
        last = jnp.logical_or(step == steps - 1, group != table_ref[at["owner"] + step + 1])
        pair = table_ref[at["src"] + 2 * step + 1] >= 0
        for copy in copies(0, 0, slot, 0):
            copy.wait()

        @pl.when(pair)
        def _():
            for copy in copies(0, 0, slot, 1):
                copy.wait()
            accumulate(slot, fresh, 2 * TILE)

        @pl.when(jnp.logical_not(pair))
        def _():
            accumulate(slot, fresh, TILE)

        @pl.when(last)
        def _():
            drain()
            width = acc.shape[1] // outs
            for i in range(outs):
                staged[i, :, :] = acc[:, i * width:(i + 1) * width].astype(staged.dtype)

            if own_out:
                @pl.when(group < experts)
                def _():
                    for copy in out_copies([out.at[group] for out in own_out]):
                        copy.start()

            if helped_out:
                @pl.when(group == experts)
                def _():
                    for copy in out_copies([out.at[0] for out in helped_out]):
                        copy.start()

            pending[0] = 1

    drain()
    if carried:
        @pl.when(place >= 0)
        def _():
            @pl.when(begin >= steps)
            def _():
                for one, other in zip(fetch, store):
                    one.wait()
                    other.start()

            for copy in store:
                copy.wait()


def weight_grad(layout, table, lhs, rhs, experts, outs, groups="all", back=(), grads=()):
    left, right = lhs[0].shape[1], rhs[0].shape[1]
    width = right // outs
    carried = len(back)
    scratch = [
        pltpu.VMEM((2, 2 * TILE, left), jnp.bfloat16),
        pltpu.VMEM((2, 2 * TILE, right), jnp.bfloat16),
        pltpu.VMEM((left, 2 * TILE), jnp.bfloat16),
        pltpu.VMEM((left, right), jnp.float32),
        pltpu.VMEM((outs, left, width), jnp.bfloat16),
        pltpu.SMEM((1,), jnp.int32),
        pltpu.SemaphoreType.DMA((2, 2, 2)),
        pltpu.SemaphoreType.DMA((outs,)),
    ]
    if carried:
        scratch += [pltpu.VMEM(b.shape[1:], b.dtype) for b in back]
        scratch += [pltpu.SemaphoreType.DMA((carried,)), pltpu.SemaphoreType.DMA((carried,))]
    counts = ([experts] * outs if groups != "helped" else []) + ([1] * outs if groups != "own" else [])
    out_shape = [jax.ShapeDtypeStruct((n, left, width), jnp.bfloat16) for n in counts]
    first = len(out_shape)
    out_shape += [jax.ShapeDtypeStruct(g.shape, g.dtype) for g in grads]
    operands = (*lhs, *rhs, *back, *grads)
    at = layout["grad"] | {"experts": experts}
    return pl.pallas_call(
        functools.partial(weight_grad_kernel, at, layout["tiles_max"], outs, groups, carried),
        grid_spec=pltpu.PrefetchScalarGridSpec(
            num_scalar_prefetch=1, in_specs=[ANY] * len(operands), out_specs=[ANY] * len(out_shape), scratch_shapes=scratch
        ),
        out_shape=out_shape,
        input_output_aliases={1 + 2 * CHUNKS + carried + i: first + i for i in range(len(grads))},
        compiler_params=pltpu.CompilerParams(vmem_limit_bytes=VMEM_LIMIT),
        cost_estimate=pl.CostEstimate(flops=(400 if groups == "helped" else 2000) * 9 * left * right, bytes_accessed=100 * 10**6, transcendentals=0),
        name="weight_grad",
    )(table, *operands)


def row_blocks(height, dim):
    specs, first = [], 0
    for part in PARTS:
        blocks = part // height
        specs.append(pl.BlockSpec((height, dim), lambda t, *_, first=first, last=blocks - 1: (jnp.clip(t - first, 0, last), 0)))
        first += blocks
    return specs


def of_this_chunk(height, refs):
    step, first, value = pl.program_id(0), 0, None
    for part, ref in zip(PARTS, refs):
        value = ref[...] if value is None else jnp.where(step >= first, ref[...], value)
        first += part // height
    return value


def norm_kernel(x_ref, gain_ref, out_ref):
    x = x_ref[...].astype(jnp.float32)
    inv_rms = lax.rsqrt(jnp.mean(x * x, axis=-1, keepdims=True) + NORM_EPS)
    out_ref[...] = (x * inv_rms * gain_ref[...]).astype(out_ref.dtype)


def normalize(x, gain, first, count):
    dim = x.shape[1]
    height = LANES
    return pl.pallas_call(
        norm_kernel,
        grid=(count // height,),
        in_specs=[pl.BlockSpec((height, dim), lambda t: (t + first // height, 0)), pl.BlockSpec((1, dim), lambda t: (0, 0))],
        out_specs=pl.BlockSpec((height, dim), lambda t: (t, 0)),
        out_shape=jax.ShapeDtypeStruct((count, dim), jnp.bfloat16),
        cost_estimate=pl.CostEstimate(flops=10**7, bytes_accessed=4 * 10**6, transcendentals=0),
        name="normalize",
    )(x, gain.reshape(1, dim))


def finish_kernel(x_ref, y_grad_ref, prob_ref, gate_grad_ref, balance_ref, gain_ref, router_ref, *rest):
    in_refs, out_refs, (y_ref, x_grad_ref, stats_ref) = rest[:CHUNKS], rest[CHUNKS:2 * CHUNKS], rest[2 * CHUNKS:]
    height = x_ref.shape[0]
    prob = prob_ref[...]
    prob_grad = gate_grad_ref[...] + balance_ref[...]
    logit_grad = (prob * (prob_grad - jnp.sum(prob * prob_grad, axis=0, keepdims=True))).astype(jnp.bfloat16)
    x = x_ref[...].astype(jnp.float32)
    inv_rms = lax.rsqrt(jnp.mean(x * x, axis=-1, keepdims=True) + NORM_EPS)
    unit = x * inv_rms
    gain = gain_ref[...]
    moe_out = of_this_chunk(height, out_refs).astype(jnp.float32)
    y_ref[...] = (x + moe_out).astype(y_ref.dtype)
    routed = lax.dot_general(logit_grad, router_ref[...], (((0,), (0,)), ((), ())), preferred_element_type=jnp.float32)
    x_norm_grad = of_this_chunk(height, in_refs).astype(jnp.float32) + routed
    unit_grad = x_norm_grad * gain
    x_grad = y_grad_ref[...].astype(jnp.float32) + inv_rms * (unit_grad - unit * jnp.mean(unit_grad * unit, axis=-1, keepdims=True))
    x_grad_ref[...] = x_grad.astype(x_grad_ref.dtype)
    x_norm = (unit * gain).astype(jnp.bfloat16)

    @pl.when(pl.program_id(0) == 0)
    def _():
        stats_ref[...] = jnp.zeros_like(stats_ref)

    def folded(values):
        return jnp.sum(values.reshape(height // 8, 8, values.shape[1]), axis=0)

    stats_ref[0:8, :] += jnp.dot(logit_grad, x_norm, preferred_element_type=jnp.float32)
    stats_ref[8:16, :] += folded(x_norm_grad * unit)
    stats_ref[16:24, :] += folded(moe_out * moe_out)


def finish(x, y_grad, prob, gate_grad, balance, gain, router, in_raw, out_raw):
    tokens, dim = x.shape
    height = LANES
    rows = pl.BlockSpec((height, dim), lambda t: (t, 0))
    of_tokens = pl.BlockSpec((8, height), lambda t: (0, t))
    return pl.pallas_call(
        finish_kernel,
        grid=(tokens // height,),
        in_specs=[
            rows, rows, of_tokens, of_tokens, pl.BlockSpec((8, height), lambda t: (0, 0)), pl.BlockSpec((1, dim), lambda t: (0, 0)),
            pl.BlockSpec((8, dim), lambda t: (0, 0)), *row_blocks(height, dim), *row_blocks(height, dim),
        ],
        out_specs=[rows, rows, pl.BlockSpec((32, dim), lambda t: (0, 0))],
        out_shape=[
            jax.ShapeDtypeStruct((tokens, dim), jnp.bfloat16), jax.ShapeDtypeStruct((tokens, dim), jnp.bfloat16),
            jax.ShapeDtypeStruct((32, dim), jnp.float32),
        ],
        compiler_params=pltpu.CompilerParams(vmem_limit_bytes=VMEM_LIMIT),
        cost_estimate=pl.CostEstimate(flops=10**9, bytes_accessed=25 * 10**6, transcendentals=0),
        name="finish",
    )(x, y_grad, prob, gate_grad, balance, gain.reshape(1, dim), router, *in_raw, *out_raw)


def below(size, strict):
    i = lax.broadcasted_iota(jnp.int32, (size, size), 0)
    j = lax.broadcasted_iota(jnp.int32, (size, size), 1)
    return (i < j if strict else i <= j).astype(jnp.float32)


def running(values):
    size = values.shape[-1]
    i = lax.broadcasted_iota(jnp.int32, (size, size), 0)
    j = lax.broadcasted_iota(jnp.int32, (size, size), 1)
    return jnp.sum(jnp.where(i <= j, values[..., :, None], 0), axis=-2)


def count(condition, axis):
    return jnp.sum(condition.astype(jnp.int32), axis=axis)


def choose_swap(rows, experts):
    work = 4 * ((rows + TILE - 1) // TILE) + (rows + TILE // 2 - 1) // (TILE // 2)
    none = jnp.zeros((rows.shape[0], 1), jnp.int32)
    sides = [work[:, :experts], work[:, experts:]]
    options = [jnp.concatenate([none, side], axis=1) for side in sides]
    moved = options[1][:, None, :] - options[0][:, :, None]
    loads = [jnp.sum(side, axis=1)[:, None, None] for side in sides]
    cost = jnp.sum(jnp.maximum(loads[0] + moved, loads[1] - moved), axis=0)
    index = lax.broadcasted_iota(jnp.int32, cost.shape, 0) * (experts + 1) + lax.broadcasted_iota(jnp.int32, cost.shape, 1)
    best = jnp.min(jnp.where(cost == jnp.min(cost), index, cost.size))
    return best // (experts + 1) - 1, best % (experts + 1) - 1


def routing(hot, experts_of, place):
    groups, span_total, _ = hot.shape
    spans_of = [part * (span_total * LANES // sum(PARTS)) // LANES for part in PARTS]
    firsts = [sum(spans_of[:c]) for c in range(CHUNKS)]
    chunk_of = jnp.concatenate([jnp.full((n,), c, jnp.int32) for c, n in enumerate(spans_of)])
    member = chunk_of[:, None] == jnp.arange(CHUNKS, dtype=jnp.int32)[None, :]
    same = chunk_of[:, None] == chunk_of[None, :]
    tiles_of = [2 * n * LANES // TILE + groups for n in spans_of]
    tiles_max = max(tiles_of)

    within = jnp.einsum("gsi,ij->gsj", hot, below(LANES, False), preferred_element_type=jnp.float32)
    span_count = jnp.sum(hot, axis=-1)
    before = jnp.einsum("gi,ij->gj", span_count, jnp.where(same, below(span_total, True), 0.0), preferred_element_type=jnp.float32)
    total = jnp.sum(jnp.where(member[:, None, :], span_count.T[:, :, None], 0.0), axis=0).T.astype(jnp.int32)
    tiles = (total + TILE - 1) // TILE
    none = jnp.logical_and(jnp.sum(tiles, axis=1, keepdims=True) == 0, jnp.arange(groups, dtype=jnp.int32) == 0)
    tiles = jnp.where(none, 1, tiles)
    stop = running(tiles)
    begin = stop - tiles

    def to_spans(values):
        return jnp.sum(jnp.where(member[None], values.T[:, None, :], 0), axis=2)

    span_first = to_spans(begin) * TILE + before.astype(jnp.int32)
    span_stop = span_first + span_count.astype(jnp.int32)
    pos = jnp.where(hot > 0, span_first[:, :, None] + within.astype(jnp.int32) - 1, -1)

    index = jnp.arange(groups, dtype=jnp.int32)
    tile = jnp.arange(tiles_max, dtype=jnp.int32)
    group = jnp.minimum(count(tile[None, :, None] >= stop[:, None, :], 2), groups - 1)
    mine = group[:, :, None] == index
    ordinal = running((tiles > 0).astype(jnp.int32)) - 1
    later = jnp.logical_and(index[None, None, :] > group[:, :, None], tiles[:, None, :] > 0)
    follow = jnp.min(jnp.where(later, index, groups), axis=2)
    follow = jnp.where(follow == groups, -1, follow)
    fresh = jnp.sum(jnp.where(mine, begin[:, None, :], 0), axis=2) == tile
    slot = jnp.sum(jnp.where(mine, ordinal[:, None, :], 0), axis=2) % 2
    rows_left = jnp.sum(jnp.where(mine, (total + begin * TILE)[:, None, :], 0), axis=2) - tile * TILE
    half = rows_left <= TILE // 2

    half_mine = jnp.repeat(mine, 2, axis=1)
    stops = jnp.sum(jnp.where(half_mine[..., None], span_stop[None, None], 0), axis=2)
    row0 = jnp.arange(2 * tiles_max, dtype=jnp.int32)[None, :, None] * LANES
    inside = member.T[:, None, :]
    lo = count(jnp.logical_and(inside, stops <= row0), 2)
    hi = jnp.minimum(count(jnp.logical_and(inside, stops < row0 + LANES), 2), jnp.array(spans_of, jnp.int32)[:, None] - 1)
    width = jnp.maximum(jnp.max(((hi - lo + 2) // 2).reshape(CHUNKS, tiles_max, 2), axis=2), 1)
    start = jnp.minimum(span_first // 16 * 16, to_spans(stop) * TILE - REACH)
    empty = to_spans(tiles) == 0
    leading = jnp.logical_and(jnp.logical_not(empty), to_spans(ordinal) == 0)
    start = jnp.where(empty, jnp.sum(jnp.where(leading, start, 0), axis=0), start)
    over = jnp.any(jnp.logical_and(jnp.logical_not(empty), span_stop - start > REACH), axis=0)
    over = jnp.any(over.reshape(-1, GROUP), axis=1)

    in_chunks = running(tiles.T)
    both = in_chunks[:, -1]
    step_stop = running((both + 1) // 2)
    step_first = step_stop - (both + 1) // 2
    steps = CHUNKS * tiles_max // 2 + groups
    step = jnp.arange(steps, dtype=jnp.int32)
    owner = jnp.minimum(count(step[:, None] >= step_stop[None, :], 1), groups - 1)
    step_mine = owner[:, None] == index

    def of_step(values):
        return jnp.sum(jnp.where(step_mine[:, :, None], values[None], 0), axis=1)[:, None, :]

    local = 2 * (step - of_step(step_first[:, None])[:, 0, 0])[:, None, None] + jnp.arange(2, dtype=jnp.int32)[None, :, None]
    ends, sizes = of_step(in_chunks), of_step(tiles.T)
    offset = local - (ends - sizes)
    found = jnp.logical_and(offset >= 0, local < ends)
    chunk_at = jnp.arange(CHUNKS, dtype=jnp.int32) * tiles_max
    src = jnp.sum(jnp.where(found, of_step(begin.T) + offset + chunk_at + 1, 0), axis=2) - 1

    sections = (
        ("expert", experts_of), ("insert", place.reshape(1)), ("steps", step_stop[-1:]), ("own_steps", step_first[-1:]), ("owner", owner), ("src", src),
        ("count", stop[:, -1:]), ("group", group), ("slot", slot), ("fresh", fresh), ("half", half), ("next", follow), ("lo", lo), ("width", width),
        ("first", jnp.concatenate([jnp.zeros((CHUNKS, 1), jnp.int32), stop], axis=1)), ("start", start), ("over", over),
    )
    table = jnp.concatenate([values.reshape(-1).astype(jnp.int32) for _, values in sections])
    places, sizes_of, at = {}, {}, 0
    for name, values in sections:
        places[name], sizes_of[name] = at, values.size
        at += values.size
    layout = {}
    for c in range(CHUNKS):
        layout[c] = {name: places[name] + c * (sizes_of[name] // CHUNKS) for name in ("count", "group", "slot", "fresh", "half", "next", "lo", "width", "first")}
        layout[c] |= {
            "expert": places["expert"], "spans": (firsts[c], spans_of[c]), "part": PARTS[c], "rows_max": tiles_of[c] * TILE,
            "start": [places["start"] + g * span_total + firsts[c] for g in range(groups)],
            "over": places["over"] + firsts[c] // GROUP,
        }
    layout |= {"grad": {name: places[name] for name in ("steps", "own_steps", "owner", "src", "insert")}, "insert": places["insert"], "tiles_max": tiles_max}
    return pos, table, layout


def solution(mesh):
    tp_size = mesh.shape["tp"]
    ep_size = mesh.shape["ep"]
    dev_count = tp_size * ep_size
    rows_axes = ("ep", "tp")
    row_spec = P(rows_axes, None)
    wide_spec = P("ep", None, "tp")
    down_spec = P("ep", "tp", None)
    swap = [(0, 1), (1, 0)]

    def body(x, y_grad, expert_ids, norm_gain, w_router, w_gate, w_up, w_down):
        tokens, model_dim = x.shape
        top_k = expert_ids.shape[1]
        num_experts = w_router.shape[1]
        local_experts = w_gate.shape[0]
        total_tokens = tokens * dev_count
        my_ep = lax.axis_index("ep").astype(jnp.int32)
        firsts = [sum(PARTS[:c]) for c in range(CHUNKS)]

        def of_chunk(rows, c, axis=0):
            return lax.slice_in_dim(rows, firsts[c], firsts[c] + PARTS[c], axis=axis)

        def gather(rows):
            return lax.all_gather(rows, rows_axes, axis=0, tiled=True)

        def scatter(rows):
            return lax.psum_scatter(rows, rows_axes, scatter_dimension=0, tiled=True)

        def of_chunk_span(values, c):
            return values[:, firsts[c] * dev_count:(firsts[c] + PARTS[c]) * dev_count]

        def after(values, first):
            return lax.optimization_barrier((values, first))

        gain = norm_gain.astype(jnp.float32)
        rest = tokens - PARTS[0]
        head, tail = normalize(x, gain, 0, PARTS[0]), normalize(x, gain, PARTS[0], rest)
        gathered = [gather(head), gather(tail)]
        tok = [(gathered[0], (0, PARTS[0]))] + [(gathered[1], (firsts[c] - PARTS[0], rest)) for c in range(1, CHUNKS)]

        x_norm = jnp.concatenate([head, tail], axis=0)
        route_prob = jax.nn.softmax(jnp.dot(x_norm, w_router, preferred_element_type=jnp.float32), axis=-1)
        expert_range = jnp.arange(num_experts, dtype=jnp.int32)
        choice = jnp.sum((expert_ids[:, :, None] == expert_range[None, None, :]).astype(jnp.float32), axis=1)
        small = lax.all_gather(jnp.concatenate([choice, route_prob], axis=1).T, rows_axes, axis=0, tiled=False)
        counts = jnp.sum(small[:, :num_experts], axis=(0, 2))
        balance_scale = BALANCE_COEF * num_experts / (total_tokens * total_tokens * top_k)
        balance_loss = balance_scale * jnp.sum(counts * jnp.sum(small[:, num_experts:], axis=(0, 2)))

        rows_in = jnp.stack([jnp.sum(of_chunk(small[:, :num_experts], c, 2), axis=(0, 2)) for c in range(CHUNKS)])
        gives = choose_swap(rows_in.astype(jnp.int32), local_experts)
        given = jnp.where(my_ep == 0, gives[0], gives[1])
        taken = jnp.where(my_ep == 0, gives[1], gives[0])
        my_base = my_ep * local_experts
        local = jnp.arange(local_experts, dtype=jnp.int32)
        group_experts = jnp.concatenate([my_base + local, (local_experts - my_base + jnp.maximum(taken, 0)).reshape(1)])
        active = jnp.concatenate([local != given, (taken >= 0).reshape(1)])
        take = jnp.logical_and(group_experts[:, None] == expert_range, active[:, None])
        spread = jnp.concatenate([of_chunk(small, c, 2).transpose(1, 0, 2).reshape(2 * num_experts, -1) for c in range(CHUNKS)], axis=1)
        spread = spread.reshape(2, 1, num_experts, -1, LANES)
        own = jnp.sum(jnp.where(take[None, :, :, None, None], spread, 0.0), axis=2)
        prob = own[1]
        pos, table, layout = routing(own[0], group_experts, given)
        helped = [lax.ppermute(lax.dynamic_slice_in_dim(w, jnp.maximum(given, 0), 1, axis=0), "ep", swap) for w in (w_gate, w_up, w_down)]
        weights = (w_gate, w_up, w_down, *helped)

        grad_scale = 2.0 * ACT_COEF / (total_tokens * model_dim)
        own_prob = route_prob.T
        balance_row = jnp.broadcast_to(balance_scale * counts[:, None], (num_experts, LANES))
        router = w_router.T
        first_tok, (own_prob, balance_row, router, balance_loss) = after(tok[0][0], (own_prob, balance_row, router, balance_loss))
        tok[0] = (first_tok, tok[0][1])
        x_rows, gate_rows, pre, hidden, d_rows, mg_rows = [], [], [], [], [], []
        out_raw, moe_out, m_own, m_tok, in_raw, gate_part = [], [], [], [], [], []

        def send_cotangent(c, gate):
            raw, (gate, _) = after(out_raw[c], (gate, m_own[-1:]))
            moe_out.append(raw)
            moe_grad = of_chunk(y_grad, c).astype(jnp.float32) + grad_scale * raw.astype(jnp.float32)
            m_own.append(moe_grad.astype(jnp.bfloat16))
            m_tok.append(gather(m_own[c]))
            return gate

        for c in range(CHUNKS):
            rows, gates, ab, h, out_rows = forward(layout, c, table, pos, prob, tok[c], weights)
            if c == 1:
                out_rows = send_cotangent(0, out_rows)
            (partial,) = combine(layout, c, table, pos, out_rows)
            if c == 0:
                partial, later = after(partial, gathered[1])
                tok[1:] = [(later, place) for _, place in tok[1:]]
            if c > 1:
                partial = send_cotangent(c - 1, partial)
            out_raw.append(scatter(partial))
            x_rows.append(rows)
            gate_rows.append(gates)
            pre.append(ab)
            hidden.append(h)
        for c in range(CHUNKS):
            d, in_rows, mg, dgate = backward(layout, c, table, pos, m_tok[c], pre[c], hidden[c], gate_rows[c], weights)
            if c == 0:
                in_rows = send_cotangent(CHUNKS - 1, in_rows)
            partial, gate_terms = combine(layout, c, table, pos, in_rows, dgate)
            if c == 0:
                m_tok[1], partial = after(m_tok[1], partial)
            in_raw.append(scatter(partial))
            gate_part.append(gate_terms)
            d_rows.append(d)
            mg_rows.append(mg)
        *wide_grads, helped_gate, helped_up = weight_grad(layout, table, x_rows, d_rows, local_experts, 2)
        back = []
        for grad in (helped_gate, helped_up):
            back.append(lax.ppermute(grad, "ep", swap))

        mg_rows[0], _ = after(mg_rows[0], wide_grads[0])
        (helped_down,) = weight_grad(layout, table, hidden, mg_rows, local_experts, 1, "helped")
        back.append(lax.ppermute(helped_down, "ep", swap))

        gate_sums = lax.psum(jnp.concatenate(gate_part, axis=1), ("tp", "ep"))
        device = my_ep * tp_size + lax.axis_index("tp")
        gate_sums = [
            lax.dynamic_slice_in_dim(of_chunk_span(gate_sums, c), device * PARTS[c], PARTS[c], axis=1) for c in range(CHUNKS)
        ]
        gate_weight_grad = jnp.concatenate(gate_sums, axis=1)
        gate_weight_grad, (helped_down, in_raw) = after(gate_weight_grad, (helped_down, in_raw))
        y, x_grad, stats = finish(x, y_grad, own_prob, gate_weight_grad, balance_row, gain, router, in_raw, moe_out)
        stats, (mg_rows[0], x_grad) = after(stats, (mg_rows[0], x_grad))
        down_grad, gate_grad, up_grad = weight_grad(layout, table, hidden, mg_rows, local_experts, 1, "own", back, wide_grads)
        stats = lax.psum(stats, ("tp", "ep"))
        router_sum = stats[:num_experts].T
        gain_sum = jnp.sum(stats[8:16], axis=0)
        act_loss = ACT_COEF * jnp.sum(stats[16:24]) / (total_tokens * model_dim)
        return (y, x_grad, gain_sum.astype(jnp.bfloat16), router_sum.astype(jnp.bfloat16), gate_grad, up_grad, down_grad, balance_loss, act_loss)

    return jax.shard_map(body, mesh=mesh, in_specs=(row_spec, row_spec, row_spec, P(), P(), wide_spec, wide_spec, down_spec), out_specs=(row_spec, row_spec, P(), P(), wide_spec, wide_spec, down_spec, P(), P()), check_vma=False)
```

```python
import functools

import jax
import jax.numpy as jnp
from jax import lax
from jax.experimental import pallas as pl
from jax.experimental.pallas import tpu as pltpu
from jax.sharding import PartitionSpec as P


NORM_EPS = 1e-6
ACT_COEF = 1e-5
BALANCE_COEF = 1e-3
TILE = 256
LANES = 128
GROUP = 4
REACH = 96
PARTS = (384, 256, 384)
CHUNKS = len(PARTS)
WINDOWS = (1, 2, 3, 4)
WIDE_WINDOWS = (6, 8)
WHOLE_CHUNK = 99
VMEM_LIMIT = 67_043_328


def call(kernel, table, operands, in_specs, out_shape, out_specs, scratch, cost, grid=()):
    return pl.pallas_call(
        kernel,
        grid_spec=pltpu.PrefetchScalarGridSpec(
            num_scalar_prefetch=1, grid=grid, in_specs=in_specs, out_specs=out_specs, scratch_shapes=scratch
        ),
        out_shape=out_shape,
        compiler_params=pltpu.CompilerParams(vmem_limit_bytes=VMEM_LIMIT),
        cost_estimate=pl.CostEstimate(flops=cost[0], bytes_accessed=cost[1], transcendentals=0),
    )(table, *operands)


ANY = pl.BlockSpec(memory_space=pl.ANY)
WHOLE = pl.BlockSpec(memory_space=pltpu.VMEM)


def row_block(width):
    return pl.BlockSpec((TILE, width), lambda t: (t, 0))


class Dispatch:
    def __init__(self, at, place, table_ref, pos_ref, prob_ref, tok_hbm, scratch):
        self.at, self.table_ref, self.pos_ref, self.prob_ref, self.tok_hbm = at, table_ref, pos_ref, prob_ref, tok_hbm
        self.tok, self.waited, self.sems = scratch
        self.first, self.spans = at["spans"]
        self.offset, self.stride = place
        self.part = at["part"]

    def span_copy(self, index, row):
        into = pl.ds(index * LANES if isinstance(index, int) else pl.multiple_of(index * LANES, LANES), LANES)
        return pltpu.make_async_copy(self.tok_hbm.at[pl.ds(row, LANES), :], self.tok.at[into, :], self.sems.at[index])

    def begin(self, stream):
        self.waited[0] = 0
        for index in range(self.spans):
            if index == 2 * WINDOWS[-1]:
                stream.begin()
            device, token = divmod(index * LANES, self.part)
            self.span_copy(index, device * self.stride + self.offset + token).start()

    def await_tokens(self, stop_span):
        @pl.loop(self.waited[0], stop_span)
        def _(index):
            self.span_copy(index, 0).wait()

        self.waited[0] = jnp.maximum(self.waited[0], stop_span)

    def end(self):
        self.await_tokens(self.spans)

    def tile(self, x_ref, gate_ref=None):
        tile = pl.program_id(0)
        group = self.table_ref[self.at["group"] + tile]
        width = self.table_ref[self.at["width"] + tile]

        def window(half, count, start):
            row_id = lax.broadcasted_iota(jnp.int32, (LANES, LANES), 0) + (tile * TILE + half * LANES)
            into = pl.ds(half * LANES if isinstance(half, int) else pl.multiple_of(half * LANES, LANES), LANES)
            hot, gate = [], jnp.zeros((LANES, LANES), jnp.float32)
            for q in range(count):
                span = pl.ds(self.first + start + q, 1)
                match = self.pos_ref[group, span, :] == row_id
                hot.append(jnp.where(match, 1.0, 0.0).astype(jnp.bfloat16))
                if gate_ref is not None:
                    gate = gate + jnp.where(match, self.prob_ref[group, span, :], 0.0)
            rows = self.tok[pl.ds(pl.multiple_of(start * LANES, LANES), count * LANES), :]
            out = jnp.dot(jnp.concatenate(hot, axis=1), rows, preferred_element_type=jnp.float32)
            x_ref[into, :] = out.astype(x_ref.dtype)
            if gate_ref is not None:
                gate_ref[into, :] = jnp.broadcast_to(jnp.sum(gate, axis=1, keepdims=True), (LANES, LANES))

        halves = 2 - self.table_ref[self.at["half"] + tile]

        def start_of(half, count):
            return jnp.minimum(self.table_ref[self.at["lo"] + 2 * tile + half], self.spans - count)

        def one_by_one(count):
            self.await_tokens(jnp.maximum(start_of(0, count), start_of(1, count)) + count)

            @pl.loop(0, halves)
            def _(half):
                window(half, count, start_of(half, count))

            @pl.when(halves == 1)
            def _():
                for ref in (x_ref,) if gate_ref is None else (x_ref, gate_ref):
                    ref[LANES:, :] = jnp.zeros((TILE - LANES, ref.shape[1]), ref.dtype)

        @pl.when(width == WHOLE_CHUNK)
        def _():
            one_by_one(self.spans)

        for k in WIDE_WINDOWS:
            @pl.when(width == k)
            def _(k=k):
                one_by_one(2 * k)

        for k in WINDOWS:
            @pl.when(width == k)
            def _(k=k):
                starts = [start_of(half, 2 * k) for half in range(2)]
                self.await_tokens(jnp.maximum(starts[0], starts[1]) + 2 * k)
                for half in range(2):
                    window(half, 2 * k, starts[half])


def dispatch_scratch(at, tok):
    spans = at["spans"][1]
    return [pltpu.VMEM((spans * LANES, tok.shape[1]), tok.dtype), pltpu.SMEM((1,), jnp.int32), pltpu.SemaphoreType.DMA((spans,))]


def combine_kernel(at, spans, groups, with_gate, table_ref, pos_ref, rows_hbm, *rest):
    if with_gate:
        gate_hbm, out_ref, gout_ref, rows, gates, waited, sems = rest
    else:
        out_ref, rows, waited, sems = rest
    step = pl.program_id(0)
    steps = pl.num_programs(0)
    row_iota = lax.broadcasted_iota(jnp.int32, (REACH, LANES), 0)
    over = table_ref[at["over"] + step]

    def region(g):
        return table_ref[at["first"] + g], table_ref[at["first"] + g + 1]

    def start_of(g, span):
        return pl.multiple_of(table_ref[at["start"][g] + span], 16)

    def block_copies(index):
        into = pl.ds(pl.multiple_of(index * TILE, TILE), TILE)
        copies = [pltpu.make_async_copy(rows_hbm.at[into, :], rows.at[into, :], sems.at[0, index])]
        if with_gate:
            copies.append(pltpu.make_async_copy(gate_hbm.at[into, :], gates.at[into, :], sems.at[1, index]))
        return copies

    @pl.when(step == 0)
    def _():
        for g in range(groups):
            waited[g] = region(g)[0]
        longest = region(0)[1] - region(0)[0]
        for g in range(1, groups):
            longest = jnp.maximum(longest, region(g)[1] - region(g)[0])

        @pl.loop(0, longest)
        def _(index):
            for g in range(groups):
                begin, stop = region(g)

                @pl.when(begin + index < stop)
                def _(begin=begin):
                    for copy in block_copies(begin + index):
                        copy.start()

    for g in range(groups):
        stop = region(g)[1]
        need = jnp.minimum((start_of(g, (step + 1) * GROUP - 1) + REACH + over * REACH + TILE - 1) // TILE, stop)
        need = jnp.where(step == steps - 1, stop, need)

        @pl.loop(waited[g], need)
        def _(index):
            for copy in block_copies(index):
                copy.wait()

        waited[g] = jnp.maximum(waited[g], need)

    def window(q, second):
        span = step * GROUP + q
        hot, data, gdata = [], [], []
        for g in range(groups):
            begin = place = start_of(g, span)
            if second:
                first, stop = region(g)
                place = pl.multiple_of(jnp.where(first == stop, begin, jnp.minimum(begin + REACH, stop * TILE - REACH)), 16)
                begin = begin + REACH
            row = row_iota + place
            match = pos_ref[g, pl.ds(spans[0] + span, 1), :] == row
            if second:
                match = jnp.logical_and(match, row >= begin)
            hot.append(jnp.where(match, 1.0, 0.0).astype(jnp.bfloat16))
            data.append(rows[pl.ds(place, REACH), :])
            if with_gate:
                gdata.append(gates[pl.ds(place, REACH), :])
        hot = jnp.concatenate(hot, axis=0)
        dims = (((0,), (0,)), ((), ()))
        out = lax.dot_general(hot, jnp.concatenate(data, axis=0), dims, preferred_element_type=jnp.float32)
        if not with_gate:
            return out, None
        exact = jnp.concatenate(gdata, axis=0)
        high = exact.astype(jnp.bfloat16)
        low = (exact - high.astype(jnp.float32)).astype(jnp.bfloat16)
        pair = lax.dot_general(hot, jnp.concatenate([high, low], axis=1), dims, preferred_element_type=jnp.float32)
        return out, pair[:, :LANES] + pair[:, LANES:]

    def put(q, wide):
        out, gate = window(q, False)
        if wide:
            out2, gate2 = window(q, True)
            out = out + out2
            gate = gate + gate2 if with_gate else None
        into = pl.ds(q * LANES if isinstance(q, int) else pl.multiple_of(q * LANES, LANES), LANES)
        out_ref[into, :] = out.astype(out_ref.dtype)
        if with_gate:
            gout_ref[:, into] = jnp.transpose(gate, (1, 0))[:8, :]

    @pl.when(over == 0)
    def _():
        for q in range(GROUP):
            put(q, False)

    @pl.when(over != 0)
    def _():
        @pl.loop(0, GROUP)
        def _(q):
            put(q, True)


def combine(layout, chunk, table, pos, rows, gate_rows=None):
    rows_max, dim = rows.shape
    groups = pos.shape[0]
    spans = layout[chunk]["spans"]
    tokens = spans[1] * LANES
    with_gate = gate_rows is not None
    block = GROUP * LANES
    operands, in_specs = [pos, rows], [WHOLE, ANY]
    out_shape = [jax.ShapeDtypeStruct((tokens, dim), jnp.bfloat16)]
    out_specs = [pl.BlockSpec((block, dim), lambda t, *_: (t, 0))]
    scratch = [pltpu.VMEM((rows_max, dim), jnp.bfloat16)]
    if with_gate:
        operands.append(gate_rows)
        in_specs.append(ANY)
        out_shape.append(jax.ShapeDtypeStruct((8, tokens), jnp.float32))
        out_specs.append(pl.BlockSpec((8, block), lambda t, *_: (0, t)))
        scratch.append(pltpu.VMEM((rows_max, LANES), jnp.float32))
    scratch += [pltpu.SMEM((groups,), jnp.int32), pltpu.SemaphoreType.DMA((2, rows_max // TILE))]
    kernel = functools.partial(combine_kernel, layout[chunk], spans, groups, with_gate)
    return call(kernel, table, operands, in_specs, out_shape, out_specs, scratch, (9 * 10**9, 35 * 10**6), (tokens // block,))


class WeightStream:
    def __init__(self, at, table_ref, weights, scratch):
        self.at, self.table_ref, self.own, self.helped = at, table_ref, weights[:3], weights[3:]
        self.wide, self.down, self.sems = scratch
        self.experts, _, self.ffn = weights[0].shape

    def copies(self, sources, s):
        wg, wu, wd = sources
        return (
            pltpu.make_async_copy(wg, self.wide.at[s, :, pl.ds(0, self.ffn)], self.sems.at[s, 0]),
            pltpu.make_async_copy(wu, self.wide.at[s, :, pl.ds(self.ffn, self.ffn)], self.sems.at[s, 1]),
            pltpu.make_async_copy(wd, self.down.at[s], self.sems.at[s, 2]),
        )

    def start(self, group, s):
        @pl.when(jnp.logical_and(group >= 0, group < self.experts))
        def _():
            for copy in self.copies([w.at[group] for w in self.own], s):
                copy.start()

        @pl.when(group == self.experts)
        def _():
            for copy in self.copies([w.at[0] for w in self.helped], s):
                copy.start()

    def begin(self):
        self.start(self.table_ref[self.at["group"]], 0)

    def slot(self):
        tile = pl.program_id(0)
        s = table_slot = self.table_ref[self.at["slot"] + tile]

        @pl.when(self.table_ref[self.at["fresh"] + tile] != 0)
        def _():
            self.start(self.table_ref[self.at["next"] + tile], 1 - table_slot)
            for copy in self.copies([w.at[0] for w in self.own], table_slot):
                copy.wait()

        return s


def run_tiles(at, table_ref, tile_body, piped_in, piped_out):
    pltpu.emit_pipeline(
        tile_body, grid=(table_ref[at["count"]],),
        in_specs=[row_block(ref.shape[1]) for ref in piped_in],
        out_specs=[row_block(ref.shape[1]) for ref in piped_out],
    )(*piped_in, *piped_out)


def forward_kernel(at, place, table_ref, pos_ref, prob_ref, tok_hbm, *rest):
    stream = WeightStream(at, table_ref, rest[:6], rest[11:14])
    dispatch = Dispatch(at, place, table_ref, pos_ref, prob_ref, tok_hbm, rest[14:])
    wide, down, ffn = stream.wide, stream.down, stream.ffn
    dispatch.begin(stream)

    def tile_body(x_ref, gate_ref, ab_ref, h_ref, out_ref):
        dispatch.tile(x_ref, gate_ref)
        slot = stream.slot()

        def matmuls(height):
            used = slice(0, height)
            x = x_ref[used, :]
            for j in range(ffn // LANES):
                cols = slice(j * LANES, (j + 1) * LANES)
                ucols = slice(ffn + j * LANES, ffn + (j + 1) * LANES)
                both = jnp.dot(x, jnp.concatenate([wide[slot, :, cols], wide[slot, :, ucols]], axis=1), preferred_element_type=jnp.float32)
                a, b = both[:, :LANES], both[:, LANES:]
                ab_ref[used, cols] = a
                ab_ref[used, ucols] = b
                h_ref[used, cols] = (a * jax.nn.sigmoid(a) * b).astype(h_ref.dtype)
            out = jnp.dot(h_ref[used, :], down[slot], preferred_element_type=jnp.float32)
            gate = gate_ref[used, :]
            for j in range(out.shape[1] // LANES):
                cols = slice(j * LANES, (j + 1) * LANES)
                out_ref[used, cols] = (out[:, cols] * gate).astype(out_ref.dtype)

        half = table_ref[at["half"] + pl.program_id(0)] != 0

        @pl.when(jnp.logical_not(half))
        def _():
            matmuls(TILE)

        @pl.when(half)
        def _():
            matmuls(TILE // 2)
            for ref in (ab_ref, h_ref, out_ref):
                ref[TILE // 2:, :] = jnp.zeros((TILE // 2, ref.shape[1]), ref.dtype)

    run_tiles(at, table_ref, tile_body, (), rest[6:11])
    dispatch.end()


def backward_kernel(at, place, table_ref, pos_ref, tok_hbm, ab_hbm, h_hbm, gate_hbm, *rest):
    stream = WeightStream(at, table_ref, rest[:6], rest[10:13])
    m_ref = rest[13]
    dispatch = Dispatch(at, place, table_ref, pos_ref, None, tok_hbm, rest[14:])
    wide, down, ffn = stream.wide, stream.down, stream.ffn
    trans = (((1,), (1,)), ((), ()))
    dispatch.begin(stream)

    def tile_body(ab_ref, h_ref, gate_ref, d_ref, in_ref, mg_ref, dgate_ref):
        dispatch.tile(m_ref)
        slot = stream.slot()
        m = m_ref[...]
        gate = gate_ref[...]
        dgate = jnp.zeros(gate.shape, jnp.float32)
        for c in range(0, ffn, 2 * LANES):
            width = min(2 * LANES, ffn - c)
            raw = lax.dot_general(m, down[slot, c:c + width, :], trans, preferred_element_type=jnp.float32)
            for k in range(width // LANES):
                lo = c + k * LANES
                cols = slice(lo, lo + LANES)
                ucols = slice(ffn + lo, ffn + lo + LANES)
                g = raw[:, k * LANES:(k + 1) * LANES]
                a, b = ab_ref[:, cols], ab_ref[:, ucols]
                sig = jax.nn.sigmoid(a)
                hidden_grad = g * gate
                d_ref[:, cols] = (hidden_grad * b * sig * (1.0 + a * (1.0 - sig))).astype(d_ref.dtype)
                d_ref[:, ucols] = (hidden_grad * (a * sig)).astype(d_ref.dtype)
                dgate = dgate + g * h_ref[:, cols].astype(jnp.float32)
        in_ref[...] = lax.dot_general(d_ref[...], wide[slot], trans, preferred_element_type=jnp.float32).astype(in_ref.dtype)
        for j in range(m.shape[1] // LANES):
            cols = slice(j * LANES, (j + 1) * LANES)
            mg_ref[:, cols] = (m[:, cols].astype(jnp.float32) * gate).astype(mg_ref.dtype)
        lane = lax.broadcasted_iota(jnp.int32, gate.shape, 1)
        expert = table_ref[at["expert"] + table_ref[at["group"] + pl.program_id(0)]]
        dgate_ref[...] = jnp.where(lane == expert, jnp.sum(dgate, axis=1, keepdims=True), 0.0)

    run_tiles(at, table_ref, tile_body, (ab_hbm, h_hbm, gate_hbm), rest[6:10])
    dispatch.end()


def weight_scratch(wg):
    _, dim, ffn = wg.shape
    return [
        pltpu.VMEM((2, dim, 2 * ffn), wg.dtype),
        pltpu.VMEM((2, ffn, dim), wg.dtype),
        pltpu.SemaphoreType.DMA((2, 3)),
    ]


def shapes(rows_max, *kinds):
    return [jax.ShapeDtypeStruct((rows_max, width), dtype) for width, dtype in kinds]


def forward(layout, chunk, table, pos, prob, tokens, weights):
    _, dim, ffn = weights[0].shape
    kinds = ((dim, jnp.bfloat16), (LANES, jnp.float32), (2 * ffn, jnp.float32), (ffn, jnp.bfloat16), (dim, jnp.bfloat16))
    at = layout[chunk]
    tok, place = tokens
    return call(
        functools.partial(forward_kernel, at, place), table, (pos, prob, tok, *weights), [WHOLE, WHOLE] + [ANY] * 7,
        shapes(at["rows_max"], *kinds), [ANY] * 5, weight_scratch(weights[0]) + dispatch_scratch(at, tok), (75 * 10**9, 150 * 10**6),
    )


def backward(layout, chunk, table, pos, tok, ab, hidden, gates, weights):
    _, dim, ffn = weights[0].shape
    kinds = ((2 * ffn, jnp.bfloat16), (dim, jnp.bfloat16), (dim, jnp.bfloat16), (LANES, jnp.float32))
    at = layout[chunk]
    scratch = [*weight_scratch(weights[0]), pltpu.VMEM((TILE, dim), jnp.bfloat16), *dispatch_scratch(at, tok)]
    return call(
        functools.partial(backward_kernel, at, (0, at["part"])), table, (pos, tok, ab, hidden, gates, *weights), [WHOLE] + [ANY] * 10,
        shapes(at["rows_max"], *kinds), [ANY] * 4, scratch, (75 * 10**9, 150 * 10**6),
    )


def weight_grad_kernel(at, tiles_max, outs, carried, table_ref, *rest):
    lhs_hbm, rhs_hbm, back, rest = rest[:CHUNKS], rest[CHUNKS:2 * CHUNKS], rest[2 * CHUNKS:2 * CHUNKS + carried], rest[2 * CHUNKS + 2 * carried:]
    own_out, helped_out, rest = rest[:outs], rest[outs:2 * outs], rest[2 * outs:]
    filled, rest = rest[:carried], rest[carried:]
    lhs, rhs, lhs_t, acc, staged, pending, sems, out_sems = rest[:8]
    experts = at["experts"]
    steps = table_ref[at["steps"]]

    def copies(chunk, row, s, half):
        source = pl.ds(pl.multiple_of(row, TILE), TILE)
        into = pl.ds(half * TILE, TILE)
        return (
            pltpu.make_async_copy(lhs_hbm[chunk].at[source, :], lhs.at[s, into, :], sems.at[s, half, 0]),
            pltpu.make_async_copy(rhs_hbm[chunk].at[source, :], rhs.at[s, into, :], sems.at[s, half, 1]),
        )

    def start(index, s):
        for half in range(2):
            src = table_ref[at["src"] + 2 * index + half]
            for chunk in range(CHUNKS):
                @pl.when(jnp.logical_and(src >= chunk * tiles_max, src < (chunk + 1) * tiles_max))
                def _(chunk=chunk, src=src, half=half):
                    for copy in copies(chunk, (src - chunk * tiles_max) * TILE, s, half):
                        copy.start()

    def out_copies(targets):
        return [pltpu.make_async_copy(staged.at[i], target, out_sems.at[i]) for i, target in enumerate(targets)]

    def drain():
        @pl.when(pending[0] != 0)
        def _():
            for copy in out_copies([out.at[0] for out in own_out]):
                copy.wait()

        pending[0] = 0

    pending[0] = 0

    start(0, 0)

    place = table_ref[at["insert"]]
    if carried:
        *bounce, fetch_sems, store_sems = rest[8:]
        fetch = [pltpu.make_async_copy(back[i].at[0], bounce[i], fetch_sems.at[i]) for i in range(carried)]
        store = [pltpu.make_async_copy(bounce[i], filled[i].at[jnp.maximum(place, 0)], store_sems.at[i]) for i in range(carried)]

        @pl.when(place >= 0)
        def _():
            for copy in fetch:
                copy.start()

    def accumulate(slot, fresh, depth):
        lhs_t[:, :depth] = jnp.transpose(lhs[slot, :depth, :], (1, 0))
        block = 2 * LANES
        for c in range(0, acc.shape[1], block):
            part = jnp.dot(lhs_t[:, :depth], rhs[slot, :depth, c:c + block], preferred_element_type=jnp.float32)
            acc[:, c:c + block] = jnp.where(fresh, 0.0, acc[:, c:c + block]) + part

    @pl.loop(0, steps)
    def _(step):
        slot = lax.rem(step, 2)
        group = table_ref[at["owner"] + step]

        @pl.when(step + 1 < steps)
        def _():
            start(step + 1, 1 - slot)

        if carried:
            @pl.when(jnp.logical_and(place >= 0, step == steps // 2))
            def _():
                for one, other in zip(fetch, store):
                    one.wait()
                    other.start()

        fresh = jnp.logical_or(step == 0, group != table_ref[at["owner"] + jnp.maximum(step - 1, 0)])
        last = jnp.logical_or(step == steps - 1, group != table_ref[at["owner"] + step + 1])
        pair = table_ref[at["src"] + 2 * step + 1] >= 0
        for copy in copies(0, 0, slot, 0):
            copy.wait()

        @pl.when(pair)
        def _():
            for copy in copies(0, 0, slot, 1):
                copy.wait()
            accumulate(slot, fresh, 2 * TILE)

        @pl.when(jnp.logical_not(pair))
        def _():
            accumulate(slot, fresh, TILE)

        @pl.when(last)
        def _():
            drain()
            width = acc.shape[1] // outs
            for i in range(outs):
                staged[i, :, :] = acc[:, i * width:(i + 1) * width].astype(staged.dtype)

            @pl.when(group < experts)
            def _():
                for copy in out_copies([out.at[group] for out in own_out]):
                    copy.start()

            @pl.when(group == experts)
            def _():
                for copy in out_copies([out.at[0] for out in helped_out]):
                    copy.start()

            pending[0] = 1

    drain()
    if carried:
        @pl.when(place >= 0)
        def _():
            for copy in store:
                copy.wait()


def weight_grad(layout, table, lhs, rhs, experts, outs, back=(), grads=()):
    left, right = lhs[0].shape[1], rhs[0].shape[1]
    width = right // outs
    carried = len(back)
    scratch = [
        pltpu.VMEM((2, 2 * TILE, left), jnp.bfloat16),
        pltpu.VMEM((2, 2 * TILE, right), jnp.bfloat16),
        pltpu.VMEM((left, 2 * TILE), jnp.bfloat16),
        pltpu.VMEM((left, right), jnp.float32),
        pltpu.VMEM((outs, left, width), jnp.bfloat16),
        pltpu.SMEM((1,), jnp.int32),
        pltpu.SemaphoreType.DMA((2, 2, 2)),
        pltpu.SemaphoreType.DMA((outs,)),
    ]
    if carried:
        scratch += [pltpu.VMEM(b.shape[1:], b.dtype) for b in back]
        scratch += [pltpu.SemaphoreType.DMA((carried,)), pltpu.SemaphoreType.DMA((carried,))]
    out_shape = [jax.ShapeDtypeStruct((n, left, width), jnp.bfloat16) for n in [experts] * outs + [1] * outs]
    first = len(out_shape)
    out_shape += [jax.ShapeDtypeStruct(g.shape, g.dtype) for g in grads]
    operands = (*lhs, *rhs, *back, *grads)
    at = layout["grad"] | {"experts": experts}
    return pl.pallas_call(
        functools.partial(weight_grad_kernel, at, layout["tiles_max"], outs, carried),
        grid_spec=pltpu.PrefetchScalarGridSpec(
            num_scalar_prefetch=1, in_specs=[ANY] * len(operands), out_specs=[ANY] * len(out_shape), scratch_shapes=scratch
        ),
        out_shape=out_shape,
        input_output_aliases={1 + 2 * CHUNKS + carried + i: first + i for i in range(len(grads))},
        compiler_params=pltpu.CompilerParams(vmem_limit_bytes=VMEM_LIMIT),
        cost_estimate=pl.CostEstimate(flops=2 * 9000 * left * right, bytes_accessed=100 * 10**6, transcendentals=0),
        name="weight_grad",
    )(table, *operands)


def insert_kernel(at, size, table_ref, *rest):
    back, outs, staged, sems = rest[:size], rest[2 * size:3 * size], rest[3 * size:4 * size], rest[4 * size]
    place = table_ref[at]

    @pl.when(place >= 0)
    def _():
        fetch = [pltpu.make_async_copy(b.at[0], s, sems.at[0, i]) for i, (b, s) in enumerate(zip(back, staged))]
        store = [pltpu.make_async_copy(s, out.at[place], sems.at[1, i]) for i, (s, out) in enumerate(zip(staged, outs))]
        for copy in fetch:
            copy.start()
        for i in range(size):
            fetch[i].wait()
            store[i].start()
        for copy in store:
            copy.wait()


def insert(layout, table, back, grads):
    size = len(grads)
    return pl.pallas_call(
        functools.partial(insert_kernel, layout["insert"], size),
        grid_spec=pltpu.PrefetchScalarGridSpec(
            num_scalar_prefetch=1,
            in_specs=[ANY] * (2 * size),
            out_specs=[ANY] * size,
            scratch_shapes=[pltpu.VMEM(g.shape[1:], g.dtype) for g in grads] + [pltpu.SemaphoreType.DMA((2, size))],
        ),
        out_shape=[jax.ShapeDtypeStruct(g.shape, g.dtype) for g in grads],
        input_output_aliases={1 + size + i: i for i in range(size)},
        compiler_params=pltpu.CompilerParams(vmem_limit_bytes=VMEM_LIMIT),
        cost_estimate=pl.CostEstimate(flops=10**9, bytes_accessed=15 * 10**6 * size, transcendentals=0),
        name="insert",
    )(table, *back, *grads)


def row_blocks(height, dim):
    specs, first = [], 0
    for part in PARTS:
        blocks = part // height
        specs.append(pl.BlockSpec((height, dim), lambda t, *_, first=first, last=blocks - 1: (jnp.clip(t - first, 0, last), 0)))
        first += blocks
    return specs


def of_this_chunk(height, refs):
    step, first, value = pl.program_id(0), 0, None
    for part, ref in zip(PARTS, refs):
        value = ref[...] if value is None else jnp.where(step >= first, ref[...], value)
        first += part // height
    return value


def norm_kernel(x_ref, gain_ref, out_ref):
    x = x_ref[...].astype(jnp.float32)
    inv_rms = lax.rsqrt(jnp.mean(x * x, axis=-1, keepdims=True) + NORM_EPS)
    out_ref[...] = (x * inv_rms * gain_ref[...]).astype(out_ref.dtype)


def normalize(x, gain, first, count):
    dim = x.shape[1]
    height = LANES
    return pl.pallas_call(
        norm_kernel,
        grid=(count // height,),
        in_specs=[pl.BlockSpec((height, dim), lambda t: (t + first // height, 0)), pl.BlockSpec((1, dim), lambda t: (0, 0))],
        out_specs=pl.BlockSpec((height, dim), lambda t: (t, 0)),
        out_shape=jax.ShapeDtypeStruct((count, dim), jnp.bfloat16),
        cost_estimate=pl.CostEstimate(flops=10**7, bytes_accessed=4 * 10**6, transcendentals=0),
        name="normalize",
    )(x, gain.reshape(1, dim))


def finish_kernel(x_ref, y_grad_ref, prob_ref, gate_grad_ref, balance_ref, gain_ref, router_ref, *rest):
    in_refs, out_refs, (y_ref, x_grad_ref, stats_ref) = rest[:CHUNKS], rest[CHUNKS:2 * CHUNKS], rest[2 * CHUNKS:]
    height = x_ref.shape[0]
    prob = prob_ref[...]
    prob_grad = gate_grad_ref[...] + balance_ref[...]
    logit_grad = (prob * (prob_grad - jnp.sum(prob * prob_grad, axis=0, keepdims=True))).astype(jnp.bfloat16)
    x = x_ref[...].astype(jnp.float32)
    inv_rms = lax.rsqrt(jnp.mean(x * x, axis=-1, keepdims=True) + NORM_EPS)
    unit = x * inv_rms
    gain = gain_ref[...]
    moe_out = of_this_chunk(height, out_refs).astype(jnp.float32)
    y_ref[...] = (x + moe_out).astype(y_ref.dtype)
    routed = lax.dot_general(logit_grad, router_ref[...], (((0,), (0,)), ((), ())), preferred_element_type=jnp.float32)
    x_norm_grad = of_this_chunk(height, in_refs).astype(jnp.float32) + routed
    unit_grad = x_norm_grad * gain
    x_grad = y_grad_ref[...].astype(jnp.float32) + inv_rms * (unit_grad - unit * jnp.mean(unit_grad * unit, axis=-1, keepdims=True))
    x_grad_ref[...] = x_grad.astype(x_grad_ref.dtype)
    x_norm = (unit * gain).astype(jnp.bfloat16)

    @pl.when(pl.program_id(0) == 0)
    def _():
        stats_ref[...] = jnp.zeros_like(stats_ref)

    def folded(values):
        return jnp.sum(values.reshape(height // 8, 8, values.shape[1]), axis=0)

    stats_ref[0:8, :] += jnp.dot(logit_grad, x_norm, preferred_element_type=jnp.float32)
    stats_ref[8:16, :] += folded(x_norm_grad * unit)
    stats_ref[16:24, :] += folded(moe_out * moe_out)


def finish(x, y_grad, prob, gate_grad, balance, gain, router, in_raw, out_raw):
    tokens, dim = x.shape
    height = LANES
    rows = pl.BlockSpec((height, dim), lambda t: (t, 0))
    of_tokens = pl.BlockSpec((8, height), lambda t: (0, t))
    return pl.pallas_call(
        finish_kernel,
        grid=(tokens // height,),
        in_specs=[
            rows, rows, of_tokens, of_tokens, pl.BlockSpec((8, height), lambda t: (0, 0)), pl.BlockSpec((1, dim), lambda t: (0, 0)),
            pl.BlockSpec((8, dim), lambda t: (0, 0)), *row_blocks(height, dim), *row_blocks(height, dim),
        ],
        out_specs=[rows, rows, pl.BlockSpec((32, dim), lambda t: (0, 0))],
        out_shape=[
            jax.ShapeDtypeStruct((tokens, dim), jnp.bfloat16), jax.ShapeDtypeStruct((tokens, dim), jnp.bfloat16),
            jax.ShapeDtypeStruct((32, dim), jnp.float32),
        ],
        compiler_params=pltpu.CompilerParams(vmem_limit_bytes=VMEM_LIMIT),
        cost_estimate=pl.CostEstimate(flops=10**9, bytes_accessed=25 * 10**6, transcendentals=0),
        name="finish",
    )(x, y_grad, prob, gate_grad, balance, gain.reshape(1, dim), router, *in_raw, *out_raw)


def below(size, strict):
    i = lax.broadcasted_iota(jnp.int32, (size, size), 0)
    j = lax.broadcasted_iota(jnp.int32, (size, size), 1)
    return (i < j if strict else i <= j).astype(jnp.float32)


def running(values):
    size = values.shape[-1]
    i = lax.broadcasted_iota(jnp.int32, (size, size), 0)
    j = lax.broadcasted_iota(jnp.int32, (size, size), 1)
    return jnp.sum(jnp.where(i <= j, values[..., :, None], 0), axis=-2)


def count(condition, axis):
    return jnp.sum(condition.astype(jnp.int32), axis=axis)


def choose_swap(rows, experts):
    work = 4 * ((rows + TILE - 1) // TILE) + (rows + TILE // 2 - 1) // (TILE // 2)
    none = jnp.zeros((rows.shape[0], 1), jnp.int32)
    sides = [work[:, :experts], work[:, experts:]]
    options = [jnp.concatenate([none, side], axis=1) for side in sides]
    moved = options[1][:, None, :] - options[0][:, :, None]
    loads = [jnp.sum(side, axis=1)[:, None, None] for side in sides]
    cost = jnp.sum(jnp.maximum(loads[0] + moved, loads[1] - moved), axis=0)
    index = lax.broadcasted_iota(jnp.int32, cost.shape, 0) * (experts + 1) + lax.broadcasted_iota(jnp.int32, cost.shape, 1)
    best = jnp.min(jnp.where(cost == jnp.min(cost), index, cost.size))
    return best // (experts + 1) - 1, best % (experts + 1) - 1


def routing(hot, experts_of, place):
    groups, span_total, _ = hot.shape
    spans_of = [part * (span_total * LANES // sum(PARTS)) // LANES for part in PARTS]
    firsts = [sum(spans_of[:c]) for c in range(CHUNKS)]
    chunk_of = jnp.concatenate([jnp.full((n,), c, jnp.int32) for c, n in enumerate(spans_of)])
    member = chunk_of[:, None] == jnp.arange(CHUNKS, dtype=jnp.int32)[None, :]
    same = chunk_of[:, None] == chunk_of[None, :]
    tiles_of = [2 * n * LANES // TILE + groups for n in spans_of]
    tiles_max = max(tiles_of)

    within = jnp.einsum("gsi,ij->gsj", hot, below(LANES, False), preferred_element_type=jnp.float32)
    span_count = jnp.sum(hot, axis=-1)
    before = jnp.einsum("gi,ij->gj", span_count, jnp.where(same, below(span_total, True), 0.0), preferred_element_type=jnp.float32)
    total = jnp.sum(jnp.where(member[:, None, :], span_count.T[:, :, None], 0.0), axis=0).T.astype(jnp.int32)
    tiles = (total + TILE - 1) // TILE
    none = jnp.logical_and(jnp.sum(tiles, axis=1, keepdims=True) == 0, jnp.arange(groups, dtype=jnp.int32) == 0)
    tiles = jnp.where(none, 1, tiles)
    stop = running(tiles)
    begin = stop - tiles

    def to_spans(values):
        return jnp.sum(jnp.where(member[None], values.T[:, None, :], 0), axis=2)

    span_first = to_spans(begin) * TILE + before.astype(jnp.int32)
    span_stop = span_first + span_count.astype(jnp.int32)
    pos = jnp.where(hot > 0, span_first[:, :, None] + within.astype(jnp.int32) - 1, -1)

    index = jnp.arange(groups, dtype=jnp.int32)
    tile = jnp.arange(tiles_max, dtype=jnp.int32)
    group = jnp.minimum(count(tile[None, :, None] >= stop[:, None, :], 2), groups - 1)
    mine = group[:, :, None] == index
    ordinal = running((tiles > 0).astype(jnp.int32)) - 1
    later = jnp.logical_and(index[None, None, :] > group[:, :, None], tiles[:, None, :] > 0)
    follow = jnp.min(jnp.where(later, index, groups), axis=2)
    follow = jnp.where(follow == groups, -1, follow)
    fresh = jnp.sum(jnp.where(mine, begin[:, None, :], 0), axis=2) == tile
    slot = jnp.sum(jnp.where(mine, ordinal[:, None, :], 0), axis=2) % 2
    rows_left = jnp.sum(jnp.where(mine, (total + begin * TILE)[:, None, :], 0), axis=2) - tile * TILE
    half = rows_left <= TILE // 2

    half_mine = jnp.repeat(mine, 2, axis=1)
    stops = jnp.sum(jnp.where(half_mine[..., None], span_stop[None, None], 0), axis=2)
    row0 = jnp.arange(2 * tiles_max, dtype=jnp.int32)[None, :, None] * LANES
    inside = member.T[:, None, :]
    lo = count(jnp.logical_and(inside, stops <= row0), 2)
    hi = jnp.minimum(count(jnp.logical_and(inside, stops < row0 + LANES), 2), jnp.array(spans_of, jnp.int32)[:, None] - 1)
    width = jnp.maximum(jnp.max(((hi - lo + 2) // 2).reshape(CHUNKS, tiles_max, 2), axis=2), 1)
    for narrower, wider in zip((WINDOWS[-1], *WIDE_WINDOWS), (*WIDE_WINDOWS, WHOLE_CHUNK)):
        width = jnp.where(jnp.logical_and(width > narrower, width <= wider), wider, width)
    start = jnp.minimum(span_first // 16 * 16, to_spans(stop) * TILE - REACH)
    empty = to_spans(tiles) == 0
    leading = jnp.logical_and(jnp.logical_not(empty), to_spans(ordinal) == 0)
    start = jnp.where(empty, jnp.sum(jnp.where(leading, start, 0), axis=0), start)
    over = jnp.any(jnp.logical_and(jnp.logical_not(empty), span_stop - start > REACH), axis=0)
    over = jnp.any(over.reshape(-1, GROUP), axis=1)

    in_chunks = running(tiles.T)
    both = in_chunks[:, -1]
    step_stop = running((both + 1) // 2)
    step_first = step_stop - (both + 1) // 2
    steps = CHUNKS * tiles_max // 2 + groups
    step = jnp.arange(steps, dtype=jnp.int32)
    owner = jnp.minimum(count(step[:, None] >= step_stop[None, :], 1), groups - 1)
    step_mine = owner[:, None] == index

    def of_step(values):
        return jnp.sum(jnp.where(step_mine[:, :, None], values[None], 0), axis=1)[:, None, :]

    local = 2 * (step - of_step(step_first[:, None])[:, 0, 0])[:, None, None] + jnp.arange(2, dtype=jnp.int32)[None, :, None]
    ends, sizes = of_step(in_chunks), of_step(tiles.T)
    offset = local - (ends - sizes)
    found = jnp.logical_and(offset >= 0, local < ends)
    chunk_at = jnp.arange(CHUNKS, dtype=jnp.int32) * tiles_max
    src = jnp.sum(jnp.where(found, of_step(begin.T) + offset + chunk_at + 1, 0), axis=2) - 1

    sections = (
        ("expert", experts_of), ("insert", place.reshape(1)), ("steps", step_stop[-1:]), ("owner", owner), ("src", src),
        ("count", stop[:, -1:]), ("group", group), ("slot", slot), ("fresh", fresh), ("half", half), ("next", follow), ("lo", lo), ("width", width),
        ("first", jnp.concatenate([jnp.zeros((CHUNKS, 1), jnp.int32), stop], axis=1)), ("start", start), ("over", over),
    )
    table = jnp.concatenate([values.reshape(-1).astype(jnp.int32) for _, values in sections])
    places, sizes_of, at = {}, {}, 0
    for name, values in sections:
        places[name], sizes_of[name] = at, values.size
        at += values.size
    layout = {}
    for c in range(CHUNKS):
        layout[c] = {name: places[name] + c * (sizes_of[name] // CHUNKS) for name in ("count", "group", "slot", "fresh", "half", "next", "lo", "width", "first")}
        layout[c] |= {
            "expert": places["expert"], "spans": (firsts[c], spans_of[c]), "part": PARTS[c], "rows_max": tiles_of[c] * TILE,
            "start": [places["start"] + g * span_total + firsts[c] for g in range(groups)],
            "over": places["over"] + firsts[c] // GROUP,
        }
    layout |= {"grad": {name: places[name] for name in ("steps", "owner", "src", "insert")}, "insert": places["insert"], "tiles_max": tiles_max}
    return pos, table, layout


def solution(mesh):
    tp_size = mesh.shape["tp"]
    ep_size = mesh.shape["ep"]
    dev_count = tp_size * ep_size
    rows_axes = ("ep", "tp")
    row_spec = P(rows_axes, None)
    wide_spec = P("ep", None, "tp")
    down_spec = P("ep", "tp", None)
    swap = [(0, 1), (1, 0)]

    def body(x, y_grad, expert_ids, norm_gain, w_router, w_gate, w_up, w_down):
        tokens, model_dim = x.shape
        top_k = expert_ids.shape[1]
        num_experts = w_router.shape[1]
        local_experts = w_gate.shape[0]
        total_tokens = tokens * dev_count
        my_ep = lax.axis_index("ep").astype(jnp.int32)
        firsts = [sum(PARTS[:c]) for c in range(CHUNKS)]

        def of_chunk(rows, c, axis=0):
            return lax.slice_in_dim(rows, firsts[c], firsts[c] + PARTS[c], axis=axis)

        def gather(rows):
            return lax.all_gather(rows, rows_axes, axis=0, tiled=True)

        def scatter(rows):
            return lax.psum_scatter(rows, rows_axes, scatter_dimension=0, tiled=True)

        def of_chunk_span(values, c):
            return values[:, firsts[c] * dev_count:(firsts[c] + PARTS[c]) * dev_count]

        def after(values, first):
            return lax.optimization_barrier((values, first))

        gain = norm_gain.astype(jnp.float32)
        rest = tokens - PARTS[0]
        head, tail = normalize(x, gain, 0, PARTS[0]), normalize(x, gain, PARTS[0], rest)
        gathered = [gather(head), gather(tail)]
        tok = [(gathered[0], (0, PARTS[0]))] + [(gathered[1], (firsts[c] - PARTS[0], rest)) for c in range(1, CHUNKS)]

        x_norm = jnp.concatenate([head, tail], axis=0)
        route_prob = jax.nn.softmax(jnp.dot(x_norm, w_router, preferred_element_type=jnp.float32), axis=-1)
        expert_range = jnp.arange(num_experts, dtype=jnp.int32)
        choice = jnp.sum((expert_ids[:, :, None] == expert_range[None, None, :]).astype(jnp.float32), axis=1)
        small = lax.all_gather(jnp.concatenate([choice, route_prob], axis=1).T, rows_axes, axis=0, tiled=False)
        counts = jnp.sum(small[:, :num_experts], axis=(0, 2))
        balance_scale = BALANCE_COEF * num_experts / (total_tokens * total_tokens * top_k)
        balance_loss = balance_scale * jnp.sum(counts * jnp.sum(small[:, num_experts:], axis=(0, 2)))

        rows_in = jnp.stack([jnp.sum(of_chunk(small[:, :num_experts], c, 2), axis=(0, 2)) for c in range(CHUNKS)])
        gives = choose_swap(rows_in.astype(jnp.int32), local_experts)
        given = jnp.where(my_ep == 0, gives[0], gives[1])
        taken = jnp.where(my_ep == 0, gives[1], gives[0])
        my_base = my_ep * local_experts
        local = jnp.arange(local_experts, dtype=jnp.int32)
        group_experts = jnp.concatenate([my_base + local, (local_experts - my_base + jnp.maximum(taken, 0)).reshape(1)])
        active = jnp.concatenate([local != given, (taken >= 0).reshape(1)])
        take = jnp.logical_and(group_experts[:, None] == expert_range, active[:, None])
        spread = jnp.concatenate([of_chunk(small, c, 2).transpose(1, 0, 2).reshape(2 * num_experts, -1) for c in range(CHUNKS)], axis=1)
        spread = spread.reshape(2, 1, num_experts, -1, LANES)
        own = jnp.sum(jnp.where(take[None, :, :, None, None], spread, 0.0), axis=2)
        prob = own[1]
        pos, table, layout = routing(own[0], group_experts, given)
        helped = [lax.ppermute(lax.dynamic_slice_in_dim(w, jnp.maximum(given, 0), 1, axis=0), "ep", swap) for w in (w_gate, w_up, w_down)]
        weights = (w_gate, w_up, w_down, *helped)

        grad_scale = 2.0 * ACT_COEF / (total_tokens * model_dim)
        own_prob = route_prob.T
        balance_row = jnp.broadcast_to(balance_scale * counts[:, None], (num_experts, LANES))
        router = w_router.T
        first_tok, (own_prob, balance_row, router, balance_loss) = after(tok[0][0], (own_prob, balance_row, router, balance_loss))
        tok[0] = (first_tok, tok[0][1])
        x_rows, gate_rows, pre, hidden, d_rows, mg_rows = [], [], [], [], [], []
        out_raw, moe_out, m_own, m_tok, in_raw, gate_part = [], [], [], [], [], []

        def send_cotangent(c, gate):
            raw, (gate, _) = after(out_raw[c], (gate, m_own[-1:]))
            moe_out.append(raw)
            moe_grad = of_chunk(y_grad, c).astype(jnp.float32) + grad_scale * raw.astype(jnp.float32)
            m_own.append(moe_grad.astype(jnp.bfloat16))
            m_tok.append(gather(m_own[c]))
            return gate

        for c in range(CHUNKS):
            rows, gates, ab, h, out_rows = forward(layout, c, table, pos, prob, tok[c], weights)
            if c == 1:
                out_rows = send_cotangent(0, out_rows)
            (partial,) = combine(layout, c, table, pos, out_rows)
            if c == 0:
                partial, later = after(partial, gathered[1])
                tok[1:] = [(later, place) for _, place in tok[1:]]
            if c > 1:
                partial = send_cotangent(c - 1, partial)
            out_raw.append(scatter(partial))
            x_rows.append(rows)
            gate_rows.append(gates)
            pre.append(ab)
            hidden.append(h)
        for c in range(CHUNKS):
            d, in_rows, mg, dgate = backward(layout, c, table, pos, m_tok[c], pre[c], hidden[c], gate_rows[c], weights)
            if c == 0:
                in_rows = send_cotangent(CHUNKS - 1, in_rows)
            partial, gate_terms = combine(layout, c, table, pos, in_rows, dgate)
            if c == 0:
                m_tok[1], partial = after(m_tok[1], partial)
            in_raw.append(scatter(partial))
            gate_part.append(gate_terms)
            d_rows.append(d)
            mg_rows.append(mg)
        *wide_grads, helped_gate, helped_up = weight_grad(layout, table, x_rows, d_rows, local_experts, 2)
        back = []
        for grad in (helped_gate, helped_up):
            back.append(lax.ppermute(grad, "ep", swap))

        gate_sums = lax.psum(jnp.concatenate(gate_part, axis=1), ("tp", "ep"))
        device = my_ep * tp_size + lax.axis_index("tp")
        gate_sums = [
            lax.dynamic_slice_in_dim(of_chunk_span(gate_sums, c), device * PARTS[c], PARTS[c], axis=1) for c in range(CHUNKS)
        ]
        gate_weight_grad = jnp.concatenate(gate_sums, axis=1)
        gate_weight_grad, (wide_grads, in_raw) = after(gate_weight_grad, (wide_grads, in_raw))
        y, x_grad, stats = finish(x, y_grad, own_prob, gate_weight_grad, balance_row, gain, router, in_raw, moe_out)
        stats, (mg_rows[0], x_grad) = after(stats, (mg_rows[0], x_grad))
        down_grad, helped_down, gate_grad, up_grad = weight_grad(layout, table, hidden, mg_rows, local_experts, 1, back, wide_grads)
        (down_grad,) = insert(layout, table, [lax.ppermute(helped_down, "ep", swap)], [down_grad])
        stats = lax.psum(stats, ("tp", "ep"))
        router_sum = stats[:num_experts].T
        gain_sum = jnp.sum(stats[8:16], axis=0)
        act_loss = ACT_COEF * jnp.sum(stats[16:24]) / (total_tokens * model_dim)
        return (y, x_grad, gain_sum.astype(jnp.bfloat16), router_sum.astype(jnp.bfloat16), gate_grad, up_grad, down_grad, balance_loss, act_loss)

    return jax.shard_map(body, mesh=mesh, in_specs=(row_spec, row_spec, row_spec, P(), P(), wide_spec, wide_spec, down_spec), out_specs=(row_spec, row_spec, P(), P(), wide_spec, wide_spec, down_spec, P(), P()), check_vma=False)
```

```python
import functools

import jax
import jax.numpy as jnp
from jax import lax
from jax.experimental import pallas as pl
from jax.experimental.pallas import tpu as pltpu
from jax.sharding import PartitionSpec as P


NORM_EPS = 1e-6
ACT_COEF = 1e-5
BALANCE_COEF = 1e-3
TILE = 256
LANES = 128
GROUP = 4
REACH = 96
PARTS = (384, 256, 384)
CHUNKS = len(PARTS)
WINDOWS = (1, 2, 3, 4)
WIDE_WINDOWS = (6, 8)
WHOLE_CHUNK = 99
UNITS = 4
VMEM_LIMIT = 67_043_328


def call(kernel, table, operands, in_specs, out_shape, out_specs, scratch, cost, grid=()):
    return pl.pallas_call(
        kernel,
        grid_spec=pltpu.PrefetchScalarGridSpec(
            num_scalar_prefetch=1, grid=grid, in_specs=in_specs, out_specs=out_specs, scratch_shapes=scratch
        ),
        out_shape=out_shape,
        compiler_params=pltpu.CompilerParams(vmem_limit_bytes=VMEM_LIMIT),
        cost_estimate=pl.CostEstimate(flops=cost[0], bytes_accessed=cost[1], transcendentals=0),
    )(table, *operands)


ANY = pl.BlockSpec(memory_space=pl.ANY)
WHOLE = pl.BlockSpec(memory_space=pltpu.VMEM)


def row_block(width):
    return pl.BlockSpec((TILE, width), lambda t: (t, 0))


class Dispatch:
    def __init__(self, at, place, table_ref, pos_ref, prob_ref, tok_hbm, scratch):
        self.at, self.table_ref, self.pos_ref, self.prob_ref, self.tok_hbm = at, table_ref, pos_ref, prob_ref, tok_hbm
        self.tok, self.waited, self.sems = scratch
        self.first, self.spans = at["spans"]
        self.offset, self.stride = place
        self.part = at["part"]

    def span_copy(self, index, row):
        into = pl.ds(index * LANES if isinstance(index, int) else pl.multiple_of(index * LANES, LANES), LANES)
        return pltpu.make_async_copy(self.tok_hbm.at[pl.ds(row, LANES), :], self.tok.at[into, :], self.sems.at[index])

    def begin(self, stream):
        self.waited[0] = 0
        for index in range(self.spans):
            if index == 2 * WINDOWS[-1]:
                stream.begin()
            device, token = divmod(index * LANES, self.part)
            self.span_copy(index, device * self.stride + self.offset + token).start()

    def await_tokens(self, stop_span):
        @pl.loop(self.waited[0], stop_span)
        def _(index):
            self.span_copy(index, 0).wait()

        self.waited[0] = jnp.maximum(self.waited[0], stop_span)

    def end(self):
        self.await_tokens(self.spans)

    def tile(self, x_ref, gate_ref=None):
        tile = pl.program_id(0)
        group = self.table_ref[self.at["group"] + tile]
        width = self.table_ref[self.at["width"] + tile]

        def window(half, count, start):
            row_id = lax.broadcasted_iota(jnp.int32, (LANES, LANES), 0) + (tile * TILE + half * LANES)
            into = pl.ds(half * LANES if isinstance(half, int) else pl.multiple_of(half * LANES, LANES), LANES)
            hot, gate = [], jnp.zeros((LANES, LANES), jnp.float32)
            for q in range(count):
                span = pl.ds(self.first + start + q, 1)
                match = self.pos_ref[group, span, :] == row_id
                hot.append(jnp.where(match, 1.0, 0.0).astype(jnp.bfloat16))
                if gate_ref is not None:
                    gate = gate + jnp.where(match, self.prob_ref[group, span, :], 0.0)
            rows = self.tok[pl.ds(pl.multiple_of(start * LANES, LANES), count * LANES), :]
            out = jnp.dot(jnp.concatenate(hot, axis=1), rows, preferred_element_type=jnp.float32)
            x_ref[into, :] = out.astype(x_ref.dtype)
            if gate_ref is not None:
                gate_ref[into, :] = jnp.broadcast_to(jnp.sum(gate, axis=1, keepdims=True), (LANES, LANES))

        halves = 2 - self.table_ref[self.at["half"] + tile]

        def start_of(half, count):
            return jnp.minimum(self.table_ref[self.at["lo"] + 2 * tile + half], self.spans - count)

        def one_by_one(count):
            self.await_tokens(jnp.maximum(start_of(0, count), start_of(1, count)) + count)

            @pl.loop(0, halves)
            def _(half):
                window(half, count, start_of(half, count))

            @pl.when(halves == 1)
            def _():
                for ref in (x_ref,) if gate_ref is None else (x_ref, gate_ref):
                    ref[LANES:, :] = jnp.zeros((TILE - LANES, ref.shape[1]), ref.dtype)

        @pl.when(width == WHOLE_CHUNK)
        def _():
            one_by_one(self.spans)

        for k in WIDE_WINDOWS:
            @pl.when(width == k)
            def _(k=k):
                one_by_one(2 * k)

        for k in WINDOWS:
            @pl.when(width == k)
            def _(k=k):
                starts = [start_of(half, 2 * k) for half in range(2)]
                self.await_tokens(jnp.maximum(starts[0], starts[1]) + 2 * k)
                for half in range(2):
                    window(half, 2 * k, starts[half])


def dispatch_scratch(at, tok):
    spans = at["spans"][1]
    return [pltpu.VMEM((spans * LANES, tok.shape[1]), tok.dtype), pltpu.SMEM((1,), jnp.int32), pltpu.SemaphoreType.DMA((spans,))]


def combine_kernel(at, spans, groups, with_gate, table_ref, pos_ref, rows_hbm, *rest):
    if with_gate:
        gate_hbm, out_ref, gout_ref, rows, gates, waited, sems = rest
    else:
        out_ref, rows, waited, sems = rest
    step = pl.program_id(0)
    steps = pl.num_programs(0)
    row_iota = lax.broadcasted_iota(jnp.int32, (REACH, LANES), 0)
    over = table_ref[at["over"] + step]

    def region(g):
        return table_ref[at["first"] + g], table_ref[at["first"] + g + 1]

    def start_of(g, span):
        return pl.multiple_of(table_ref[at["start"][g] + span], 16)

    def block_copies(index):
        into = pl.ds(pl.multiple_of(index * TILE, TILE), TILE)
        copies = [pltpu.make_async_copy(rows_hbm.at[into, :], rows.at[into, :], sems.at[0, index])]
        if with_gate:
            copies.append(pltpu.make_async_copy(gate_hbm.at[into, :], gates.at[into, :], sems.at[1, index]))
        return copies

    @pl.when(step == 0)
    def _():
        for g in range(groups):
            waited[g] = region(g)[0]
        longest = region(0)[1] - region(0)[0]
        for g in range(1, groups):
            longest = jnp.maximum(longest, region(g)[1] - region(g)[0])

        @pl.loop(0, longest)
        def _(index):
            for g in range(groups):
                begin, stop = region(g)

                @pl.when(begin + index < stop)
                def _(begin=begin):
                    for copy in block_copies(begin + index):
                        copy.start()

    for g in range(groups):
        stop = region(g)[1]
        need = jnp.minimum((start_of(g, (step + 1) * GROUP - 1) + REACH + over * REACH + TILE - 1) // TILE, stop)
        need = jnp.where(step == steps - 1, stop, need)

        @pl.loop(waited[g], need)
        def _(index):
            for copy in block_copies(index):
                copy.wait()

        waited[g] = jnp.maximum(waited[g], need)

    def window(q, second):
        span = step * GROUP + q
        hot, data, gdata = [], [], []
        for g in range(groups):
            begin = place = start_of(g, span)
            if second:
                first, stop = region(g)
                place = pl.multiple_of(jnp.where(first == stop, begin, jnp.minimum(begin + REACH, stop * TILE - REACH)), 16)
                begin = begin + REACH
            row = row_iota + place
            match = pos_ref[g, pl.ds(spans[0] + span, 1), :] == row
            if second:
                match = jnp.logical_and(match, row >= begin)
            hot.append(jnp.where(match, 1.0, 0.0).astype(jnp.bfloat16))
            data.append(rows[pl.ds(place, REACH), :])
            if with_gate:
                gdata.append(gates[pl.ds(place, REACH), :])
        hot = jnp.concatenate(hot, axis=0)
        dims = (((0,), (0,)), ((), ()))
        out = lax.dot_general(hot, jnp.concatenate(data, axis=0), dims, preferred_element_type=jnp.float32)
        if not with_gate:
            return out, None
        exact = jnp.concatenate(gdata, axis=0)
        high = exact.astype(jnp.bfloat16)
        low = (exact - high.astype(jnp.float32)).astype(jnp.bfloat16)
        pair = lax.dot_general(hot, jnp.concatenate([high, low], axis=1), dims, preferred_element_type=jnp.float32)
        return out, pair[:, :LANES] + pair[:, LANES:]

    def put(q, wide):
        out, gate = window(q, False)
        if wide:
            out2, gate2 = window(q, True)
            out = out + out2
            gate = gate + gate2 if with_gate else None
        into = pl.ds(q * LANES if isinstance(q, int) else pl.multiple_of(q * LANES, LANES), LANES)
        out_ref[into, :] = out.astype(out_ref.dtype)
        if with_gate:
            gout_ref[:, into] = jnp.transpose(gate, (1, 0))[:8, :]

    @pl.when(over == 0)
    def _():
        for q in range(GROUP):
            put(q, False)

    @pl.when(over != 0)
    def _():
        @pl.loop(0, GROUP)
        def _(q):
            put(q, True)


def combine(layout, chunk, table, pos, rows, gate_rows=None):
    rows_max, dim = rows.shape
    groups = pos.shape[0]
    spans = layout[chunk]["spans"]
    tokens = spans[1] * LANES
    with_gate = gate_rows is not None
    block = GROUP * LANES
    operands, in_specs = [pos, rows], [WHOLE, ANY]
    out_shape = [jax.ShapeDtypeStruct((tokens, dim), jnp.bfloat16)]
    out_specs = [pl.BlockSpec((block, dim), lambda t, *_: (t, 0))]
    scratch = [pltpu.VMEM((rows_max, dim), jnp.bfloat16)]
    if with_gate:
        operands.append(gate_rows)
        in_specs.append(ANY)
        out_shape.append(jax.ShapeDtypeStruct((8, tokens), jnp.float32))
        out_specs.append(pl.BlockSpec((8, block), lambda t, *_: (0, t)))
        scratch.append(pltpu.VMEM((rows_max, LANES), jnp.float32))
    scratch += [pltpu.SMEM((groups,), jnp.int32), pltpu.SemaphoreType.DMA((2, rows_max // TILE))]
    kernel = functools.partial(combine_kernel, layout[chunk], spans, groups, with_gate)
    return call(kernel, table, operands, in_specs, out_shape, out_specs, scratch, (9 * 10**9, 35 * 10**6), (tokens // block,))


class WeightStream:
    def __init__(self, at, table_ref, weights, scratch):
        self.at, self.table_ref, self.own, self.helped = at, table_ref, weights[:3], weights[3:]
        self.wide, self.down, self.sems = scratch
        self.experts, _, self.ffn = weights[0].shape

    def copies(self, sources, s):
        wg, wu, wd = sources
        return (
            pltpu.make_async_copy(wg, self.wide.at[s, :, pl.ds(0, self.ffn)], self.sems.at[s, 0]),
            pltpu.make_async_copy(wu, self.wide.at[s, :, pl.ds(self.ffn, self.ffn)], self.sems.at[s, 1]),
            pltpu.make_async_copy(wd, self.down.at[s], self.sems.at[s, 2]),
        )

    def start(self, group, s):
        @pl.when(jnp.logical_and(group >= 0, group < self.experts))
        def _():
            for copy in self.copies([w.at[group] for w in self.own], s):
                copy.start()

        @pl.when(group == self.experts)
        def _():
            for copy in self.copies([w.at[0] for w in self.helped], s):
                copy.start()

    def begin(self):
        self.start(self.table_ref[self.at["group"]], 0)

    def slot(self):
        tile = pl.program_id(0)
        s = table_slot = self.table_ref[self.at["slot"] + tile]

        @pl.when(self.table_ref[self.at["fresh"] + tile] != 0)
        def _():
            self.start(self.table_ref[self.at["next"] + tile], 1 - table_slot)
            for copy in self.copies([w.at[0] for w in self.own], table_slot):
                copy.wait()

        return s


def run_tiles(at, table_ref, tile_body, piped_in, piped_out):
    pltpu.emit_pipeline(
        tile_body, grid=(table_ref[at["count"]],),
        in_specs=[row_block(ref.shape[1]) for ref in piped_in],
        out_specs=[row_block(ref.shape[1]) for ref in piped_out],
    )(*piped_in, *piped_out)


def forward_kernel(at, place, table_ref, pos_ref, prob_ref, tok_hbm, *rest):
    stream = WeightStream(at, table_ref, rest[:6], rest[11:14])
    dispatch = Dispatch(at, place, table_ref, pos_ref, prob_ref, tok_hbm, rest[14:])
    wide, down, ffn = stream.wide, stream.down, stream.ffn
    dispatch.begin(stream)

    def tile_body(x_ref, gate_ref, ab_ref, h_ref, out_ref):
        dispatch.tile(x_ref, gate_ref)
        slot = stream.slot()

        def matmuls(height):
            used = slice(0, height)
            x = x_ref[used, :]
            for j in range(ffn // LANES):
                cols = slice(j * LANES, (j + 1) * LANES)
                ucols = slice(ffn + j * LANES, ffn + (j + 1) * LANES)
                both = jnp.dot(x, jnp.concatenate([wide[slot, :, cols], wide[slot, :, ucols]], axis=1), preferred_element_type=jnp.float32)
                a, b = both[:, :LANES], both[:, LANES:]
                ab_ref[used, cols] = a
                ab_ref[used, ucols] = b
                h_ref[used, cols] = (a * jax.nn.sigmoid(a) * b).astype(h_ref.dtype)
            out = jnp.dot(h_ref[used, :], down[slot], preferred_element_type=jnp.float32)
            gate = gate_ref[used, :]
            for j in range(out.shape[1] // LANES):
                cols = slice(j * LANES, (j + 1) * LANES)
                out_ref[used, cols] = (out[:, cols] * gate).astype(out_ref.dtype)

        half = table_ref[at["half"] + pl.program_id(0)] != 0

        @pl.when(jnp.logical_not(half))
        def _():
            matmuls(TILE)

        @pl.when(half)
        def _():
            matmuls(TILE // 2)
            for ref in (ab_ref, h_ref, out_ref):
                ref[TILE // 2:, :] = jnp.zeros((TILE // 2, ref.shape[1]), ref.dtype)

    run_tiles(at, table_ref, tile_body, (), rest[6:11])
    dispatch.end()


def backward_kernel(at, place, table_ref, pos_ref, tok_hbm, ab_hbm, h_hbm, gate_hbm, *rest):
    stream = WeightStream(at, table_ref, rest[:6], rest[10:13])
    m_ref = rest[13]
    dispatch = Dispatch(at, place, table_ref, pos_ref, None, tok_hbm, rest[14:])
    wide, down, ffn = stream.wide, stream.down, stream.ffn
    trans = (((1,), (1,)), ((), ()))
    dispatch.begin(stream)

    def tile_body(ab_ref, h_ref, gate_ref, d_ref, in_ref, mg_ref, dgate_ref):
        dispatch.tile(m_ref)
        slot = stream.slot()
        m = m_ref[...]
        gate = gate_ref[...]
        dgate = jnp.zeros(gate.shape, jnp.float32)
        for c in range(0, ffn, 2 * LANES):
            width = min(2 * LANES, ffn - c)
            raw = lax.dot_general(m, down[slot, c:c + width, :], trans, preferred_element_type=jnp.float32)
            for k in range(width // LANES):
                lo = c + k * LANES
                cols = slice(lo, lo + LANES)
                ucols = slice(ffn + lo, ffn + lo + LANES)
                g = raw[:, k * LANES:(k + 1) * LANES]
                a, b = ab_ref[:, cols], ab_ref[:, ucols]
                sig = jax.nn.sigmoid(a)
                hidden_grad = g * gate
                d_ref[:, cols] = (hidden_grad * b * sig * (1.0 + a * (1.0 - sig))).astype(d_ref.dtype)
                d_ref[:, ucols] = (hidden_grad * (a * sig)).astype(d_ref.dtype)
                dgate = dgate + g * h_ref[:, cols].astype(jnp.float32)
        in_ref[...] = lax.dot_general(d_ref[...], wide[slot], trans, preferred_element_type=jnp.float32).astype(in_ref.dtype)
        for j in range(m.shape[1] // LANES):
            cols = slice(j * LANES, (j + 1) * LANES)
            mg_ref[:, cols] = (m[:, cols].astype(jnp.float32) * gate).astype(mg_ref.dtype)
        lane = lax.broadcasted_iota(jnp.int32, gate.shape, 1)
        expert = table_ref[at["expert"] + table_ref[at["group"] + pl.program_id(0)]]
        dgate_ref[...] = jnp.where(lane == expert, jnp.sum(dgate, axis=1, keepdims=True), 0.0)

    run_tiles(at, table_ref, tile_body, (ab_hbm, h_hbm, gate_hbm), rest[6:10])
    dispatch.end()


def weight_scratch(wg):
    _, dim, ffn = wg.shape
    return [
        pltpu.VMEM((2, dim, 2 * ffn), wg.dtype),
        pltpu.VMEM((2, ffn, dim), wg.dtype),
        pltpu.SemaphoreType.DMA((2, 3)),
    ]


def shapes(rows_max, *kinds):
    return [jax.ShapeDtypeStruct((rows_max, width), dtype) for width, dtype in kinds]


def forward(layout, chunk, table, pos, prob, tokens, weights):
    _, dim, ffn = weights[0].shape
    kinds = ((dim, jnp.bfloat16), (LANES, jnp.float32), (2 * ffn, jnp.float32), (ffn, jnp.bfloat16), (dim, jnp.bfloat16))
    at = layout[chunk]
    tok, place = tokens
    return call(
        functools.partial(forward_kernel, at, place), table, (pos, prob, tok, *weights), [WHOLE, WHOLE] + [ANY] * 7,
        shapes(at["rows_max"], *kinds), [ANY] * 5, weight_scratch(weights[0]) + dispatch_scratch(at, tok), (75 * 10**9, 150 * 10**6),
    )


def backward(layout, chunk, table, pos, tok, ab, hidden, gates, weights):
    _, dim, ffn = weights[0].shape
    kinds = ((2 * ffn, jnp.bfloat16), (dim, jnp.bfloat16), (dim, jnp.bfloat16), (LANES, jnp.float32))
    at = layout[chunk]
    scratch = [*weight_scratch(weights[0]), pltpu.VMEM((TILE, dim), jnp.bfloat16), *dispatch_scratch(at, tok)]
    return call(
        functools.partial(backward_kernel, at, (0, at["part"])), table, (pos, tok, ab, hidden, gates, *weights), [WHOLE] + [ANY] * 10,
        shapes(at["rows_max"], *kinds), [ANY] * 4, scratch, (75 * 10**9, 150 * 10**6),
    )


def weight_grad_kernel(at, tiles_max, outs, carried, table_ref, *rest):
    lhs_hbm, rhs_hbm, back, rest = rest[:CHUNKS], rest[CHUNKS:2 * CHUNKS], rest[2 * CHUNKS:2 * CHUNKS + carried], rest[2 * CHUNKS + 2 * carried:]
    own_out, helped_out, rest = rest[:outs], rest[outs:2 * outs], rest[2 * outs:]
    filled, rest = rest[:carried], rest[carried:]
    lhs, rhs, lhs_t, acc, staged, pending, sems, out_sems = rest[:8]
    experts = at["experts"]
    steps = table_ref[at["steps"]]

    def copies(chunk, row, s, half):
        source = pl.ds(pl.multiple_of(row, LANES), LANES)
        into = pl.ds(half * LANES, LANES)
        return (
            pltpu.make_async_copy(lhs_hbm[chunk].at[source, :], lhs.at[s, into, :], sems.at[s, half, 0]),
            pltpu.make_async_copy(rhs_hbm[chunk].at[source, :], rhs.at[s, into, :], sems.at[s, half, 1]),
        )

    def start(index, s):
        for unit in range(UNITS):
            src = table_ref[at["src"] + UNITS * index + unit]
            for chunk in range(CHUNKS):
                first = 2 * chunk * tiles_max

                @pl.when(jnp.logical_and(src >= first, src < first + 2 * tiles_max))
                def _(first=first, chunk=chunk, src=src, unit=unit):
                    for copy in copies(chunk, (src - first) * LANES, s, unit):
                        copy.start()

    def out_copies(targets):
        return [pltpu.make_async_copy(staged.at[i], target, out_sems.at[i]) for i, target in enumerate(targets)]

    def drain():
        @pl.when(pending[0] != 0)
        def _():
            for copy in out_copies([out.at[0] for out in own_out]):
                copy.wait()

        pending[0] = 0

    pending[0] = 0

    start(0, 0)

    place = table_ref[at["insert"]]
    if carried:
        *bounce, fetch_sems, store_sems = rest[8:]
        fetch = [pltpu.make_async_copy(back[i].at[0], bounce[i], fetch_sems.at[i]) for i in range(carried)]
        store = [pltpu.make_async_copy(bounce[i], filled[i].at[jnp.maximum(place, 0)], store_sems.at[i]) for i in range(carried)]

        @pl.when(place >= 0)
        def _():
            for copy in fetch:
                copy.start()

    def accumulate(slot, fresh, depth):
        lhs_t[:, :depth] = jnp.transpose(lhs[slot, :depth, :], (1, 0))
        block = 2 * LANES
        for c in range(0, acc.shape[1], block):
            part = jnp.dot(lhs_t[:, :depth], rhs[slot, :depth, c:c + block], preferred_element_type=jnp.float32)
            acc[:, c:c + block] = jnp.where(fresh, 0.0, acc[:, c:c + block]) + part

    @pl.loop(0, steps)
    def _(step):
        slot = lax.rem(step, 2)
        group = table_ref[at["owner"] + step]

        @pl.when(step + 1 < steps)
        def _():
            start(step + 1, 1 - slot)

        if carried:
            @pl.when(jnp.logical_and(place >= 0, step == steps // 2))
            def _():
                for one, other in zip(fetch, store):
                    one.wait()
                    other.start()

        fresh = jnp.logical_or(step == 0, group != table_ref[at["owner"] + jnp.maximum(step - 1, 0)])
        last = jnp.logical_or(step == steps - 1, group != table_ref[at["owner"] + step + 1])
        there = [table_ref[at["src"] + UNITS * step + unit] >= 0 for unit in range(UNITS)]
        for unit in range(UNITS):
            @pl.when(there[unit])
            def _(unit=unit):
                for copy in copies(0, 0, slot, unit):
                    copy.wait()

        for unit in range(1, UNITS, 2):
            @pl.when(jnp.logical_and(there[unit - 1], jnp.logical_not(there[unit])))
            def _(unit=unit):
                for ref in (lhs, rhs):
                    ref[slot, unit * LANES:(unit + 1) * LANES, :] = jnp.zeros((LANES, ref.shape[2]), ref.dtype)

        @pl.when(there[2])
        def _():
            accumulate(slot, fresh, 2 * TILE)

        @pl.when(jnp.logical_not(there[2]))
        def _():
            accumulate(slot, fresh, TILE)

        @pl.when(last)
        def _():
            drain()
            width = acc.shape[1] // outs
            for i in range(outs):
                staged[i, :, :] = acc[:, i * width:(i + 1) * width].astype(staged.dtype)

            @pl.when(group < experts)
            def _():
                for copy in out_copies([out.at[group] for out in own_out]):
                    copy.start()

            @pl.when(group == experts)
            def _():
                for copy in out_copies([out.at[0] for out in helped_out]):
                    copy.start()

            pending[0] = 1

    drain()
    if carried:
        @pl.when(place >= 0)
        def _():
            for copy in store:
                copy.wait()


def weight_grad(layout, table, lhs, rhs, experts, outs, back=(), grads=()):
    left, right = lhs[0].shape[1], rhs[0].shape[1]
    width = right // outs
    carried = len(back)
    scratch = [
        pltpu.VMEM((2, 2 * TILE, left), jnp.bfloat16),
        pltpu.VMEM((2, 2 * TILE, right), jnp.bfloat16),
        pltpu.VMEM((left, 2 * TILE), jnp.bfloat16),
        pltpu.VMEM((left, right), jnp.float32),
        pltpu.VMEM((outs, left, width), jnp.bfloat16),
        pltpu.SMEM((1,), jnp.int32),
        pltpu.SemaphoreType.DMA((2, UNITS, 2)),
        pltpu.SemaphoreType.DMA((outs,)),
    ]
    if carried:
        scratch += [pltpu.VMEM(b.shape[1:], b.dtype) for b in back]
        scratch += [pltpu.SemaphoreType.DMA((carried,)), pltpu.SemaphoreType.DMA((carried,))]
    out_shape = [jax.ShapeDtypeStruct((n, left, width), jnp.bfloat16) for n in [experts] * outs + [1] * outs]
    first = len(out_shape)
    out_shape += [jax.ShapeDtypeStruct(g.shape, g.dtype) for g in grads]
    operands = (*lhs, *rhs, *back, *grads)
    at = layout["grad"] | {"experts": experts}
    return pl.pallas_call(
        functools.partial(weight_grad_kernel, at, layout["tiles_max"], outs, carried),
        grid_spec=pltpu.PrefetchScalarGridSpec(
            num_scalar_prefetch=1, in_specs=[ANY] * len(operands), out_specs=[ANY] * len(out_shape), scratch_shapes=scratch
        ),
        out_shape=out_shape,
        input_output_aliases={1 + 2 * CHUNKS + carried + i: first + i for i in range(len(grads))},
        compiler_params=pltpu.CompilerParams(vmem_limit_bytes=VMEM_LIMIT),
        cost_estimate=pl.CostEstimate(flops=2 * 9000 * left * right, bytes_accessed=100 * 10**6, transcendentals=0),
        name="weight_grad",
    )(table, *operands)


def insert_kernel(at, size, table_ref, *rest):
    back, outs, staged, sems = rest[:size], rest[2 * size:3 * size], rest[3 * size:4 * size], rest[4 * size]
    place = table_ref[at]

    @pl.when(place >= 0)
    def _():
        fetch = [pltpu.make_async_copy(b.at[0], s, sems.at[0, i]) for i, (b, s) in enumerate(zip(back, staged))]
        store = [pltpu.make_async_copy(s, out.at[place], sems.at[1, i]) for i, (s, out) in enumerate(zip(staged, outs))]
        for copy in fetch:
            copy.start()
        for i in range(size):
            fetch[i].wait()
            store[i].start()
        for copy in store:
            copy.wait()


def insert(layout, table, back, grads):
    size = len(grads)
    return pl.pallas_call(
        functools.partial(insert_kernel, layout["insert"], size),
        grid_spec=pltpu.PrefetchScalarGridSpec(
            num_scalar_prefetch=1,
            in_specs=[ANY] * (2 * size),
            out_specs=[ANY] * size,
            scratch_shapes=[pltpu.VMEM(g.shape[1:], g.dtype) for g in grads] + [pltpu.SemaphoreType.DMA((2, size))],
        ),
        out_shape=[jax.ShapeDtypeStruct(g.shape, g.dtype) for g in grads],
        input_output_aliases={1 + size + i: i for i in range(size)},
        compiler_params=pltpu.CompilerParams(vmem_limit_bytes=VMEM_LIMIT),
        cost_estimate=pl.CostEstimate(flops=10**9, bytes_accessed=15 * 10**6 * size, transcendentals=0),
        name="insert",
    )(table, *back, *grads)


def row_blocks(height, dim):
    specs, first = [], 0
    for part in PARTS:
        blocks = part // height
        specs.append(pl.BlockSpec((height, dim), lambda t, *_, first=first, last=blocks - 1: (jnp.clip(t - first, 0, last), 0)))
        first += blocks
    return specs


def of_this_chunk(height, refs):
    step, first, value = pl.program_id(0), 0, None
    for part, ref in zip(PARTS, refs):
        value = ref[...] if value is None else jnp.where(step >= first, ref[...], value)
        first += part // height
    return value


def norm_kernel(x_ref, gain_ref, out_ref):
    x = x_ref[...].astype(jnp.float32)
    inv_rms = lax.rsqrt(jnp.mean(x * x, axis=-1, keepdims=True) + NORM_EPS)
    out_ref[...] = (x * inv_rms * gain_ref[...]).astype(out_ref.dtype)


def normalize(x, gain, first, count):
    dim = x.shape[1]
    height = LANES
    return pl.pallas_call(
        norm_kernel,
        grid=(count // height,),
        in_specs=[pl.BlockSpec((height, dim), lambda t: (t + first // height, 0)), pl.BlockSpec((1, dim), lambda t: (0, 0))],
        out_specs=pl.BlockSpec((height, dim), lambda t: (t, 0)),
        out_shape=jax.ShapeDtypeStruct((count, dim), jnp.bfloat16),
        cost_estimate=pl.CostEstimate(flops=10**7, bytes_accessed=4 * 10**6, transcendentals=0),
        name="normalize",
    )(x, gain.reshape(1, dim))


def finish_kernel(x_ref, y_grad_ref, prob_ref, gate_grad_ref, balance_ref, gain_ref, router_ref, *rest):
    in_refs, out_refs, (y_ref, x_grad_ref, stats_ref) = rest[:CHUNKS], rest[CHUNKS:2 * CHUNKS], rest[2 * CHUNKS:]
    height = x_ref.shape[0]
    prob = prob_ref[...]
    prob_grad = gate_grad_ref[...] + balance_ref[...]
    logit_grad = (prob * (prob_grad - jnp.sum(prob * prob_grad, axis=0, keepdims=True))).astype(jnp.bfloat16)
    x = x_ref[...].astype(jnp.float32)
    inv_rms = lax.rsqrt(jnp.mean(x * x, axis=-1, keepdims=True) + NORM_EPS)
    unit = x * inv_rms
    gain = gain_ref[...]
    moe_out = of_this_chunk(height, out_refs).astype(jnp.float32)
    y_ref[...] = (x + moe_out).astype(y_ref.dtype)
    routed = lax.dot_general(logit_grad, router_ref[...], (((0,), (0,)), ((), ())), preferred_element_type=jnp.float32)
    x_norm_grad = of_this_chunk(height, in_refs).astype(jnp.float32) + routed
    unit_grad = x_norm_grad * gain
    x_grad = y_grad_ref[...].astype(jnp.float32) + inv_rms * (unit_grad - unit * jnp.mean(unit_grad * unit, axis=-1, keepdims=True))
    x_grad_ref[...] = x_grad.astype(x_grad_ref.dtype)
    x_norm = (unit * gain).astype(jnp.bfloat16)

    @pl.when(pl.program_id(0) == 0)
    def _():
        stats_ref[...] = jnp.zeros_like(stats_ref)

    def folded(values):
        return jnp.sum(values.reshape(height // 8, 8, values.shape[1]), axis=0)

    stats_ref[0:8, :] += jnp.dot(logit_grad, x_norm, preferred_element_type=jnp.float32)
    stats_ref[8:16, :] += folded(x_norm_grad * unit)
    stats_ref[16:24, :] += folded(moe_out * moe_out)


def finish(x, y_grad, prob, gate_grad, balance, gain, router, in_raw, out_raw):
    tokens, dim = x.shape
    height = LANES
    rows = pl.BlockSpec((height, dim), lambda t: (t, 0))
    of_tokens = pl.BlockSpec((8, height), lambda t: (0, t))
    return pl.pallas_call(
        finish_kernel,
        grid=(tokens // height,),
        in_specs=[
            rows, rows, of_tokens, of_tokens, pl.BlockSpec((8, height), lambda t: (0, 0)), pl.BlockSpec((1, dim), lambda t: (0, 0)),
            pl.BlockSpec((8, dim), lambda t: (0, 0)), *row_blocks(height, dim), *row_blocks(height, dim),
        ],
        out_specs=[rows, rows, pl.BlockSpec((32, dim), lambda t: (0, 0))],
        out_shape=[
            jax.ShapeDtypeStruct((tokens, dim), jnp.bfloat16), jax.ShapeDtypeStruct((tokens, dim), jnp.bfloat16),
            jax.ShapeDtypeStruct((32, dim), jnp.float32),
        ],
        compiler_params=pltpu.CompilerParams(vmem_limit_bytes=VMEM_LIMIT),
        cost_estimate=pl.CostEstimate(flops=10**9, bytes_accessed=25 * 10**6, transcendentals=0),
        name="finish",
    )(x, y_grad, prob, gate_grad, balance, gain.reshape(1, dim), router, *in_raw, *out_raw)


def below(size, strict):
    i = lax.broadcasted_iota(jnp.int32, (size, size), 0)
    j = lax.broadcasted_iota(jnp.int32, (size, size), 1)
    return (i < j if strict else i <= j).astype(jnp.float32)


def running(values):
    size = values.shape[-1]
    i = lax.broadcasted_iota(jnp.int32, (size, size), 0)
    j = lax.broadcasted_iota(jnp.int32, (size, size), 1)
    return jnp.sum(jnp.where(i <= j, values[..., :, None], 0), axis=-2)


def count(condition, axis):
    return jnp.sum(condition.astype(jnp.int32), axis=axis)


def choose_swap(rows, experts):
    work = 4 * ((rows + TILE - 1) // TILE) + (rows + TILE // 2 - 1) // (TILE // 2)
    none = jnp.zeros((rows.shape[0], 1), jnp.int32)
    sides = [work[:, :experts], work[:, experts:]]
    options = [jnp.concatenate([none, side], axis=1) for side in sides]
    moved = options[1][:, None, :] - options[0][:, :, None]
    loads = [jnp.sum(side, axis=1)[:, None, None] for side in sides]
    cost = jnp.sum(jnp.maximum(loads[0] + moved, loads[1] - moved), axis=0)
    index = lax.broadcasted_iota(jnp.int32, cost.shape, 0) * (experts + 1) + lax.broadcasted_iota(jnp.int32, cost.shape, 1)
    best = jnp.min(jnp.where(cost == jnp.min(cost), index, cost.size))
    return best // (experts + 1) - 1, best % (experts + 1) - 1


def routing(hot, experts_of, place):
    groups, span_total, _ = hot.shape
    spans_of = [part * (span_total * LANES // sum(PARTS)) // LANES for part in PARTS]
    firsts = [sum(spans_of[:c]) for c in range(CHUNKS)]
    chunk_of = jnp.concatenate([jnp.full((n,), c, jnp.int32) for c, n in enumerate(spans_of)])
    member = chunk_of[:, None] == jnp.arange(CHUNKS, dtype=jnp.int32)[None, :]
    same = chunk_of[:, None] == chunk_of[None, :]
    tiles_of = [2 * n * LANES // TILE + groups for n in spans_of]
    tiles_max = max(tiles_of)

    within = jnp.einsum("gsi,ij->gsj", hot, below(LANES, False), preferred_element_type=jnp.float32)
    span_count = jnp.sum(hot, axis=-1)
    before = jnp.einsum("gi,ij->gj", span_count, jnp.where(same, below(span_total, True), 0.0), preferred_element_type=jnp.float32)
    total = jnp.sum(jnp.where(member[:, None, :], span_count.T[:, :, None], 0.0), axis=0).T.astype(jnp.int32)
    tiles = (total + TILE - 1) // TILE
    none = jnp.logical_and(jnp.sum(tiles, axis=1, keepdims=True) == 0, jnp.arange(groups, dtype=jnp.int32) == 0)
    tiles = jnp.where(none, 1, tiles)
    stop = running(tiles)
    begin = stop - tiles

    def to_spans(values):
        return jnp.sum(jnp.where(member[None], values.T[:, None, :], 0), axis=2)

    span_first = to_spans(begin) * TILE + before.astype(jnp.int32)
    span_stop = span_first + span_count.astype(jnp.int32)
    pos = jnp.where(hot > 0, span_first[:, :, None] + within.astype(jnp.int32) - 1, -1)

    index = jnp.arange(groups, dtype=jnp.int32)
    tile = jnp.arange(tiles_max, dtype=jnp.int32)
    group = jnp.minimum(count(tile[None, :, None] >= stop[:, None, :], 2), groups - 1)
    mine = group[:, :, None] == index
    ordinal = running((tiles > 0).astype(jnp.int32)) - 1
    later = jnp.logical_and(index[None, None, :] > group[:, :, None], tiles[:, None, :] > 0)
    follow = jnp.min(jnp.where(later, index, groups), axis=2)
    follow = jnp.where(follow == groups, -1, follow)
    fresh = jnp.sum(jnp.where(mine, begin[:, None, :], 0), axis=2) == tile
    slot = jnp.sum(jnp.where(mine, ordinal[:, None, :], 0), axis=2) % 2
    rows_left = jnp.sum(jnp.where(mine, (total + begin * TILE)[:, None, :], 0), axis=2) - tile * TILE
    half = rows_left <= TILE // 2

    half_mine = jnp.repeat(mine, 2, axis=1)
    stops = jnp.sum(jnp.where(half_mine[..., None], span_stop[None, None], 0), axis=2)
    row0 = jnp.arange(2 * tiles_max, dtype=jnp.int32)[None, :, None] * LANES
    inside = member.T[:, None, :]
    lo = count(jnp.logical_and(inside, stops <= row0), 2)
    hi = jnp.minimum(count(jnp.logical_and(inside, stops < row0 + LANES), 2), jnp.array(spans_of, jnp.int32)[:, None] - 1)
    width = jnp.maximum(jnp.max(((hi - lo + 2) // 2).reshape(CHUNKS, tiles_max, 2), axis=2), 1)
    for narrower, wider in zip((WINDOWS[-1], *WIDE_WINDOWS), (*WIDE_WINDOWS, WHOLE_CHUNK)):
        width = jnp.where(jnp.logical_and(width > narrower, width <= wider), wider, width)
    start = jnp.minimum(span_first // 16 * 16, to_spans(stop) * TILE - REACH)
    empty = to_spans(tiles) == 0
    leading = jnp.logical_and(jnp.logical_not(empty), to_spans(ordinal) == 0)
    start = jnp.where(empty, jnp.sum(jnp.where(leading, start, 0), axis=0), start)
    over = jnp.any(jnp.logical_and(jnp.logical_not(empty), span_stop - start > REACH), axis=0)
    over = jnp.any(over.reshape(-1, GROUP), axis=1)

    units = (total + LANES - 1) // LANES
    in_chunks = running(units.T)
    both = in_chunks[:, -1]
    step_stop = running((both + UNITS - 1) // UNITS)
    step_first = step_stop - (both + UNITS - 1) // UNITS
    steps = CHUNKS * tiles_max // 2 + groups
    step = jnp.arange(steps, dtype=jnp.int32)
    owner = jnp.minimum(count(step[:, None] >= step_stop[None, :], 1), groups - 1)
    step_mine = owner[:, None] == index

    def of_step(values):
        return jnp.sum(jnp.where(step_mine[:, :, None], values[None], 0), axis=1)[:, None, :]

    local = UNITS * (step - of_step(step_first[:, None])[:, 0, 0])[:, None, None] + jnp.arange(UNITS, dtype=jnp.int32)[None, :, None]
    ends, sizes = of_step(in_chunks), of_step(units.T)
    offset = local - (ends - sizes)
    found = jnp.logical_and(offset >= 0, local < ends)
    chunk_at = jnp.arange(CHUNKS, dtype=jnp.int32) * 2 * tiles_max
    src = jnp.sum(jnp.where(found, 2 * of_step(begin.T) + offset + chunk_at + 1, 0), axis=2) - 1

    sections = (
        ("expert", experts_of), ("insert", place.reshape(1)), ("steps", step_stop[-1:]), ("owner", owner), ("src", src),
        ("count", stop[:, -1:]), ("group", group), ("slot", slot), ("fresh", fresh), ("half", half), ("next", follow), ("lo", lo), ("width", width),
        ("first", jnp.concatenate([jnp.zeros((CHUNKS, 1), jnp.int32), stop], axis=1)), ("start", start), ("over", over),
    )
    table = jnp.concatenate([values.reshape(-1).astype(jnp.int32) for _, values in sections])
    places, sizes_of, at = {}, {}, 0
    for name, values in sections:
        places[name], sizes_of[name] = at, values.size
        at += values.size
    layout = {}
    for c in range(CHUNKS):
        layout[c] = {name: places[name] + c * (sizes_of[name] // CHUNKS) for name in ("count", "group", "slot", "fresh", "half", "next", "lo", "width", "first")}
        layout[c] |= {
            "expert": places["expert"], "spans": (firsts[c], spans_of[c]), "part": PARTS[c], "rows_max": tiles_of[c] * TILE,
            "start": [places["start"] + g * span_total + firsts[c] for g in range(groups)],
            "over": places["over"] + firsts[c] // GROUP,
        }
    layout |= {"grad": {name: places[name] for name in ("steps", "owner", "src", "insert")}, "insert": places["insert"], "tiles_max": tiles_max}
    return pos, table, layout


def solution(mesh):
    tp_size = mesh.shape["tp"]
    ep_size = mesh.shape["ep"]
    dev_count = tp_size * ep_size
    rows_axes = ("ep", "tp")
    row_spec = P(rows_axes, None)
    wide_spec = P("ep", None, "tp")
    down_spec = P("ep", "tp", None)
    swap = [(0, 1), (1, 0)]

    def body(x, y_grad, expert_ids, norm_gain, w_router, w_gate, w_up, w_down):
        tokens, model_dim = x.shape
        top_k = expert_ids.shape[1]
        num_experts = w_router.shape[1]
        local_experts = w_gate.shape[0]
        total_tokens = tokens * dev_count
        my_ep = lax.axis_index("ep").astype(jnp.int32)
        firsts = [sum(PARTS[:c]) for c in range(CHUNKS)]

        def of_chunk(rows, c, axis=0):
            return lax.slice_in_dim(rows, firsts[c], firsts[c] + PARTS[c], axis=axis)

        def gather(rows):
            return lax.all_gather(rows, rows_axes, axis=0, tiled=True)

        def scatter(rows):
            return lax.psum_scatter(rows, rows_axes, scatter_dimension=0, tiled=True)

        def of_chunk_span(values, c):
            return values[:, firsts[c] * dev_count:(firsts[c] + PARTS[c]) * dev_count]

        def after(values, first):
            return lax.optimization_barrier((values, first))

        gain = norm_gain.astype(jnp.float32)
        rest = tokens - PARTS[0]
        head, tail = normalize(x, gain, 0, PARTS[0]), normalize(x, gain, PARTS[0], rest)
        gathered = [gather(head), gather(tail)]
        tok = [(gathered[0], (0, PARTS[0]))] + [(gathered[1], (firsts[c] - PARTS[0], rest)) for c in range(1, CHUNKS)]

        x_norm = jnp.concatenate([head, tail], axis=0)
        route_prob = jax.nn.softmax(jnp.dot(x_norm, w_router, preferred_element_type=jnp.float32), axis=-1)
        expert_range = jnp.arange(num_experts, dtype=jnp.int32)
        choice = jnp.sum((expert_ids[:, :, None] == expert_range[None, None, :]).astype(jnp.float32), axis=1)
        small = lax.all_gather(jnp.concatenate([choice, route_prob], axis=1).T, rows_axes, axis=0, tiled=False)
        counts = jnp.sum(small[:, :num_experts], axis=(0, 2))
        balance_scale = BALANCE_COEF * num_experts / (total_tokens * total_tokens * top_k)
        balance_loss = balance_scale * jnp.sum(counts * jnp.sum(small[:, num_experts:], axis=(0, 2)))

        rows_in = jnp.stack([jnp.sum(of_chunk(small[:, :num_experts], c, 2), axis=(0, 2)) for c in range(CHUNKS)])
        gives = choose_swap(rows_in.astype(jnp.int32), local_experts)
        given = jnp.where(my_ep == 0, gives[0], gives[1])
        taken = jnp.where(my_ep == 0, gives[1], gives[0])
        my_base = my_ep * local_experts
        local = jnp.arange(local_experts, dtype=jnp.int32)
        group_experts = jnp.concatenate([my_base + local, (local_experts - my_base + jnp.maximum(taken, 0)).reshape(1)])
        active = jnp.concatenate([local != given, (taken >= 0).reshape(1)])
        take = jnp.logical_and(group_experts[:, None] == expert_range, active[:, None])
        spread = jnp.concatenate([of_chunk(small, c, 2).transpose(1, 0, 2).reshape(2 * num_experts, -1) for c in range(CHUNKS)], axis=1)
        spread = spread.reshape(2, 1, num_experts, -1, LANES)
        own = jnp.sum(jnp.where(take[None, :, :, None, None], spread, 0.0), axis=2)
        prob = own[1]
        pos, table, layout = routing(own[0], group_experts, given)
        helped = [lax.ppermute(lax.dynamic_slice_in_dim(w, jnp.maximum(given, 0), 1, axis=0), "ep", swap) for w in (w_gate, w_up, w_down)]
        weights = (w_gate, w_up, w_down, *helped)

        grad_scale = 2.0 * ACT_COEF / (total_tokens * model_dim)
        own_prob = route_prob.T
        balance_row = jnp.broadcast_to(balance_scale * counts[:, None], (num_experts, LANES))
        router = w_router.T
        first_tok, (own_prob, balance_row, router, balance_loss) = after(tok[0][0], (own_prob, balance_row, router, balance_loss))
        tok[0] = (first_tok, tok[0][1])
        x_rows, gate_rows, pre, hidden, d_rows, mg_rows = [], [], [], [], [], []
        out_raw, moe_out, m_own, m_tok, in_raw, gate_part = [], [], [], [], [], []

        def send_cotangent(c, gate):
            raw, (gate, _) = after(out_raw[c], (gate, m_own[-1:]))
            moe_out.append(raw)
            moe_grad = of_chunk(y_grad, c).astype(jnp.float32) + grad_scale * raw.astype(jnp.float32)
            m_own.append(moe_grad.astype(jnp.bfloat16))
            m_tok.append(gather(m_own[c]))
            return gate

        for c in range(CHUNKS):
            rows, gates, ab, h, out_rows = forward(layout, c, table, pos, prob, tok[c], weights)
            if c == 1:
                out_rows = send_cotangent(0, out_rows)
            (partial,) = combine(layout, c, table, pos, out_rows)
            if c == 0:
                partial, later = after(partial, gathered[1])
                tok[1:] = [(later, place) for _, place in tok[1:]]
            if c > 1:
                partial = send_cotangent(c - 1, partial)
            out_raw.append(scatter(partial))
            x_rows.append(rows)
            gate_rows.append(gates)
            pre.append(ab)
            hidden.append(h)
        for c in range(CHUNKS):
            d, in_rows, mg, dgate = backward(layout, c, table, pos, m_tok[c], pre[c], hidden[c], gate_rows[c], weights)
            if c == 0:
                in_rows = send_cotangent(CHUNKS - 1, in_rows)
            partial, gate_terms = combine(layout, c, table, pos, in_rows, dgate)
            if c == 0:
                m_tok[1], partial = after(m_tok[1], partial)
            in_raw.append(scatter(partial))
            gate_part.append(gate_terms)
            d_rows.append(d)
            mg_rows.append(mg)
        *wide_grads, helped_gate, helped_up = weight_grad(layout, table, x_rows, d_rows, local_experts, 2)
        back = []
        for grad in (helped_gate, helped_up):
            back.append(lax.ppermute(grad, "ep", swap))

        gate_sums = lax.psum(jnp.concatenate(gate_part, axis=1), ("tp", "ep"))
        device = my_ep * tp_size + lax.axis_index("tp")
        gate_sums = [
            lax.dynamic_slice_in_dim(of_chunk_span(gate_sums, c), device * PARTS[c], PARTS[c], axis=1) for c in range(CHUNKS)
        ]
        gate_weight_grad = jnp.concatenate(gate_sums, axis=1)
        gate_weight_grad, (wide_grads, in_raw) = after(gate_weight_grad, (wide_grads, in_raw))
        y, x_grad, stats = finish(x, y_grad, own_prob, gate_weight_grad, balance_row, gain, router, in_raw, moe_out)
        stats, (mg_rows[0], x_grad) = after(stats, (mg_rows[0], x_grad))
        down_grad, helped_down, gate_grad, up_grad = weight_grad(layout, table, hidden, mg_rows, local_experts, 1, back, wide_grads)
        (down_grad,) = insert(layout, table, [lax.ppermute(helped_down, "ep", swap)], [down_grad])
        stats = lax.psum(stats, ("tp", "ep"))
        router_sum = stats[:num_experts].T
        gain_sum = jnp.sum(stats[8:16], axis=0)
        act_loss = ACT_COEF * jnp.sum(stats[16:24]) / (total_tokens * model_dim)
        return (y, x_grad, gain_sum.astype(jnp.bfloat16), router_sum.astype(jnp.bfloat16), gate_grad, up_grad, down_grad, balance_loss, act_loss)

    return jax.shard_map(body, mesh=mesh, in_specs=(row_spec, row_spec, row_spec, P(), P(), wide_spec, wide_spec, down_spec), out_specs=(row_spec, row_spec, P(), P(), wide_spec, wide_spec, down_spec, P(), P()), check_vma=False)
```
